128 devices in a mesh: row: 8 (over z, y_hi), col: 16 (over x, y_lo, core).
Axes of the slice: x: 4, y: 4 (y_hi: 2, y_lo: 2; y = y_hi * 2 + y_lo), z: 4, core: 2. Of those that a mesh axis runs over, the one named last changes fastest.
Arguments:
- tokens_in: bfloat16 [16384, 1408], P(('row', 'col')), may hold values from -300 to 300
- ln1_gain: bfloat16 [1408], replicated, may hold values from 0.099609375 to 1.8984375
- ln1_bias: bfloat16 [1408], replicated, may hold values from -3 to 3
- qkv_weight: bfloat16 [1408, 4224], P('row', 'col'), may hold values from -0.8 to 0.8
- qkv_bias: bfloat16 [4224], P('col'), may hold values from -3 to 3
- proj_weight: bfloat16 [1408, 1408], P('col', 'row'), may hold values from -0.15625 to 0.15625
- proj_bias: bfloat16 [1408], replicated, may hold values from -3 to 3
- ln2_gain: bfloat16 [1408], replicated, may hold values from 0.099609375 to 1.8984375
- ln2_bias: bfloat16 [1408], replicated, may hold values from -3 to 3
- fc1_weight: bfloat16 [1408, 6144], P('row', 'col'), may hold values from -0.15625 to 0.15625
- fc1_bias: bfloat16 [6144], P('col'), may hold values from -3 to 3
- fc2_weight: bfloat16 [1408, 6144], P('row', 'col'), may hold values from -0.078125 to 0.078125
- fc2_bias: bfloat16 [1408], replicated, may hold values from -3 to 3
Outputs:
- tokens_out: bfloat16 [16384, 1408], P(('row', 'col'))
The draws below stay inside these ranges and needn't reach their ends.
All inputs are finite; a program needn't handle non-finite values.
Results may differ from the reference program's by a relative error of at most 0.01.
Values may be sent and summed in bfloat16 or wider, within the bound.
No kernel may reach another device: no remote copies, remote signals or barrier semaphores. Data moves between devices by JAX's collectives and lax.ppermute only.
A program may use at most 64 MiB of HBM per device.

```python
import jax
import jax.numpy as jnp
from jax import lax

D = 1408
HEADS = 16
FF = 6144
LEN = 2048
TOKENS = 16384
N_ROW = 8
N_COL = 16


def draw_tokens_in(key, part):
    key_base = jax.random.fold_in(key, 11)
    columns = 1.0 + 2.0 * jnp.arange(D, dtype=jnp.float32) / (D - 1)
    base = jax.random.normal(key_base, (TOKENS, D), jnp.float32)
    return (base * columns).astype(jnp.bfloat16)


def draw_qkv_weight(key, part):
    noise = jax.random.normal(jax.random.fold_in(key, 21), (D, 3 * D), jnp.float32) * D ** (-0.5)
    return jnp.clip(noise, -0.8, 0.8).astype(jnp.bfloat16)


def shard_levels(stream_key, dims, cuts, low, largest):
    level, own = 1.0, jax.random.fold_in(stream_key, 6)
    for position, shards_of in cuts:
        draws = jnp.exp(jax.random.uniform(jax.random.fold_in(own, position), (shards_of,), jnp.float32, low / len(cuts), largest / len(cuts)))
        level = level * jnp.repeat(draws, dims[position] // shards_of).reshape([-1 if axis == position else 1 for axis in range(len(dims))])
    return level


def normal_values(own_key, dims, spread, reach, pieces=(), held_as=jnp.bfloat16):
    level = shard_levels(own_key, dims, pieces, -0.22, 0.18) if pieces else 1.0
    drawn = jax.random.normal(own_key, dims, jnp.float32) * spread * level
    return jnp.minimum(jnp.maximum(drawn, -reach), reach).astype(held_as)


def setup_inputs(seed: int = 0) -> dict:
    streams_of = jax.random.split(jax.random.key(seed), 14)
    return {
        "tokens_in": draw_tokens_in(jax.random.fold_in(streams_of[13], 71), 0),
        "ln1_gain": jnp.clip(1.0 + 0.18 * jax.random.normal(streams_of[1], (D,), jnp.float32), 0.099609375, 1.8984375).astype(jnp.bfloat16),
        "ln1_bias": normal_values(streams_of[2], (D,), 0.5, 3.0),
        "qkv_weight": draw_qkv_weight(jax.random.fold_in(streams_of[13], 71), 0),
        "qkv_bias": normal_values(streams_of[4], (3 * D,), 0.5, 3.0, ((0, 16),)),
        "proj_weight": normal_values(streams_of[5], (D, D), D ** -0.5, 0.15625, ((0, 16), (1, 8))),
        "proj_bias": normal_values(streams_of[6], (D,), 0.5, 3.0),
        "ln2_gain": jnp.clip(1.0 + 0.18 * jax.random.normal(streams_of[7], (D,), jnp.float32), 0.099609375, 1.8984375).astype(jnp.bfloat16),
        "ln2_bias": normal_values(streams_of[8], (D,), 0.5, 3.0),
        "fc1_weight": normal_values(streams_of[9], (D, FF), D ** -0.5, 0.15625, ((0, 8), (1, 16))),
        "fc1_bias": normal_values(streams_of[10], (FF,), 0.5, 3.0, ((0, 16),)),
        "fc2_weight": normal_values(streams_of[11], (D, FF), FF ** -0.5, 0.078125, ((0, 8), (1, 16))),
        "fc2_bias": normal_values(streams_of[12], (D,), 0.5, 3.0),
    }


def layer_norm(values, gain, bias):
    mean = lax.optimization_barrier(jnp.mean(values, axis=-1, keepdims=True))
    centred = values - mean
    var = lax.optimization_barrier(jnp.mean(centred * centred, axis=-1, keepdims=True))
    return centred * lax.rsqrt(var + 1e-06) * gain.astype(jnp.float32) + bias.astype(jnp.float32)

def attend(qkv, heads):
    length = qkv.shape[0]
    head_size = qkv.shape[1] // (3 * heads)
    parts = qkv.reshape(length, heads, 3, head_size).astype(jnp.float32)
    query = parts[:, :, 0]
    keys = parts[:, :, 1]
    values = parts[:, :, 2]
    block = min(512, length)
    blocks = query.reshape(length // block, block, heads, head_size)
    scale = 1.0 / head_size ** 0.5

    def one_block(qblock):
        scores = jnp.einsum('qhe,khe->hqk', qblock, keys) * scale
        top = lax.optimization_barrier(jnp.max(scores, axis=-1, keepdims=True))
        expo = jnp.exp(scores - top)
        probs = (expo / lax.optimization_barrier(jnp.sum(expo, axis=-1, keepdims=True))).astype(jnp.bfloat16)
        mixed = jnp.einsum('hqk,khe->qhe', probs.astype(jnp.float32), values)
        return mixed.astype(jnp.bfloat16).reshape(block, heads * head_size)
    return lax.map(one_block, blocks).reshape(length, heads * head_size)

def grouped_sum(left, right, groups):
    width = left.shape[1] // groups
    lefts = left.reshape(left.shape[0], groups, width).transpose(1, 0, 2)
    rights = right.reshape(groups, width, right.shape[1])

    def add_group(total, pair):
        part = jnp.dot(pair[0], pair[1], preferred_element_type=jnp.float32).astype(jnp.bfloat16)
        part = lax.optimization_barrier(part)
        return (total + part.astype(jnp.float32), None)
    start = jnp.zeros((left.shape[0], right.shape[1]), jnp.float32)
    total, _ = lax.scan(add_group, start, (lefts, rights))
    return total

def reference(tokens_in, ln1_gain, ln1_bias, qkv_weight, qkv_bias, proj_weight, proj_bias, ln2_gain, ln2_bias, fc1_weight, fc1_bias, fc2_weight, fc2_bias):
    inputs = tokens_in.astype(jnp.float32)
    ln1 = layer_norm(inputs, ln1_gain, ln1_bias).astype(jnp.bfloat16)
    qkv = jnp.dot(ln1, qkv_weight, preferred_element_type=jnp.float32) + qkv_bias.astype(jnp.float32)
    qkv = qkv.astype(jnp.bfloat16)
    clips = qkv.reshape(N_ROW, LEN, 3 * D)
    attn = lax.map(lambda clip: attend(clip, HEADS), clips).reshape(TOKENS, D)
    resid = inputs + grouped_sum(attn, proj_weight, N_COL) + proj_bias.astype(jnp.float32)
    ln2 = layer_norm(resid, ln2_gain, ln2_bias).astype(jnp.bfloat16)
    hidden = jnp.dot(ln2, fc1_weight, preferred_element_type=jnp.float32) + fc1_bias.astype(jnp.float32)
    hidden = jax.nn.gelu(hidden, approximate=False).astype(jnp.bfloat16)
    result = resid + grouped_sum(hidden, fc2_weight.T, N_COL) + fc2_bias.astype(jnp.float32)
    return result.astype(jnp.bfloat16)
```

```python
import itertools

import jax
import jax.numpy as jnp
import numpy as np
from jax import lax
from jax.sharding import Mesh
from jax.sharding import PartitionSpec as P

AXES = ("z", "yh", "x", "yl", "core")
SIZES = (4, 2, 4, 2, 2)
ROW = ("z", "yh")
COL = ("x", "yl", "core")


def shift(value, dz=0, dyh=0, dx=0, dyl=0, dc=0):
    pairs = []
    for place in itertools.product(*[range(n) for n in SIZES]):
        target = [(p + d) % n for p, d, n in zip(place, (dz, dyh, dx, dyl, dc), SIZES)]
        pairs.append(
            (int(np.ravel_multi_index(place, SIZES)), int(np.ravel_multi_index(target, SIZES)))
        )
    return lax.ppermute(value, AXES, pairs)


def copy_for_each(value, axis):
    size = lax.axis_size(axis)
    return lax.all_to_all(
        jnp.broadcast_to(value[None], (size, *value.shape)), axis, 0, 0, tiled=True
    )


def norm_local(values, gain, bias):
    mean = jnp.mean(values, axis=-1, keepdims=True)
    centred = values - mean
    var = jnp.mean(centred * centred, axis=-1, keepdims=True)
    return centred * lax.rsqrt(var + 1e-06) * gain.astype(jnp.float32) + bias.astype(jnp.float32)


def attend(qkv, head_size):
    length = qkv.shape[0]
    query = qkv[:, :head_size]
    keys = qkv[:, head_size : 2 * head_size]
    values = qkv[:, 2 * head_size :]
    block = 512
    blocks = query.reshape(length // block, block, head_size)
    scale = 1.0 / head_size**0.5

    def one_block(qblock):
        scores = jnp.einsum("qe,ke->qk", qblock, keys, preferred_element_type=jnp.float32) * scale
        top = jnp.max(scores, axis=-1, keepdims=True)
        expo = jnp.exp(scores - top)
        probs = (expo / jnp.sum(expo, axis=-1, keepdims=True)).astype(jnp.bfloat16)
        mixed = jnp.einsum("qk,ke->qe", probs, values, preferred_element_type=jnp.float32)
        return mixed.astype(jnp.bfloat16)

    return lax.map(one_block, blocks).reshape(length, head_size)


def local(
    tokens_in,
    ln1_gain,
    ln1_bias,
    qkv_weight,
    qkv_bias,
    proj_weight,
    proj_bias,
    ln2_gain,
    ln2_bias,
    fc1_weight,
    fc1_bias,
    fc2_weight,
    fc2_bias,
):
    f32, bf16 = jnp.float32, jnp.bfloat16
    own = tokens_in.shape[0]
    width = tokens_in.shape[1]
    head = proj_weight.shape[0]
    slab = qkv_weight.shape[0]
    hid = fc1_weight.shape[1]
    inputs = tokens_in.astype(f32)
    core = lax.axis_index("core")

    ln1 = norm_local(inputs, ln1_gain, ln1_bias).astype(bf16)
    ln1_full = lax.all_gather(ln1, COL, axis=0, tiled=True)
    qkv_full = copy_for_each(qkv_weight, ROW)
    proj_rows = copy_for_each(proj_weight, ROW)

    bias_rows = jnp.broadcast_to(fc1_bias[None], (16, hid))
    stack = jnp.concatenate([fc1_weight, fc2_weight, bias_rows], axis=0)
    stack, ln1_full, qkv_full, proj_rows = lax.optimization_barrier(
        (stack, ln1_full, qkv_full, proj_rows)
    )
    qkv_full = qkv_full.reshape(width, qkv_weight.shape[1])
    proj_own = jnp.moveaxis(proj_rows, 0, 1).reshape(head, width)
    mlp = lax.all_gather(stack, ("z", "yh", "yl", "core"), axis=0, tiled=False)
    mlp = mlp.reshape(8, 4, stack.shape[0], hid)

    me = lax.axis_index("x") * 2 + lax.axis_index("yl")
    proj = jnp.zeros((8, head, width), bf16)
    for dx, dyl in itertools.product(range(4), range(2)):
        piece = shift(proj_own, dx=dx, dyl=dyl) if dx + dyl else proj_own
        at = (lax.axis_index("x") + 4 - dx) % 4 * 2 + (lax.axis_index("yl") + dyl) % 2
        proj = lax.dynamic_update_slice(proj, piece[None], (at, 0, 0))
    del me
    proj = proj.reshape(8 * head, width)

    qkv = jnp.dot(ln1_full, qkv_full, preferred_element_type=f32) + qkv_bias.astype(f32)
    attn = attend(qkv.astype(bf16), head)
    heads = lax.all_to_all(attn, ("x", "yl"), split_axis=0, concat_axis=1, tiled=True)
    part = jnp.dot(heads, proj, preferred_element_type=f32).astype(bf16)
    mine = lax.dynamic_slice(part, (core * own, 0), (own, width))
    other = lax.dynamic_slice(part, ((1 - core) * own, 0), (own, width))
    other = shift(other, dc=1)
    resid = inputs + (mine.astype(f32) + other.astype(f32)) + proj_bias.astype(f32)
    ln2 = norm_local(resid, ln2_gain, ln2_bias).astype(bf16)

    half = own // 2
    left = shift(ln2, dx=1)
    right = shift(ln2, dx=3)
    far_a = shift(left[:half], dx=1)
    far_b = shift(right[half:], dx=3)
    rows = jnp.concatenate([ln2, left, right, far_a, far_b], axis=0)

    w1 = mlp[:, :, :slab].transpose(0, 2, 1, 3).reshape(width, 4 * hid)
    w2 = mlp[:, :, slab : 2 * slab].transpose(0, 2, 1, 3).reshape(width, 4 * hid)
    b1 = mlp[0, :, 2 * slab].reshape(4 * hid).astype(f32)
    hidden = jnp.dot(rows, w1, preferred_element_type=f32) + b1
    hidden = jax.nn.gelu(hidden, approximate=False).astype(bf16)
    out = lax.dot_general(hidden, w2, (((1,), (1,)), ((), ())), preferred_element_type=f32)

    p_own, p_left, p_right = out[:own], out[own : 2 * own], out[2 * own : 3 * own]
    p_far = out[3 * own :].astype(bf16)
    via_a = shift(p_far[:half], dx=1)
    via_b = shift(p_far[half:], dx=3)
    to_right = jnp.concatenate([p_right[:half] + via_a.astype(f32), p_right[half:]], axis=0)
    to_left = jnp.concatenate([p_left[:half], p_left[half:] + via_b.astype(f32)], axis=0)
    from_left = shift(to_right.astype(bf16), dx=1)
    from_right = shift(to_left.astype(bf16), dx=3)
    total = p_own + from_left.astype(f32) + from_right.astype(f32)
    result = resid + total + fc2_bias.astype(f32)
    return result.astype(bf16)


def solution(mesh):
    fine = Mesh(np.asarray(mesh.devices).reshape(SIZES), AXES)
    in_specs = (
        P(AXES, None),
        P(),
        P(),
        P(ROW, COL),
        P(COL),
        P(COL, ROW),
        P(),
        P(),
        P(),
        P(ROW, COL),
        P(COL),
        P(ROW, COL),
        P(),
    )
    return jax.shard_map(
        local, mesh=fine, in_specs=in_specs, out_specs=P(AXES, None), check_vma=False
    )
```

```python
import functools
import itertools

import jax
import jax.numpy as jnp
import numpy as np
from jax import lax
from jax.experimental import pallas as pl
from jax.experimental.pallas import tpu as pltpu
from jax.sharding import Mesh
from jax.sharding import PartitionSpec as P

HEADS = 16
AXES = ("z", "yh", "x", "yl", "core")
SIZES = (4, 2, 4, 2, 2)
ROW = ("z", "yh")
COL = ("x", "yl", "core")


def shift(value, dz=0, dyh=0, dx=0, dyl=0, dc=0):
    pairs = []
    for place in itertools.product(*[range(n) for n in SIZES]):
        target = [(p + d) % n for p, d, n in zip(place, (dz, dyh, dx, dyl, dc), SIZES)]
        pairs.append(
            (int(np.ravel_multi_index(place, SIZES)), int(np.ravel_multi_index(target, SIZES)))
        )
    return lax.ppermute(value, AXES, pairs)


def whole(shape_dtype=None):
    return pl.BlockSpec(memory_space=pltpu.VMEM)


def norm_rows(values, gain, bias):
    mean = jnp.mean(values, axis=-1, keepdims=True)
    centred = values - mean
    var = jnp.mean(centred * centred, axis=-1, keepdims=True)
    return centred * lax.rsqrt(var + 1e-06) * gain.astype(jnp.float32) + bias.astype(jnp.float32)


def ln1_kernel(x_ref, gain_ref, bias_ref, out_ref):
    values = x_ref[...].astype(jnp.float32)
    out_ref[...] = norm_rows(values, gain_ref[...], bias_ref[...]).astype(out_ref.dtype)


def first_norm(x, gain, bias):
    return pl.pallas_call(
        ln1_kernel,
        out_shape=jax.ShapeDtypeStruct(x.shape, jnp.bfloat16),
        in_specs=[whole()] * 3,
        out_specs=whole(),
        cost_estimate=pl.CostEstimate(flops=10 * x.size, bytes_accessed=4 * x.size, transcendentals=0),
        name="first_norm",
    )(x, gain[None], bias[None])


def place_kernel(slab, where_ref, own_ref, one_ref, two_ref, three_ref, qkv_ref, proj_ref):
    for dz, ref in enumerate((own_ref, one_ref, two_ref, three_ref)):
        for j in range(2):
            at = where_ref[2 * dz + j]
            qkv_ref[at] = ref[j, :slab]
            proj_ref[at] = ref[j, slab:, : proj_ref.shape[2]]


def place(where, pieces, slab, head):
    cols = pieces[0].shape[2]
    return pl.pallas_call(
        functools.partial(place_kernel, slab),
        out_shape=(
            jax.ShapeDtypeStruct((8, slab, cols), jnp.bfloat16),
            jax.ShapeDtypeStruct((8, head, slab), jnp.bfloat16),
        ),
        in_specs=[pl.BlockSpec(memory_space=pltpu.SMEM)] + [whole()] * 4,
        out_specs=(whole(), whole()),
        cost_estimate=pl.CostEstimate(flops=1000000, bytes_accessed=3000000, transcendentals=0),
        name="place_rows",
    )(where, *pieces)


def proj_kernel(where_ref, heads_ref, own_ref, left_ref, right_ref, fa_ref, fb_ref, mine_ref, other_ref):
    own = mine_ref.shape[0]
    core = where_ref[8]
    pieces = (
        own_ref.at[0],
        own_ref.at[1],
        left_ref.at[0],
        left_ref.at[1],
        right_ref.at[0],
        right_ref.at[1],
        fa_ref,
        fb_ref,
    )
    for target, first in ((mine_ref, core * own), (other_ref, (1 - core) * own)):
        total = jnp.zeros(target.shape, jnp.float32)
        for i, ref in enumerate(pieces):
            left = heads_ref[where_ref[i], pl.ds(pl.multiple_of(first, own), own), :]
            total += jnp.dot(left, ref[...], preferred_element_type=jnp.float32)
        target[...] = total.astype(target.dtype)


def project(where, heads, pieces, own, width):
    out = jax.ShapeDtypeStruct((own, width), jnp.bfloat16)
    return pl.pallas_call(
        proj_kernel,
        out_shape=(out, out),
        in_specs=[pl.BlockSpec(memory_space=pltpu.SMEM)] + [whole()] * 6,
        out_specs=(whole(), whole()),
        cost_estimate=pl.CostEstimate(flops=510000000, bytes_accessed=4000000, transcendentals=0),
        name="project",
    )(where, heads, *pieces)


def ln2_kernel(x_ref, mine_ref, other_ref, pbias_ref, gain_ref, bias_ref, ln2_ref, resid_ref):
    f32 = jnp.float32
    total = mine_ref[...].astype(f32) + other_ref[...].astype(f32)
    resid = x_ref[...].astype(f32) + total + pbias_ref[...].astype(f32)
    resid_ref[...] = resid
    ln2_ref[...] = norm_rows(resid, gain_ref[...], bias_ref[...]).astype(ln2_ref.dtype)


def second_norm(x, mine, other, pbias, gain, bias):
    return pl.pallas_call(
        ln2_kernel,
        out_shape=(
            jax.ShapeDtypeStruct(x.shape, jnp.bfloat16),
            jax.ShapeDtypeStruct(x.shape, jnp.float32),
        ),
        in_specs=[whole()] * 6,
        out_specs=(whole(), whole()),
        cost_estimate=pl.CostEstimate(flops=12 * x.size, bytes_accessed=12 * x.size, transcendentals=0),
        name="second_norm",
    )(x, mine, other, pbias[None], gain[None], bias[None])


def gelu(x):
    return 0.5 * x * (1.0 + lax.erf(x * 0.7071067811865476))


def mlp_kernel(slab, own_ref, left_ref, right_ref, fa_ref, fb_ref, w_ref,
               pown_ref, pleft_ref, pright_ref, pfar_ref,
               rows, w1, w2, b1, hidden, sem1, sem2, sem3):
    f32 = jnp.float32
    own = own_ref.shape[0]
    hid = w_ref.shape[3]
    loads1 = [[], [], [], []]
    loads2 = []
    for b in range(4):
        cols = pl.ds(b * hid, hid)
        for r in range(8):
            copy = pltpu.make_async_copy(
                w_ref.at[r, b, pl.ds(0, slab)], w1.at[pl.ds(r * slab, slab), cols], sem1.at[b, r]
            )
            copy.start()
            loads1[b].append(copy)
        copy = pltpu.make_async_copy(w_ref.at[0, b, pl.ds(2 * slab, 16)], b1.at[b], sem3.at[b])
        copy.start()
        loads1[b].append(copy)
    for b in range(4):
        for r in range(8):
            copy = pltpu.make_async_copy(
                w_ref.at[r, b, pl.ds(slab, slab)],
                w2.at[pl.ds(r * slab, slab), pl.ds(b * hid, hid)],
                sem2.at[b, r],
            )
            copy.start()
            loads2.append(copy)
    rows[:own] = own_ref[...]
    rows[own : 2 * own] = left_ref[...]
    rows[2 * own : 3 * own] = right_ref[...]
    rows[3 * own : 3 * own + own // 2] = fa_ref[...]
    rows[3 * own + own // 2 :] = fb_ref[...]
    for b in range(4):
        for copy in loads1[b]:
            copy.wait()
        cols = slice(b * hid, (b + 1) * hid)
        for m in range(2):
            part = slice(2 * own * m, 2 * own * (m + 1))
            value = jnp.dot(rows[part], w1[:, cols], preferred_element_type=f32)
            value = value + b1[b, 0:1].astype(f32)
            hidden[part, cols] = gelu(value).astype(hidden.dtype)
    for copy in loads2:
        copy.wait()
    for i, ref in ((3, pfar_ref), (2, pright_ref), (1, pleft_ref), (0, pown_ref)):
        out = lax.dot_general(
            hidden[i * own : (i + 1) * own],
            w2[...],
            (((1,), (1,)), ((), ())),
            preferred_element_type=f32,
        )
        ref[...] = out.astype(ref.dtype)


def mlp_block(pieces, weights, slab):
    own, width = pieces[0].shape
    hid = weights.shape[3]
    f32, bf16 = jnp.float32, jnp.bfloat16
    return pl.pallas_call(
        functools.partial(mlp_kernel, slab),
        out_shape=tuple(jax.ShapeDtypeStruct((own, width), t) for t in (f32, f32, f32, bf16)),
        in_specs=[whole()] * 5 + [pl.BlockSpec(memory_space=pl.ANY)],
        out_specs=(whole(),) * 4,
        scratch_shapes=[
            pltpu.VMEM((4 * own, width), bf16),
            pltpu.VMEM((width, 4 * hid), bf16),
            pltpu.VMEM((width, 4 * hid), bf16),
            pltpu.VMEM((4, 16, hid), bf16),
            pltpu.VMEM((4 * own, 4 * hid), bf16),
            pltpu.SemaphoreType.DMA((4, 8)),
            pltpu.SemaphoreType.DMA((4, 8)),
            pltpu.SemaphoreType.DMA((4,)),
        ],
        cost_estimate=pl.CostEstimate(flops=4430000000, bytes_accessed=12000000, transcendentals=800000),
        name="mlp_block",
    )(*pieces, weights)


def attend(qkv, head_size):
    length = qkv.shape[0]
    query = qkv[:, :head_size]
    keys = qkv[:, head_size : 2 * head_size]
    values = qkv[:, 2 * head_size :]
    block = 512
    blocks = query.reshape(length // block, block, head_size)
    scale = 1.0 / head_size**0.5

    def one_block(qblock):
        scores = jnp.einsum("qe,ke->qk", qblock, keys, preferred_element_type=jnp.float32) * scale
        top = jnp.max(scores, axis=-1, keepdims=True)
        expo = jnp.exp(scores - top)
        probs = (expo / jnp.sum(expo, axis=-1, keepdims=True)).astype(jnp.bfloat16)
        mixed = jnp.einsum("qk,ke->qe", probs, values, preferred_element_type=jnp.float32)
        return mixed.astype(jnp.bfloat16)

    return lax.map(one_block, blocks).reshape(length, head_size)


def local(
    tokens_in,
    ln1_gain,
    ln1_bias,
    qkv_weight,
    qkv_bias,
    proj_weight,
    proj_bias,
    ln2_gain,
    ln2_bias,
    fc1_weight,
    fc1_bias,
    fc2_weight,
    fc2_bias,
):
    f32, bf16 = jnp.float32, jnp.bfloat16
    own = tokens_in.shape[0]
    width = tokens_in.shape[1]
    head = proj_weight.shape[0]
    slab = qkv_weight.shape[0]
    hid = fc1_weight.shape[1]
    core = lax.axis_index("core")
    z, yh = lax.axis_index("z"), lax.axis_index("yh")
    x, yl = lax.axis_index("x"), lax.axis_index("yl")

    wide = jnp.pad(proj_weight, ((0, 0), (0, qkv_weight.shape[1] - slab)))
    rowset = jnp.concatenate([qkv_weight, wide], axis=0)
    pair = jnp.stack([rowset, shift(rowset, dyh=1)])
    pieces = [pair] + [shift(pair, dz=dz) for dz in (1, 2, 3)]
    where = jnp.stack([(z + 4 - dz) % 4 * 2 + (yh + j) % 2 for dz in range(4) for j in range(2)])
    qkv_full, proj_rows = place(where.astype(jnp.int32), pieces, slab, head)

    ln1 = first_norm(tokens_in, ln1_gain, ln1_bias)
    ln1_full = lax.all_gather(ln1, COL, axis=0, tiled=True)

    bias_rows = jnp.broadcast_to(fc1_bias[None], (16, hid))
    stack = jnp.concatenate([fc1_weight, fc2_weight, bias_rows], axis=0)
    stack, ln1_full, qkv_full, proj_rows = lax.optimization_barrier(
        (stack, ln1_full, qkv_full, proj_rows)
    )
    qkv_full = qkv_full.reshape(width, qkv_weight.shape[1])
    proj_own = jnp.moveaxis(proj_rows, 0, 1).reshape(head, width)
    mlp = lax.all_gather(stack, ("z", "yh", "yl", "core"), axis=0, tiled=False)
    mlp = mlp.reshape(8, 4, stack.shape[0], hid)

    p_pair = jnp.stack([proj_own, shift(proj_own, dyl=1)])
    p_left = shift(p_pair, dx=1)
    p_right = shift(p_pair, dx=3)
    p_fa = shift(p_left[0], dx=1)
    p_fb = shift(p_right[1], dx=3)
    order = [(0, 0), (0, 1), (1, 0), (1, 1), (3, 0), (3, 1), (2, 0), (2, 1)]
    spots = [(x + 4 - dx) % 4 * 2 + (yl + j) % 2 for dx, j in order]
    spots = jnp.stack(spots + [core]).astype(jnp.int32)

    qkv = jnp.dot(ln1_full, qkv_full, preferred_element_type=f32) + qkv_bias.astype(f32)
    attn = attend(qkv.astype(bf16), head)
    heads = lax.all_to_all(attn.reshape(8, 2 * own, head), ("x", "yl"), 0, 0, tiled=True)
    mine, other = project(spots, heads, (p_pair, p_left, p_right, p_fa, p_fb), own, width)
    other = shift(other, dc=1)
    ln2, resid = second_norm(tokens_in, mine, other, proj_bias, ln2_gain, ln2_bias)

    half = own // 2
    left = shift(ln2, dx=1)
    right = shift(ln2, dx=3)
    far_a = shift(left[:half], dx=1)
    far_b = shift(right[half:], dx=3)
    o_own, o_left, o_right, o_far = mlp_block((ln2, left, right, far_a, far_b), mlp, slab)

    via_a = shift(o_far[:half], dx=1)
    via_b = shift(o_far[half:], dx=3)
    to_right = jnp.concatenate([o_right[:half] + via_a.astype(f32), o_right[half:]], axis=0)
    to_left = jnp.concatenate([o_left[:half], o_left[half:] + via_b.astype(f32)], axis=0)
    from_left = shift(to_right.astype(bf16), dx=1)
    from_right = shift(to_left.astype(bf16), dx=3)
    total = o_own + from_left.astype(f32) + from_right.astype(f32)
    result = resid + total + fc2_bias.astype(f32)
    return result.astype(bf16)


def solution(mesh):
    fine = Mesh(np.asarray(mesh.devices).reshape(SIZES), AXES)
    in_specs = (
        P(AXES, None),
        P(),
        P(),
        P(ROW, COL),
        P(COL),
        P(COL, ROW),
        P(),
        P(),
        P(),
        P(ROW, COL),
        P(COL),
        P(ROW, COL),
        P(),
    )
    step = jax.shard_map(
        local, mesh=fine, in_specs=in_specs, out_specs=P(AXES, None), check_vma=False
    )
    return step
```

```python
import functools
import itertools

import jax
import jax.numpy as jnp
import numpy as np
from jax import lax
from jax.experimental import pallas as pl
from jax.experimental.pallas import tpu as pltpu
from jax.sharding import Mesh
from jax.sharding import PartitionSpec as P


LANES = 128
AXES = ("z", "yh", "x", "yl", "core")
SIZES = (4, 2, 4, 2, 2)
ROW = ("z", "yh")
COL = ("x", "yl", "core")


def shift(value, dz=0, dyh=0, dx=0, dyl=0, dc=0):
    pairs = []
    for place in itertools.product(*[range(n) for n in SIZES]):
        target = [(p + d) % n for p, d, n in zip(place, (dz, dyh, dx, dyl, dc), SIZES)]
        pairs.append(
            (int(np.ravel_multi_index(place, SIZES)), int(np.ravel_multi_index(target, SIZES)))
        )
    return lax.ppermute(value, AXES, pairs)


def whole():
    return pl.BlockSpec(memory_space=pltpu.VMEM)


def norm_rows(values, gain, bias):
    mean = jnp.mean(values, axis=-1, keepdims=True)
    centred = values - mean
    var = jnp.mean(centred * centred, axis=-1, keepdims=True)
    return centred * lax.rsqrt(var + 1e-06) * gain.astype(jnp.float32) + bias.astype(jnp.float32)


def row(ref):
    return ref[...].reshape(1, ref.shape[0])


def ln1_kernel(x_ref, gain_ref, bias_ref, out_ref):
    values = x_ref[...].astype(jnp.float32)
    out_ref[...] = norm_rows(values, row(gain_ref), row(bias_ref)).astype(out_ref.dtype)


def first_norm(x, gain, bias):
    return pl.pallas_call(
        ln1_kernel,
        out_shape=jax.ShapeDtypeStruct(x.shape, jnp.bfloat16),
        in_specs=[whole()] * 3,
        out_specs=whole(),
        cost_estimate=pl.CostEstimate(flops=10 * x.size, bytes_accessed=4 * x.size, transcendentals=0),
        name="first_norm",
    )(x, gain, bias)


def spread(values, head, ones):
    rows = values.shape[0]
    gap = jnp.zeros((rows, LANES - head), values.dtype)
    lane = lax.broadcasted_iota(jnp.int32, (rows, LANES - head), 1)
    last = jnp.where(lane == 0, jnp.ones_like(gap), gap) if ones else gap
    q, k, v = (values[:, n * head : (n + 1) * head] for n in range(3))
    return jnp.concatenate([q, gap, k, gap, v, last], axis=1)


def place_kernel(head, where_ref, bias_ref, pair_ref, low_ref, high_ref, fa_ref, fb_ref, out_ref):
    slab = pair_ref.shape[1]
    pieces = (pair_ref.at[0], pair_ref.at[1], low_ref.at[0], low_ref.at[1],
              high_ref.at[0], high_ref.at[1], fa_ref, fb_ref)
    for i, ref in enumerate(pieces):
        first = pl.multiple_of(where_ref[i] * slab, 16)
        value = spread(ref[...].astype(jnp.float32), head, False)
        out_ref[pl.ds(first, slab), :] = value.astype(out_ref.dtype)
    bias = spread(row(bias_ref).astype(jnp.float32), head, True)
    out_ref[8 * slab :, :] = jnp.broadcast_to(bias, (16, bias.shape[1])).astype(out_ref.dtype)


def place(where, bias, pieces, head):
    slab = pieces[0].shape[1]
    return pl.pallas_call(
        functools.partial(place_kernel, head),
        out_shape=jax.ShapeDtypeStruct((8 * slab + 16, 3 * LANES), jnp.bfloat16),
        in_specs=[pl.BlockSpec(memory_space=pltpu.SMEM)] + [whole()] * 6,
        out_specs=whole(),
        cost_estimate=pl.CostEstimate(flops=1000000, bytes_accessed=3000000, transcendentals=0),
        name="place_rows",
    )(where, bias, *pieces)


def place_proj_kernel(where_ref, own_ref, one_ref, two_ref, three_ref, out_ref):
    for dz, ref in enumerate((own_ref, one_ref, two_ref, three_ref)):
        for j in range(2):
            out_ref[where_ref[2 * dz + j]] = ref[j]


def place_proj(where, pieces):
    return pl.pallas_call(
        place_proj_kernel,
        out_shape=jax.ShapeDtypeStruct((8, *pieces[0].shape[1:]), jnp.bfloat16),
        in_specs=[pl.BlockSpec(memory_space=pltpu.SMEM)] + [whole()] * 4,
        out_specs=whole(),
        cost_estimate=pl.CostEstimate(flops=100000, bytes_accessed=1000000, transcendentals=0),
        name="place_proj",
    )(where, *pieces)


def attend_kernel(head, x_ref, w_ref, out_ref, x_buf, q_ref, k_ref, v_ref, s_ref, sems):
    f32 = jnp.float32
    length, width = x_buf.shape
    chunks = sems.shape[0]
    chunk = length // chunks
    copies = []
    for n in range(chunks):
        rows = pl.ds(n * chunk, chunk)
        copy = pltpu.make_async_copy(x_ref.at[rows], x_buf.at[rows], sems.at[n])
        copy.start()
        copies.append(copy)
    bias = w_ref[width : width + 1, :].astype(f32)
    for n in range(chunks):
        copies[n].wait()
        rows = slice(n * chunk, (n + 1) * chunk)
        value = jnp.dot(x_buf[rows, :], w_ref[:width, :], preferred_element_type=f32) + bias
        value = value.astype(q_ref.dtype)
        q_ref[rows, :] = value[:, :LANES]
        k_ref[rows, :] = value[:, LANES : 2 * LANES]
        v_ref[rows, :] = value[:, 2 * LANES :]
    block = s_ref.shape[1]
    steps = length // block
    scale = 1.4426950408889634 / head**0.5

    def scores(i):
        q = q_ref[pl.ds(pl.multiple_of(i * block, block), block), :]
        s_ref[i % 2] = lax.dot_general(
            q, k_ref[...], (((1,), (1,)), ((), ())), preferred_element_type=f32
        )

    scores(0)

    def step(i, carry):
        value = s_ref[i % 2]
        scores(jnp.minimum(i + 1, steps - 1))
        top = jnp.max(value, axis=-1, keepdims=True)
        expo = jnp.exp2((value - top) * scale).astype(jnp.bfloat16)
        mixed = jnp.dot(expo, v_ref[...], preferred_element_type=f32)
        out_ref[pl.ds(pl.multiple_of(i * block, block), block), :] = (
            mixed / mixed[:, head : head + 1]
        ).astype(out_ref.dtype)
        return carry

    lax.fori_loop(0, steps, step, 0)


def attend(rows, w_own, head):
    length, width = rows.shape
    block, bf16 = 256, jnp.bfloat16
    return pl.pallas_call(
        functools.partial(attend_kernel, head),
        out_shape=jax.ShapeDtypeStruct((length, LANES), bf16),
        in_specs=[pl.BlockSpec(memory_space=pl.ANY), whole()],
        out_specs=whole(),
        scratch_shapes=[pltpu.VMEM((length, width), bf16)]
        + [pltpu.VMEM((length, LANES), bf16)] * 3
        + [pltpu.VMEM((2, block, length), jnp.float32), pltpu.SemaphoreType.DMA((4,))],
        cost_estimate=pl.CostEstimate(
            flops=4 * length * length * LANES, bytes_accessed=8000000, transcendentals=length * length
        ),
        name="attend",
    )(rows, w_own)


def proj_kernel(where_ref, heads_ref, own_ref, side_ref, mine_ref, other_ref, h_ref, p_ref):
    own = mine_ref.shape[0]
    core = where_ref[8]
    head = own_ref.shape[1]
    for i in range(8):
        ref = own_ref if i < 4 else side_ref
        p_ref[i * LANES : i * LANES + head, :] = ref[i % 4]
        p_ref[i * LANES + head : (i + 1) * LANES, :] = jnp.zeros(
            (LANES - head, p_ref.shape[1]), p_ref.dtype
        )
        h_ref[:, i * LANES : (i + 1) * LANES] = heads_ref[where_ref[i]]
    for target, first in ((other_ref, (1 - core) * own), (mine_ref, core * own)):
        left = h_ref[pl.ds(pl.multiple_of(first, own), own), :]
        total = jnp.dot(left, p_ref[...], preferred_element_type=jnp.float32)
        target[...] = total.astype(target.dtype)


def project(where, heads, pieces, own, width):
    out = jax.ShapeDtypeStruct((own, width), jnp.bfloat16)
    return pl.pallas_call(
        proj_kernel,
        out_shape=(out, out),
        in_specs=[pl.BlockSpec(memory_space=pltpu.SMEM)] + [whole()] * 3,
        out_specs=(whole(), whole()),
        scratch_shapes=[
            pltpu.VMEM((2 * own, 8 * LANES), jnp.bfloat16),
            pltpu.VMEM((8 * LANES, width), jnp.bfloat16),
        ],
        cost_estimate=pl.CostEstimate(flops=740000000, bytes_accessed=4000000, transcendentals=0),
        name="project",
    )(where, heads, *pieces)


def ln2_kernel(x_ref, mine_ref, other_ref, pbias_ref, gain_ref, bias_ref, ln2_ref, resid_ref):
    f32 = jnp.float32
    total = mine_ref[...].astype(f32) + other_ref[...].astype(f32)
    resid = x_ref[...].astype(f32) + total + row(pbias_ref).astype(f32)
    resid_ref[...] = resid
    ln2_ref[...] = norm_rows(resid, row(gain_ref), row(bias_ref)).astype(ln2_ref.dtype)


def second_norm(x, mine, other, pbias, gain, bias):
    return pl.pallas_call(
        ln2_kernel,
        out_shape=(
            jax.ShapeDtypeStruct(x.shape, jnp.bfloat16),
            jax.ShapeDtypeStruct(x.shape, jnp.float32),
        ),
        in_specs=[whole()] * 6,
        out_specs=(whole(), whole()),
        cost_estimate=pl.CostEstimate(flops=12 * x.size, bytes_accessed=12 * x.size, transcendentals=0),
        name="second_norm",
    )(x, mine, other, pbias, gain, bias)


def pass_kernel(right_ref, via_a_ref, left_ref, via_b_ref, to_right_ref, to_left_ref):
    f32 = jnp.float32
    to_right_ref[...] = (right_ref[...] + via_a_ref[...].astype(f32)).astype(to_right_ref.dtype)
    to_left_ref[...] = (left_ref[...] + via_b_ref[...].astype(f32)).astype(to_left_ref.dtype)


def pass_on(right, via_a, left, via_b):
    out = jax.ShapeDtypeStruct(via_a.shape, via_a.dtype)
    return pl.pallas_call(
        pass_kernel,
        out_shape=(out, out),
        in_specs=[whole()] * 4,
        out_specs=(whole(), whole()),
        cost_estimate=pl.CostEstimate(flops=200000, bytes_accessed=1000000, transcendentals=0),
        name="pass_on",
    )(right, via_a, left, via_b)


def last_kernel(resid_ref, own_ref, la_ref, lb_ref, ra_ref, rb_ref, bias_ref, out_ref):
    f32 = jnp.float32
    half = la_ref.shape[0]
    bias = row(bias_ref).astype(f32)
    for rows, left, right in ((slice(0, half), la_ref, ra_ref), (slice(half, 2 * half), lb_ref, rb_ref)):
        total = own_ref[rows, :] + left[...].astype(f32) + right[...].astype(f32)
        out_ref[rows, :] = (resid_ref[rows, :] + total + bias).astype(out_ref.dtype)


def last_sum(resid, own, la, lb, ra, rb, bias):
    return pl.pallas_call(
        last_kernel,
        out_shape=jax.ShapeDtypeStruct(resid.shape, jnp.bfloat16),
        in_specs=[whole()] * 7,
        out_specs=whole(),
        cost_estimate=pl.CostEstimate(flops=1000000, bytes_accessed=3000000, transcendentals=0),
        name="last_sum",
    )(resid, own, la, lb, ra, rb, bias)


def gelu(x):
    return 0.5 * x * (1.0 + lax.erf(x * 0.7071067811865476))


def mlp_kernel(slab, own_ref, left_ref, right_ref, fa_ref, fb_ref, w_ref,
               pown_ref, pra_ref, prb_ref, pla_ref, plb_ref, pfa_ref, pfb_ref,
               rows, w1, w2, b1, hidden, sem1, sem2, sem3):
    f32 = jnp.float32
    own = own_ref.shape[0]
    hid = w_ref.shape[3]
    loads1 = [[], [], [], []]
    loads2 = []
    for b in range(4):
        cols = pl.ds(b * hid, hid)
        for r in range(8):
            copy = pltpu.make_async_copy(
                w_ref.at[r, b, pl.ds(0, slab)], w1.at[pl.ds(r * slab, slab), cols], sem1.at[b, r]
            )
            copy.start()
            loads1[b].append(copy)
        copy = pltpu.make_async_copy(w_ref.at[0, b, pl.ds(2 * slab, 16)], b1.at[b], sem3.at[b])
        copy.start()
        loads1[b].append(copy)
    for b in range(4):
        for r in range(8):
            copy = pltpu.make_async_copy(
                w_ref.at[r, b, pl.ds(slab, slab)],
                w2.at[pl.ds(r * slab, slab), pl.ds(b * hid, hid)],
                sem2.at[b, r],
            )
            copy.start()
            loads2.append(copy)
    rows[:own] = own_ref[...]
    rows[own : 2 * own] = left_ref[...]
    rows[2 * own : 3 * own] = right_ref[...]
    rows[3 * own : 3 * own + own // 2] = fa_ref[...]
    rows[3 * own + own // 2 :] = fb_ref[...]
    for b in range(4):
        for copy in loads1[b]:
            copy.wait()
        cols = slice(b * hid, (b + 1) * hid)
        for m in range(2):
            part = slice(2 * own * m, 2 * own * (m + 1))
            value = jnp.dot(rows[part], w1[:, cols], preferred_element_type=f32)
            value = value + b1[b, 0:1].astype(f32)
            hidden[part, cols] = gelu(value).astype(hidden.dtype)
    for copy in loads2:
        copy.wait()
    half = own // 2
    for i, refs in ((3, (pfa_ref, pfb_ref)), (2, (pra_ref, prb_ref)), (1, (pla_ref, plb_ref)), (0, (pown_ref,))):
        out = lax.dot_general(
            hidden[i * own : (i + 1) * own],
            w2[...],
            (((1,), (1,)), ((), ())),
            preferred_element_type=f32,
        )
        if len(refs) == 1:
            refs[0][...] = out.astype(refs[0].dtype)
        else:
            refs[0][...] = out[:half].astype(refs[0].dtype)
            refs[1][...] = out[half:].astype(refs[1].dtype)


def mlp_block(pieces, weights, slab):
    own, width = pieces[0].shape
    hid = weights.shape[3]
    f32, bf16 = jnp.float32, jnp.bfloat16
    return pl.pallas_call(
        functools.partial(mlp_kernel, slab),
        out_shape=(jax.ShapeDtypeStruct((own, width), f32),)
        + tuple(jax.ShapeDtypeStruct((own // 2, width), t) for t in (f32, bf16, bf16, f32, bf16, bf16)),
        in_specs=[whole()] * 5 + [pl.BlockSpec(memory_space=pl.ANY)],
        out_specs=(whole(),) * 7,
        scratch_shapes=[
            pltpu.VMEM((4 * own, width), bf16),
            pltpu.VMEM((width, 4 * hid), bf16),
            pltpu.VMEM((width, 4 * hid), bf16),
            pltpu.VMEM((4, 16, hid), bf16),
            pltpu.VMEM((4 * own, 4 * hid), bf16),
            pltpu.SemaphoreType.DMA((4, 8)),
            pltpu.SemaphoreType.DMA((4, 8)),
            pltpu.SemaphoreType.DMA((4,)),
        ],
        cost_estimate=pl.CostEstimate(flops=4430000000, bytes_accessed=12000000, transcendentals=800000),
        name="mlp_block",
    )(*pieces, weights)


def layer(
    tokens_in,
    ln1_gain,
    ln1_bias,
    qkv_weight,
    qkv_bias,
    proj_weight,
    proj_bias,
    ln2_gain,
    ln2_bias,
    fc1_weight,
    fc1_bias,
    fc2_weight,
    fc2_bias,
):
    own = tokens_in.shape[0]
    width = tokens_in.shape[1]
    head = proj_weight.shape[0]
    slab = qkv_weight.shape[0]
    hid = fc1_weight.shape[1]
    core = lax.axis_index("core")
    z, yh = lax.axis_index("z"), lax.axis_index("yh")
    x, yl = lax.axis_index("x"), lax.axis_index("yl")

    half = own // 2

    pair = jnp.stack([qkv_weight, shift(qkv_weight, dyh=1)])
    low = shift(pair, dz=1)
    high = shift(pair, dz=3)
    zfa = shift(low[0], dz=1)
    zfb = shift(high[1], dz=3)
    rel = [(0, 0), (0, 1), (1, 0), (1, 1), (3, 0), (3, 1), (2, 0), (2, 1)]
    where = jnp.stack([(z + 4 - dz) % 4 * 2 + (yh + j) % 2 for dz, j in rel]).astype(jnp.int32)
    w_own = place(where, qkv_bias, (pair, low, high, zfa, zfb), head)

    p_rows = [proj_weight] + [shift(proj_weight, dx=dx) for dx in (1, 2, 3)]
    p_rows = jnp.stack(p_rows)
    p_rows = jnp.stack([p_rows, shift(p_rows, dyh=1)])
    p_rows = [p_rows] + [shift(p_rows, dz=dz) for dz in (1, 2, 3)]
    zs = jnp.stack([(z + 4 - dz) % 4 * 2 + (yh + j) % 2 for dz in range(4) for j in range(2)])
    proj_own = place_proj(zs.astype(jnp.int32), p_rows)
    proj_own = jnp.moveaxis(proj_own, 0, 2).reshape(4, head, width)

    ln1 = first_norm(tokens_in, ln1_gain, ln1_bias)
    ln1_full = lax.all_gather(ln1, COL, axis=0, tiled=True)

    bias_rows = jnp.broadcast_to(fc1_bias[None], (16, hid))
    stack = jnp.concatenate([fc1_weight, fc2_weight, bias_rows], axis=0)
    stack, ln1_full, w_own, proj_own = lax.optimization_barrier((stack, ln1_full, w_own, proj_own))
    mlp = lax.all_gather(stack, ("z", "yh", "yl", "core"), axis=0, tiled=False)
    mlp = mlp.reshape(8, 4, stack.shape[0], hid)

    proj_side = shift(proj_own, dyl=1)
    attn = attend(ln1_full, w_own, head)
    heads = lax.all_to_all(attn.reshape(8, 2 * own, LANES), ("x", "yl"), 0, 0, tiled=True)
    where = [(x + 4 - dx) % 4 * 2 + (yl + j) % 2 for j in range(2) for dx in range(4)]
    where = jnp.stack(where + [core]).astype(jnp.int32)
    mine, other = project(where, heads, (proj_own, proj_side), own, width)
    other = shift(other, dc=1)
    ln2, resid = second_norm(tokens_in, mine, other, proj_bias, ln2_gain, ln2_bias)

    left = shift(ln2, dx=1)
    right = shift(ln2, dx=3)
    far_a = shift(left[:half], dx=1)
    far_b = shift(right[half:], dx=3)
    o_own, ra, rb, la, lb, fa, fb = mlp_block((ln2, left, right, far_a, far_b), mlp, slab)

    via_a = shift(fa, dx=1)
    via_b = shift(fb, dx=3)
    from_left_b = shift(rb, dx=1)
    from_right_a = shift(la, dx=3)
    to_right, to_left = pass_on(ra, via_a, lb, via_b)
    from_left_a = shift(to_right, dx=1)
    from_right_b = shift(to_left, dx=3)
    return last_sum(resid, o_own, from_left_a, from_left_b, from_right_a, from_right_b, fc2_bias)


def solution(mesh):
    fine = Mesh(np.asarray(mesh.devices).reshape(SIZES), AXES)
    in_specs = (
        P(AXES, None),
        P(),
        P(),
        P(ROW, COL),
        P(COL),
        P(COL, ROW),
        P(),
        P(),
        P(),
        P(ROW, COL),
        P(COL),
        P(ROW, COL),
        P(),
    )
    return jax.shard_map(layer, mesh=fine, in_specs=in_specs, out_specs=P(AXES, None), check_vma=False)
```

```python
import functools
import itertools

import jax
import jax.numpy as jnp
import numpy as np
from jax import lax
from jax.experimental import pallas as pl
from jax.experimental.pallas import tpu as pltpu
from jax.sharding import Mesh
from jax.sharding import PartitionSpec as P


LANES = 128
AXES = ("z", "yh", "x", "yl", "core")
SIZES = (4, 2, 4, 2, 2)
ROW = ("z", "yh")
COL = ("x", "yl", "core")


def shift(value, dz=0, dyh=0, dx=0, dyl=0, dc=0):
    pairs = []
    for place in itertools.product(*[range(n) for n in SIZES]):
        target = [(p + d) % n for p, d, n in zip(place, (dz, dyh, dx, dyl, dc), SIZES)]
        pairs.append(
            (int(np.ravel_multi_index(place, SIZES)), int(np.ravel_multi_index(target, SIZES)))
        )
    return lax.ppermute(value, AXES, pairs)


def whole():
    return pl.BlockSpec(memory_space=pltpu.VMEM)


def norm_rows(values, gain, bias):
    mean = jnp.mean(values, axis=-1, keepdims=True)
    centred = values - mean
    var = jnp.mean(centred * centred, axis=-1, keepdims=True)
    return centred * lax.rsqrt(var + 1e-06) * gain.astype(jnp.float32) + bias.astype(jnp.float32)


def row(ref):
    return ref[...].reshape(1, ref.shape[0])


def ln1_kernel(x_ref, gain_ref, bias_ref, out_ref):
    values = x_ref[...].astype(jnp.float32)
    out_ref[...] = norm_rows(values, row(gain_ref), row(bias_ref)).astype(out_ref.dtype)


def first_norm(x, gain, bias):
    return pl.pallas_call(
        ln1_kernel,
        out_shape=jax.ShapeDtypeStruct(x.shape, jnp.bfloat16),
        in_specs=[whole()] * 3,
        out_specs=whole(),
        cost_estimate=pl.CostEstimate(flops=10 * x.size, bytes_accessed=4 * x.size, transcendentals=0),
        name="first_norm",
    )(x, gain, bias)


def spread(values, head, ones):
    rows = values.shape[0]
    gap = jnp.zeros((rows, LANES - head), values.dtype)
    lane = lax.broadcasted_iota(jnp.int32, (rows, LANES - head), 1)
    last = jnp.where(lane == 0, jnp.ones_like(gap), gap) if ones else gap
    q, k, v = (values[:, n * head : (n + 1) * head] for n in range(3))
    return jnp.concatenate([q, gap, k, gap, v, last], axis=1)


def place_kernel(slab, head, where_ref, bias_ref, own_ref, one_ref, two_ref, three_ref, w_ref, proj_ref):
    for dz, ref in enumerate((own_ref, one_ref, two_ref, three_ref)):
        for j in range(2):
            at = where_ref[2 * dz + j]
            first = pl.multiple_of(at * slab, 16)
            value = spread(ref[j, :slab].astype(jnp.float32), head, False)
            w_ref[pl.ds(first, slab), :] = value.astype(w_ref.dtype)
            proj_ref[at] = ref[j, slab:, :slab]
    bias = spread(row(bias_ref).astype(jnp.float32), head, True)
    w_ref[8 * slab :, :] = jnp.broadcast_to(bias, (16, bias.shape[1])).astype(w_ref.dtype)


def place(where, bias, pieces, slab, head):
    return pl.pallas_call(
        functools.partial(place_kernel, slab, head),
        out_shape=(
            jax.ShapeDtypeStruct((8 * slab + 16, 3 * LANES), jnp.bfloat16),
            jax.ShapeDtypeStruct((8, head, slab), jnp.bfloat16),
        ),
        in_specs=[pl.BlockSpec(memory_space=pltpu.SMEM)] + [whole()] * 5,
        out_specs=(whole(), whole()),
        cost_estimate=pl.CostEstimate(flops=1000000, bytes_accessed=3000000, transcendentals=0),
        name="place_rows",
    )(where, bias, *pieces)


def attend_kernel(head, x_ref, w_ref, out_ref, x_buf, q_ref, k_ref, v_ref, s_ref, sems):
    f32 = jnp.float32
    length, width = x_buf.shape
    chunks = sems.shape[0]
    chunk = length // chunks
    copies = []
    for n in range(chunks):
        rows = pl.ds(n * chunk, chunk)
        copies.append(pltpu.make_async_copy(x_ref.at[rows], x_buf.at[rows], sems.at[n]))
    ahead = 2
    for copy in copies[:ahead]:
        copy.start()
    bias = w_ref[width : width + 1, :].astype(f32)
    for n in range(chunks):
        copies[n].wait()
        if n + ahead < chunks:
            copies[n + ahead].start()
        rows = slice(n * chunk, (n + 1) * chunk)
        value = jnp.dot(x_buf[rows, :], w_ref[:width, :], preferred_element_type=f32) + bias
        value = value.astype(q_ref.dtype)
        q_ref[rows, :] = value[:, :LANES]
        k_ref[rows, :] = value[:, LANES : 2 * LANES]
        v_ref[rows, :] = value[:, 2 * LANES :]
    block = s_ref.shape[1]
    steps = length // block
    scale = 1.4426950408889634 / head**0.5

    def scores(i):
        q = q_ref[pl.ds(pl.multiple_of(i * block, block), block), :]
        s_ref[i % 2] = lax.dot_general(
            q, k_ref[...], (((1,), (1,)), ((), ())), preferred_element_type=f32
        )

    scores(0)

    def step(i, carry):
        value = s_ref[i % 2]
        scores(jnp.minimum(i + 1, steps - 1))
        top = jnp.max(value, axis=-1, keepdims=True)
        expo = jnp.exp2((value - top) * scale).astype(jnp.bfloat16)
        mixed = jnp.dot(expo, v_ref[...], preferred_element_type=f32)
        out_ref[pl.ds(pl.multiple_of(i * block, block), block), :] = (
            mixed / mixed[:, head : head + 1]
        ).astype(out_ref.dtype)
        return carry

    lax.fori_loop(0, steps, step, 0, unroll=True)


def attend(rows, w_own, head):
    length, width = rows.shape
    block, bf16 = 256, jnp.bfloat16
    return pl.pallas_call(
        functools.partial(attend_kernel, head),
        out_shape=jax.ShapeDtypeStruct((length, LANES), bf16),
        in_specs=[pl.BlockSpec(memory_space=pl.ANY), whole()],
        out_specs=whole(),
        scratch_shapes=[pltpu.VMEM((length, width), bf16)]
        + [pltpu.VMEM((length, LANES), bf16)] * 3
        + [pltpu.VMEM((2, block, length), jnp.float32), pltpu.SemaphoreType.DMA((4,))],
        cost_estimate=pl.CostEstimate(
            flops=4 * length * length * LANES, bytes_accessed=8000000, transcendentals=length * length
        ),
        name="attend",
    )(rows, w_own)


def proj_kernel(where_ref, heads_ref, own_ref, one_ref, two_ref, three_ref, mine_ref, other_ref, h_ref, p_ref):
    own = mine_ref.shape[0]
    core = where_ref[8]
    head = own_ref.shape[1]
    for i in range(8):
        ref = (own_ref, one_ref, two_ref, three_ref)[i // 2]
        p_ref[i * LANES : i * LANES + head, :] = ref[i % 2]
        p_ref[i * LANES + head : (i + 1) * LANES, :] = jnp.zeros(
            (LANES - head, p_ref.shape[1]), p_ref.dtype
        )
        h_ref[:, i * LANES : (i + 1) * LANES] = heads_ref[where_ref[i]]
    for target, first in ((other_ref, (1 - core) * own), (mine_ref, core * own)):
        left = h_ref[pl.ds(pl.multiple_of(first, own), own), :]
        total = jnp.dot(left, p_ref[...], preferred_element_type=jnp.float32)
        target[...] = total.astype(target.dtype)


def project(where, heads, pieces, own, width):
    out = jax.ShapeDtypeStruct((own, width), jnp.bfloat16)
    return pl.pallas_call(
        proj_kernel,
        out_shape=(out, out),
        in_specs=[pl.BlockSpec(memory_space=pltpu.SMEM)] + [whole()] * 5,
        out_specs=(whole(), whole()),
        scratch_shapes=[
            pltpu.VMEM((2 * own, 8 * LANES), jnp.bfloat16),
            pltpu.VMEM((8 * LANES, width), jnp.bfloat16),
        ],
        cost_estimate=pl.CostEstimate(flops=740000000, bytes_accessed=4000000, transcendentals=0),
        name="project",
    )(where, heads, *pieces)


def ln2_kernel(x_ref, mine_ref, other_ref, pbias_ref, gain_ref, bias_ref, ln2_ref, resid_ref):
    f32 = jnp.float32
    total = mine_ref[...].astype(f32) + other_ref[...].astype(f32)
    resid = x_ref[...].astype(f32) + total + row(pbias_ref).astype(f32)
    resid_ref[...] = resid
    ln2_ref[...] = norm_rows(resid, row(gain_ref), row(bias_ref)).astype(ln2_ref.dtype)


def second_norm(x, mine, other, pbias, gain, bias):
    return pl.pallas_call(
        ln2_kernel,
        out_shape=(
            jax.ShapeDtypeStruct(x.shape, jnp.bfloat16),
            jax.ShapeDtypeStruct(x.shape, jnp.float32),
        ),
        in_specs=[whole()] * 6,
        out_specs=(whole(), whole()),
        cost_estimate=pl.CostEstimate(flops=12 * x.size, bytes_accessed=12 * x.size, transcendentals=0),
        name="second_norm",
    )(x, mine, other, pbias, gain, bias)


def pass_kernel(right_ref, via_a_ref, left_ref, via_b_ref, to_right_ref, to_left_ref):
    f32 = jnp.float32
    to_right_ref[...] = (right_ref[...] + via_a_ref[...].astype(f32)).astype(to_right_ref.dtype)
    to_left_ref[...] = (left_ref[...] + via_b_ref[...].astype(f32)).astype(to_left_ref.dtype)


def pass_on(right, via_a, left, via_b):
    out = jax.ShapeDtypeStruct(via_a.shape, via_a.dtype)
    return pl.pallas_call(
        pass_kernel,
        out_shape=(out, out),
        in_specs=[whole()] * 4,
        out_specs=(whole(), whole()),
        cost_estimate=pl.CostEstimate(flops=200000, bytes_accessed=1000000, transcendentals=0),
        name="pass_on",
    )(right, via_a, left, via_b)


def last_kernel(resid_ref, own_ref, la_ref, lb_ref, ra_ref, rb_ref, bias_ref, out_ref):
    f32 = jnp.float32
    half = la_ref.shape[0]
    bias = row(bias_ref).astype(f32)
    for rows, left, right in ((slice(0, half), la_ref, ra_ref), (slice(half, 2 * half), lb_ref, rb_ref)):
        total = own_ref[rows, :] + left[...].astype(f32) + right[...].astype(f32)
        out_ref[rows, :] = (resid_ref[rows, :] + total + bias).astype(out_ref.dtype)


def last_sum(resid, own, la, lb, ra, rb, bias):
    return pl.pallas_call(
        last_kernel,
        out_shape=jax.ShapeDtypeStruct(resid.shape, jnp.bfloat16),
        in_specs=[whole()] * 7,
        out_specs=whole(),
        cost_estimate=pl.CostEstimate(flops=1000000, bytes_accessed=3000000, transcendentals=0),
        name="last_sum",
    )(resid, own, la, lb, ra, rb, bias)


def gelu(x):
    return 0.5 * x * (1.0 + lax.erf(x * 0.7071067811865476))


def mlp_kernel(slab, own_ref, left_ref, right_ref, fa_ref, fb_ref, w_ref,
               pown_ref, pra_ref, prb_ref, pla_ref, plb_ref, pfa_ref, pfb_ref,
               rows, w1, w2, b1, hidden, sem1, sem2, sem3):
    f32 = jnp.float32
    own = own_ref.shape[0]
    hid = w_ref.shape[3]
    loads1 = [[], [], [], []]
    loads2 = [[], [], [], []]
    for b in range(4):
        cols = pl.ds(b * hid, hid)
        for r in range(8):
            rows_r = pl.ds(r * slab, slab)
            loads1[b].append(
                pltpu.make_async_copy(w_ref.at[r, b, pl.ds(0, slab)], w1.at[rows_r, cols], sem1.at[b, r])
            )
            loads2[b].append(
                pltpu.make_async_copy(w_ref.at[r, b, pl.ds(slab, slab)], w2.at[rows_r, cols], sem2.at[b, r])
            )
        loads1[b].append(
            pltpu.make_async_copy(w_ref.at[0, b, pl.ds(2 * slab, 16)], b1.at[b], sem3.at[b])
        )
    queue = loads1 + loads2
    for group in queue[:2]:
        for copy in group:
            copy.start()
    rows[:own] = own_ref[...]
    rows[own : 2 * own] = left_ref[...]
    rows[2 * own : 3 * own] = right_ref[...]
    rows[3 * own : 3 * own + own // 2] = fa_ref[...]
    rows[3 * own + own // 2 :] = fb_ref[...]
    for b in range(4):
        for copy in loads1[b]:
            copy.wait()
        for group in queue[b + 2 : b + 3] if b < 3 else queue[5:]:
            for copy in group:
                copy.start()
        cols = slice(b * hid, (b + 1) * hid)
        for m in range(2):
            part = slice(2 * own * m, 2 * own * (m + 1))
            value = jnp.dot(rows[part], w1[:, cols], preferred_element_type=f32)
            value = value + b1[b, 0:1].astype(f32)
            hidden[part, cols] = gelu(value).astype(hidden.dtype)
    for group in loads2:
        for copy in group:
            copy.wait()
    half = own // 2
    out = lax.dot_general(hidden[...], w2[...], (((1,), (1,)), ((), ())), preferred_element_type=f32)
    for i, refs in ((3, (pfa_ref, pfb_ref)), (2, (pra_ref, prb_ref)), (1, (pla_ref, plb_ref)), (0, (pown_ref,))):
        part = out[i * own : (i + 1) * own]
        if len(refs) == 1:
            refs[0][...] = part.astype(refs[0].dtype)
        else:
            refs[0][...] = part[:half].astype(refs[0].dtype)
            refs[1][...] = part[half:].astype(refs[1].dtype)


def mlp_block(pieces, weights, slab):
    own, width = pieces[0].shape
    hid = weights.shape[3]
    f32, bf16 = jnp.float32, jnp.bfloat16
    return pl.pallas_call(
        functools.partial(mlp_kernel, slab),
        out_shape=(jax.ShapeDtypeStruct((own, width), f32),)
        + tuple(jax.ShapeDtypeStruct((own // 2, width), t) for t in (f32, bf16, bf16, f32, bf16, bf16)),
        in_specs=[whole()] * 5 + [pl.BlockSpec(memory_space=pl.ANY)],
        out_specs=(whole(),) * 7,
        scratch_shapes=[
            pltpu.VMEM((4 * own, width), bf16),
            pltpu.VMEM((width, 4 * hid), bf16),
            pltpu.VMEM((width, 4 * hid), bf16),
            pltpu.VMEM((4, 16, hid), bf16),
            pltpu.VMEM((4 * own, 4 * hid), bf16),
            pltpu.SemaphoreType.DMA((4, 8)),
            pltpu.SemaphoreType.DMA((4, 8)),
            pltpu.SemaphoreType.DMA((4,)),
        ],
        cost_estimate=pl.CostEstimate(flops=4430000000, bytes_accessed=12000000, transcendentals=800000),
        name="mlp_block",
    )(*pieces, weights)


def layer(
    tokens_in,
    ln1_gain,
    ln1_bias,
    qkv_weight,
    qkv_bias,
    proj_weight,
    proj_bias,
    ln2_gain,
    ln2_bias,
    fc1_weight,
    fc1_bias,
    fc2_weight,
    fc2_bias,
):
    own = tokens_in.shape[0]
    width = tokens_in.shape[1]
    head = proj_weight.shape[0]
    slab = qkv_weight.shape[0]
    hid = fc1_weight.shape[1]
    core = lax.axis_index("core")
    z, yh = lax.axis_index("z"), lax.axis_index("yh")
    x, yl = lax.axis_index("x"), lax.axis_index("yl")

    half = own // 2

    wide = jnp.pad(proj_weight, ((0, 0), (0, qkv_weight.shape[1] - slab)))
    rowset = jnp.concatenate([qkv_weight, wide], axis=0)
    pair = jnp.stack([rowset, shift(rowset, dyh=1)])
    pieces = [pair] + [shift(pair, dz=dz) for dz in (1, 2, 3)]
    where = jnp.stack([(z + 4 - dz) % 4 * 2 + (yh + j) % 2 for dz in range(4) for j in range(2)])
    w_own, proj_own = place(where.astype(jnp.int32), qkv_bias, pieces, slab, head)
    proj_own = jnp.moveaxis(proj_own, 0, 1).reshape(head, width)
    proj_pair = jnp.stack([proj_own, shift(proj_own, dyl=1)])

    ln1 = first_norm(tokens_in, ln1_gain, ln1_bias)
    ln1_full = lax.all_gather(ln1, COL, axis=0, tiled=True)

    bias_rows = jnp.broadcast_to(fc1_bias[None], (16, hid))
    stack = jnp.concatenate([fc1_weight, fc2_weight, bias_rows], axis=0)
    stack, ln1_full, w_own, proj_pair = lax.optimization_barrier((stack, ln1_full, w_own, proj_pair))
    mlp = lax.all_gather(stack, ("z", "yh", "yl", "core"), axis=0, tiled=False)
    mlp = mlp.reshape(8, 4, stack.shape[0], hid)

    proj_sets = [proj_pair] + [shift(proj_pair, dx=dx) for dx in (1, 2, 3)]
    attn = attend(ln1_full, w_own, head)
    heads = lax.all_to_all(attn.reshape(8, 2 * own, LANES), ("x", "yl"), 0, 0, tiled=True)
    where = [(x + 4 - dx) % 4 * 2 + (yl + j) % 2 for dx in range(4) for j in range(2)]
    where = jnp.stack(where + [core]).astype(jnp.int32)
    mine, other = project(where, heads, proj_sets, own, width)
    other = shift(other, dc=1)
    ln2, resid = second_norm(tokens_in, mine, other, proj_bias, ln2_gain, ln2_bias)

    left = shift(ln2, dx=1)
    right = shift(ln2, dx=3)
    far_a = shift(left[:half], dx=1)
    far_b = shift(right[half:], dx=3)
    o_own, ra, rb, la, lb, fa, fb = mlp_block((ln2, left, right, far_a, far_b), mlp, slab)

    via_a = shift(fa, dx=1)
    via_b = shift(fb, dx=3)
    from_left_b = shift(rb, dx=1)
    from_right_a = shift(la, dx=3)
    to_right, to_left = pass_on(ra, via_a, lb, via_b)
    from_left_a = shift(to_right, dx=1)
    from_right_b = shift(to_left, dx=3)
    return last_sum(resid, o_own, from_left_a, from_left_b, from_right_a, from_right_b, fc2_bias)


def solution(mesh):
    fine = Mesh(np.asarray(mesh.devices).reshape(SIZES), AXES)
    in_specs = (
        P(AXES, None),
        P(),
        P(),
        P(ROW, COL),
        P(COL),
        P(COL, ROW),
        P(),
        P(),
        P(),
        P(ROW, COL),
        P(COL),
        P(ROW, COL),
        P(),
    )
    return jax.shard_map(layer, mesh=fine, in_specs=in_specs, out_specs=P(AXES, None), check_vma=False)
```

```python
import functools
import itertools

import jax
import jax.numpy as jnp
import numpy as np
from jax import lax
from jax.experimental import pallas as pl
from jax.experimental.pallas import tpu as pltpu
from jax.sharding import Mesh
from jax.sharding import PartitionSpec as P


LANES = 128
AXES = ("z", "yh", "x", "yl", "core")
SIZES = (4, 2, 4, 2, 2)
ROW = ("z", "yh")
COL = ("x", "yl", "core")


def shift(value, dz=0, dyh=0, dx=0, dyl=0, dc=0):
    pairs = []
    for place in itertools.product(*[range(n) for n in SIZES]):
        target = [(p + d) % n for p, d, n in zip(place, (dz, dyh, dx, dyl, dc), SIZES)]
        pairs.append(
            (int(np.ravel_multi_index(place, SIZES)), int(np.ravel_multi_index(target, SIZES)))
        )
    return lax.ppermute(value, AXES, pairs)


def whole():
    return pl.BlockSpec(memory_space=pltpu.VMEM)


def norm_rows(values, gain, bias):
    mean = jnp.mean(values, axis=-1, keepdims=True)
    centred = values - mean
    var = jnp.mean(centred * centred, axis=-1, keepdims=True)
    return centred * lax.rsqrt(var + 1e-06) * gain.astype(jnp.float32) + bias.astype(jnp.float32)


def row(ref):
    return ref[...].reshape(1, ref.shape[0])


def ln1_kernel(x_ref, gain_ref, bias_ref, out_ref):
    values = x_ref[...].astype(jnp.float32)
    out_ref[...] = norm_rows(values, row(gain_ref), row(bias_ref)).astype(out_ref.dtype)


def first_norm(x, gain, bias):
    return pl.pallas_call(
        ln1_kernel,
        out_shape=jax.ShapeDtypeStruct(x.shape, jnp.bfloat16),
        in_specs=[whole()] * 3,
        out_specs=whole(),
        cost_estimate=pl.CostEstimate(flops=10 * x.size, bytes_accessed=4 * x.size, transcendentals=0),
        compiler_params=pltpu.CompilerParams(vmem_limit_bytes=8 << 20),
        name="first_norm",
    )(x, gain, bias)


def spread(values, head, ones):
    rows = values.shape[0]
    gap = jnp.zeros((rows, LANES - head), values.dtype)
    lane = lax.broadcasted_iota(jnp.int32, (rows, LANES - head), 1)
    last = jnp.where(lane == 0, jnp.ones_like(gap), gap) if ones else gap
    q, k, v = (values[:, n * head : (n + 1) * head] for n in range(3))
    return jnp.concatenate([q, gap, k, gap, v, last], axis=1)


def place_kernel(slab, head, where_ref, bias_ref, own_ref, one_ref, two_ref, three_ref, w_ref, proj_ref):
    for dz, ref in enumerate((own_ref, one_ref, two_ref, three_ref)):
        for j in range(2):
            at = where_ref[2 * dz + j]
            first = pl.multiple_of(at * slab, 16)
            value = spread(ref[j, :slab].astype(jnp.float32), head, False)
            w_ref[pl.ds(first, slab), :] = value.astype(w_ref.dtype)
            proj_ref[at] = ref[j, slab:, :slab]
    bias = spread(row(bias_ref).astype(jnp.float32), head, True)
    w_ref[8 * slab :, :] = jnp.broadcast_to(bias, (16, bias.shape[1])).astype(w_ref.dtype)


def place(where, bias, pieces, slab, head):
    return pl.pallas_call(
        functools.partial(place_kernel, slab, head),
        out_shape=(
            jax.ShapeDtypeStruct((8 * slab + 16, 3 * LANES), jnp.bfloat16),
            jax.ShapeDtypeStruct((8, head, slab), jnp.bfloat16),
        ),
        in_specs=[pl.BlockSpec(memory_space=pltpu.SMEM)] + [whole()] * 5,
        out_specs=(whole(), whole()),
        cost_estimate=pl.CostEstimate(flops=1000000, bytes_accessed=3000000, transcendentals=0),
        compiler_params=pltpu.CompilerParams(vmem_limit_bytes=16 << 20),
        name="place_rows",
    )(where, bias, *pieces)


def attend_kernel(head, x_ref, w_ref, out_ref, x_buf, q_ref, k_ref, v_ref, s_ref, sems):
    f32 = jnp.float32
    length, width = x_buf.shape
    chunks = sems.shape[0]
    chunk = length // chunks
    copies = []
    for n in range(chunks):
        rows = pl.ds(n * chunk, chunk)
        copies.append(pltpu.make_async_copy(x_ref.at[rows], x_buf.at[rows], sems.at[n]))
    ahead = 2
    for copy in copies[:ahead]:
        copy.start()
    bias = w_ref[width : width + 1, :].astype(f32)
    for n in range(chunks):
        copies[n].wait()
        if n + ahead < chunks:
            copies[n + ahead].start()
        rows = slice(n * chunk, (n + 1) * chunk)
        value = jnp.dot(x_buf[rows, :], w_ref[:width, :], preferred_element_type=f32) + bias
        value = value.astype(q_ref.dtype)
        q_ref[rows, :] = value[:, :LANES]
        k_ref[rows, :] = value[:, LANES : 2 * LANES]
        v_ref[rows, :] = value[:, 2 * LANES :]
    block = s_ref.shape[1]
    steps = length // block
    scale = 1.4426950408889634 / head**0.5

    def scores(i):
        q = q_ref[pl.ds(pl.multiple_of(i * block, block), block), :]
        s_ref[i % 2] = lax.dot_general(
            q, k_ref[...], (((1,), (1,)), ((), ())), preferred_element_type=f32
        )

    scores(0)

    def step(i, carry):
        value = s_ref[i % 2]
        scores(jnp.minimum(i + 1, steps - 1))
        top = jnp.max(value, axis=-1, keepdims=True)
        expo = jnp.exp2((value - top) * scale).astype(jnp.bfloat16)
        mixed = jnp.dot(expo, v_ref[...], preferred_element_type=f32)
        out_ref[pl.ds(pl.multiple_of(i * block, block), block), :] = (
            mixed / mixed[:, head : head + 1]
        ).astype(out_ref.dtype)
        return carry

    lax.fori_loop(0, steps, step, 0, unroll=True)


def attend(rows, w_own, head):
    length, width = rows.shape
    block, bf16 = 256, jnp.bfloat16
    return pl.pallas_call(
        functools.partial(attend_kernel, head),
        out_shape=jax.ShapeDtypeStruct((length, LANES), bf16),
        in_specs=[pl.BlockSpec(memory_space=pltpu.HBM), whole()],
        out_specs=whole(),
        scratch_shapes=[pltpu.VMEM((length, width), bf16)]
        + [pltpu.VMEM((length, LANES), bf16)] * 3
        + [pltpu.VMEM((2, block, length), jnp.float32), pltpu.SemaphoreType.DMA((4,))],
        cost_estimate=pl.CostEstimate(
            flops=4 * length * length * LANES, bytes_accessed=8000000, transcendentals=length * length
        ),
        compiler_params=pltpu.CompilerParams(vmem_limit_bytes=59 << 20),
        name="attend",
    )(rows, w_own)


def proj_kernel(where_ref, heads_ref, own_ref, one_ref, two_ref, three_ref, mine_ref, other_ref, h_ref, p_ref):
    own = mine_ref.shape[0]
    core = where_ref[8]
    head = own_ref.shape[1]
    for i in range(8):
        ref = (own_ref, one_ref, two_ref, three_ref)[i // 2]
        p_ref[i * LANES : i * LANES + head, :] = ref[i % 2]
        p_ref[i * LANES + head : (i + 1) * LANES, :] = jnp.zeros(
            (LANES - head, p_ref.shape[1]), p_ref.dtype
        )
        h_ref[:, i * LANES : (i + 1) * LANES] = heads_ref[where_ref[i]]
    for target, first in ((other_ref, (1 - core) * own), (mine_ref, core * own)):
        left = h_ref[pl.ds(pl.multiple_of(first, own), own), :]
        total = jnp.dot(left, p_ref[...], preferred_element_type=jnp.float32)
        target[...] = total.astype(target.dtype)


def project(where, heads, pieces, own, width):
    out = jax.ShapeDtypeStruct((own, width), jnp.bfloat16)
    return pl.pallas_call(
        proj_kernel,
        out_shape=(out, out),
        in_specs=[pl.BlockSpec(memory_space=pltpu.SMEM)] + [whole()] * 5,
        out_specs=(whole(), whole()),
        scratch_shapes=[
            pltpu.VMEM((2 * own, 8 * LANES), jnp.bfloat16),
            pltpu.VMEM((8 * LANES, width), jnp.bfloat16),
        ],
        cost_estimate=pl.CostEstimate(flops=740000000, bytes_accessed=4000000, transcendentals=0),
        compiler_params=pltpu.CompilerParams(vmem_limit_bytes=24 << 20),
        name="project",
    )(where, heads, *pieces)


def ln2_kernel(x_ref, mine_ref, other_ref, pbias_ref, gain_ref, bias_ref, ln2_ref, resid_ref):
    f32 = jnp.float32
    total = mine_ref[...].astype(f32) + other_ref[...].astype(f32)
    resid = x_ref[...].astype(f32) + total + row(pbias_ref).astype(f32)
    resid_ref[...] = resid
    ln2_ref[...] = norm_rows(resid, row(gain_ref), row(bias_ref)).astype(ln2_ref.dtype)


def second_norm(x, mine, other, pbias, gain, bias):
    return pl.pallas_call(
        ln2_kernel,
        out_shape=(
            jax.ShapeDtypeStruct(x.shape, jnp.bfloat16),
            jax.ShapeDtypeStruct(x.shape, jnp.float32),
        ),
        in_specs=[whole()] * 6,
        out_specs=(whole(), whole()),
        cost_estimate=pl.CostEstimate(flops=12 * x.size, bytes_accessed=12 * x.size, transcendentals=0),
        compiler_params=pltpu.CompilerParams(vmem_limit_bytes=8 << 20),
        name="second_norm",
    )(x, mine, other, pbias, gain, bias)


def pass_kernel(right_ref, via_a_ref, left_ref, via_b_ref, to_right_ref, to_left_ref):
    f32 = jnp.float32
    half = via_a_ref.shape[0]
    near, far = slice(0, half), slice(half, 2 * half)
    to_right_ref[near, :] = (right_ref[near, :] + via_a_ref[...].astype(f32)).astype(to_right_ref.dtype)
    to_right_ref[far, :] = right_ref[far, :].astype(to_right_ref.dtype)
    to_left_ref[near, :] = left_ref[near, :].astype(to_left_ref.dtype)
    to_left_ref[far, :] = (left_ref[far, :] + via_b_ref[...].astype(f32)).astype(to_left_ref.dtype)


def pass_on(right, via_a, left, via_b):
    out = jax.ShapeDtypeStruct(right.shape, via_a.dtype)
    return pl.pallas_call(
        pass_kernel,
        out_shape=(out, out),
        in_specs=[whole()] * 4,
        out_specs=(whole(), whole()),
        cost_estimate=pl.CostEstimate(flops=200000, bytes_accessed=1000000, transcendentals=0),
        compiler_params=pltpu.CompilerParams(vmem_limit_bytes=8 << 20),
        name="pass_on",
    )(right, via_a, left, via_b)


def gelu(x):
    return 0.5 * x * (1.0 + lax.erf(x * 0.7071067811865476))


def second_product(hidden, w2):
    return lax.dot_general(hidden, w2, (((1,), (1,)), ((), ())), preferred_element_type=jnp.float32)


def head_kernel(slab, own_ref, left_ref, right_ref, fa_ref, fb_ref, w_ref,
                hidden, w2, pfa_ref, pfb_ref, rows, w1, b1, sem1, sem2, sem3):
    f32 = jnp.float32
    own = own_ref.shape[0]
    hid = w_ref.shape[3]
    loads1 = [[], [], [], []]
    loads2 = [[], [], [], []]
    for b in range(4):
        cols = pl.ds(b * hid, hid)
        for r in range(8):
            rows_r = pl.ds(r * slab, slab)
            loads1[b].append(
                pltpu.make_async_copy(w_ref.at[r, b, pl.ds(0, slab)], w1.at[rows_r, cols], sem1.at[b, r])
            )
            loads2[b].append(
                pltpu.make_async_copy(w_ref.at[r, b, pl.ds(slab, slab)], w2.at[rows_r, cols], sem2.at[b, r])
            )
        loads1[b].append(
            pltpu.make_async_copy(w_ref.at[0, b, pl.ds(2 * slab, 16)], b1.at[b], sem3.at[b])
        )
    queue = loads1 + loads2
    for group in queue[:2]:
        for copy in group:
            copy.start()
    rows[:own] = own_ref[...]
    rows[own : 2 * own] = left_ref[...]
    rows[2 * own : 3 * own] = right_ref[...]
    rows[3 * own : 3 * own + own // 2] = fa_ref[...]
    rows[3 * own + own // 2 :] = fb_ref[...]
    for b in range(4):
        for copy in loads1[b]:
            copy.wait()
        for group in queue[b + 2 : b + 3] if b < 3 else queue[5:]:
            for copy in group:
                copy.start()
        cols = slice(b * hid, (b + 1) * hid)
        for m in range(2):
            part = slice(2 * own * m, 2 * own * (m + 1))
            value = jnp.dot(rows[part], w1[:, cols], preferred_element_type=f32)
            value = value + b1[b, 0:1].astype(f32)
            hidden[part, cols] = gelu(value).astype(hidden.dtype)
    for group in loads2:
        for copy in group:
            copy.wait()
    half = own // 2
    out = second_product(hidden[3 * own :], w2[...])
    pfa_ref[...] = out[:half].astype(pfa_ref.dtype)
    pfb_ref[...] = out[half:].astype(pfb_ref.dtype)


def mlp_head(pieces, weights, slab):
    own, width = pieces[0].shape
    hid = weights.shape[3]
    bf16 = jnp.bfloat16
    far = jax.ShapeDtypeStruct((own // 2, width), bf16)
    return pl.pallas_call(
        functools.partial(head_kernel, slab),
        out_shape=(
            jax.ShapeDtypeStruct((4 * own, 4 * hid), bf16),
            jax.ShapeDtypeStruct((width, 4 * hid), bf16),
            far,
            far,
        ),
        in_specs=[whole()] * 5 + [pl.BlockSpec(memory_space=pltpu.HBM)],
        out_specs=(whole(),) * 4,
        scratch_shapes=[
            pltpu.VMEM((4 * own, width), bf16),
            pltpu.VMEM((width, 4 * hid), bf16),
            pltpu.VMEM((4, 16, hid), bf16),
            pltpu.SemaphoreType.DMA((4, 8)),
            pltpu.SemaphoreType.DMA((4, 8)),
            pltpu.SemaphoreType.DMA((4,)),
        ],
        cost_estimate=pl.CostEstimate(flops=2770000000, bytes_accessed=12000000, transcendentals=800000),
        compiler_params=pltpu.CompilerParams(vmem_limit_bytes=46 << 20),
        name="mlp_head",
    )(*pieces, weights)


def sides_kernel(hidden, w2, left_ref, right_ref):
    own = left_ref.shape[0]
    out = second_product(hidden[own : 3 * own], w2[...])
    left_ref[...] = out[:own]
    right_ref[...] = out[own:]


def mlp_sides(hidden, w2):
    out = jax.ShapeDtypeStruct((hidden.shape[0] // 4, w2.shape[0]), jnp.float32)
    return pl.pallas_call(
        sides_kernel,
        out_shape=(out, out),
        in_specs=[whole()] * 2,
        out_specs=(whole(), whole()),
        cost_estimate=pl.CostEstimate(flops=1100000000, bytes_accessed=8000000, transcendentals=0),
        compiler_params=pltpu.CompilerParams(vmem_limit_bytes=24 << 20),
        name="mlp_sides",
    )(hidden, w2)


def own_kernel(hidden, w2, resid_ref, bias_ref, out_ref):
    own = out_ref.shape[0]
    out = second_product(hidden[:own], w2[...])
    out_ref[...] = resid_ref[...] + out + row(bias_ref).astype(jnp.float32)


def mlp_own(hidden, w2, resid, bias):
    return pl.pallas_call(
        own_kernel,
        out_shape=jax.ShapeDtypeStruct(resid.shape, jnp.float32),
        in_specs=[whole()] * 4,
        out_specs=whole(),
        cost_estimate=pl.CostEstimate(flops=550000000, bytes_accessed=8000000, transcendentals=0),
        compiler_params=pltpu.CompilerParams(vmem_limit_bytes=24 << 20),
        name="mlp_own",
    )(hidden, w2, resid, bias)


def layer(
    tokens_in,
    ln1_gain,
    ln1_bias,
    qkv_weight,
    qkv_bias,
    proj_weight,
    proj_bias,
    ln2_gain,
    ln2_bias,
    fc1_weight,
    fc1_bias,
    fc2_weight,
    fc2_bias,
):
    f32, bf16 = jnp.float32, jnp.bfloat16
    own = tokens_in.shape[0]
    width = tokens_in.shape[1]
    head = proj_weight.shape[0]
    slab = qkv_weight.shape[0]
    hid = fc1_weight.shape[1]
    core = lax.axis_index("core")
    z, yh = lax.axis_index("z"), lax.axis_index("yh")
    x, yl = lax.axis_index("x"), lax.axis_index("yl")

    half = own // 2

    wide = jnp.pad(proj_weight, ((0, 0), (0, qkv_weight.shape[1] - slab)))
    rowset = jnp.concatenate([qkv_weight, wide], axis=0)
    pair = jnp.stack([rowset, shift(rowset, dyh=1)])
    pieces = [pair] + [shift(pair, dz=dz) for dz in (1, 2, 3)]
    where = jnp.stack([(z + 4 - dz) % 4 * 2 + (yh + j) % 2 for dz in range(4) for j in range(2)])
    w_own, proj_own = place(where.astype(jnp.int32), qkv_bias, pieces, slab, head)
    proj_own = jnp.moveaxis(proj_own, 0, 1).reshape(head, width)
    proj_pair = jnp.stack([proj_own, shift(proj_own, dyl=1)])

    ln1 = first_norm(tokens_in, ln1_gain, ln1_bias)
    ln1_full = lax.all_gather(ln1, COL, axis=0, tiled=True)

    bias_rows = jnp.broadcast_to(fc1_bias[None], (16, hid))
    stack = jnp.concatenate([fc1_weight, fc2_weight, bias_rows], axis=0)
    stack, ln1_full, w_own, proj_pair = lax.optimization_barrier((stack, ln1_full, w_own, proj_pair))
    mlp = lax.all_gather(stack, ("z", "yh", "yl", "core"), axis=0, tiled=False)
    mlp = mlp.reshape(8, 4, stack.shape[0], hid)

    proj_sets = [proj_pair] + [shift(proj_pair, dx=dx) for dx in (1, 2, 3)]
    attn = attend(ln1_full, w_own, head)
    heads = lax.all_to_all(attn.reshape(8, 2 * own, LANES), ("x", "yl"), 0, 0, tiled=True)
    where = [(x + 4 - dx) % 4 * 2 + (yl + j) % 2 for dx in range(4) for j in range(2)]
    where = jnp.stack(where + [core]).astype(jnp.int32)
    mine, other = project(where, heads, proj_sets, own, width)
    other = shift(other, dc=1)
    ln2, resid = second_norm(tokens_in, mine, other, proj_bias, ln2_gain, ln2_bias)

    left = shift(ln2, dx=1)
    right = shift(ln2, dx=3)
    far_a = shift(left[:half], dx=1)
    far_b = shift(right[half:], dx=3)
    hidden, w2, fa, fb = mlp_head((ln2, left, right, far_a, far_b), mlp, slab)

    via_a = shift(fa, dx=1)
    via_b = shift(fb, dx=3)
    o_left, o_right = mlp_sides(hidden, w2)
    to_right, to_left = pass_on(o_right, via_a, o_left, via_b)
    from_left = shift(to_right, dx=1)
    from_right = shift(to_left, dx=3)
    mine = mlp_own(hidden, w2, resid, fc2_bias)
    return (mine + from_left.astype(f32) + from_right.astype(f32)).astype(bf16)


def solution(mesh):
    fine = Mesh(np.asarray(mesh.devices).reshape(SIZES), AXES)
    in_specs = (
        P(AXES, None),
        P(),
        P(),
        P(ROW, COL),
        P(COL),
        P(COL, ROW),
        P(),
        P(),
        P(),
        P(ROW, COL),
        P(COL),
        P(ROW, COL),
        P(),
    )
    return jax.shard_map(layer, mesh=fine, in_specs=in_specs, out_specs=P(AXES, None), check_vma=False)
```

```python
import functools
import itertools

import jax
import jax.numpy as jnp
import numpy as np
from jax import lax
from jax.experimental import pallas as pl
from jax.experimental.pallas import tpu as pltpu
from jax.sharding import Mesh
from jax.sharding import PartitionSpec as P


LANES = 128
AXES = ("z", "yh", "x", "yl", "core")
SIZES = (4, 2, 4, 2, 2)
ROW = ("z", "yh")
COL = ("x", "yl", "core")


def shift(value, dz=0, dyh=0, dx=0, dyl=0, dc=0):
    pairs = []
    for place in itertools.product(*[range(n) for n in SIZES]):
        target = [(p + d) % n for p, d, n in zip(place, (dz, dyh, dx, dyl, dc), SIZES)]
        pairs.append(
            (int(np.ravel_multi_index(place, SIZES)), int(np.ravel_multi_index(target, SIZES)))
        )
    return lax.ppermute(value, AXES, pairs)


def whole():
    return pl.BlockSpec(memory_space=pltpu.VMEM)


def norm_rows(values, gain, bias):
    mean = jnp.mean(values, axis=-1, keepdims=True)
    centred = values - mean
    var = jnp.mean(centred * centred, axis=-1, keepdims=True)
    return centred * lax.rsqrt(var + 1e-06) * gain.astype(jnp.float32) + bias.astype(jnp.float32)


def row(ref):
    return ref[...].reshape(1, ref.shape[0])


def ln1_kernel(x_ref, gain_ref, bias_ref, out_ref):
    values = x_ref[...].astype(jnp.float32)
    out_ref[...] = norm_rows(values, row(gain_ref), row(bias_ref)).astype(out_ref.dtype)


def first_norm(x, gain, bias):
    return pl.pallas_call(
        ln1_kernel,
        out_shape=jax.ShapeDtypeStruct(x.shape, jnp.bfloat16),
        in_specs=[whole()] * 3,
        out_specs=whole(),
        cost_estimate=pl.CostEstimate(flops=10 * x.size, bytes_accessed=4 * x.size, transcendentals=0),
        compiler_params=pltpu.CompilerParams(vmem_limit_bytes=8 << 20),
        name="first_norm",
    )(x, gain, bias)


def spread(values, head, ones):
    rows = values.shape[0]
    gap = jnp.zeros((rows, LANES - head), values.dtype)
    lane = lax.broadcasted_iota(jnp.int32, (rows, LANES - head), 1)
    last = jnp.where(lane == 0, jnp.ones_like(gap), gap) if ones else gap
    q, k, v = (values[:, n * head : (n + 1) * head] for n in range(3))
    return jnp.concatenate([q, gap, k, gap, v, last], axis=1)


def place_kernel(slab, head, where_ref, bias_ref, own_ref, one_ref, two_ref, three_ref, w_ref, proj_ref):
    for dz, ref in enumerate((own_ref, one_ref, two_ref, three_ref)):
        for j in range(2):
            at = where_ref[2 * dz + j]
            first = pl.multiple_of(at * slab, 16)
            value = spread(ref[j, :slab].astype(jnp.float32), head, False)
            w_ref[pl.ds(first, slab), :] = value.astype(w_ref.dtype)
            proj_ref[at] = ref[j, slab:, :slab]
    bias = spread(row(bias_ref).astype(jnp.float32), head, True)
    w_ref[8 * slab :, :] = jnp.broadcast_to(bias, (16, bias.shape[1])).astype(w_ref.dtype)


def place(where, bias, pieces, slab, head):
    return pl.pallas_call(
        functools.partial(place_kernel, slab, head),
        out_shape=(
            jax.ShapeDtypeStruct((8 * slab + 16, 3 * LANES), jnp.bfloat16),
            jax.ShapeDtypeStruct((8, head, slab), jnp.bfloat16),
        ),
        in_specs=[pl.BlockSpec(memory_space=pltpu.SMEM)] + [whole()] * 5,
        out_specs=(whole(), whole()),
        cost_estimate=pl.CostEstimate(flops=1000000, bytes_accessed=3000000, transcendentals=0),
        compiler_params=pltpu.CompilerParams(vmem_limit_bytes=16 << 20),
        name="place_rows",
    )(where, bias, *pieces)


def qkv_kernel(count, *refs):
    pieces, (w_own, w_other, out_own, out_other, rows) = refs[:count], refs[count:]
    width = rows.shape[1]
    first = 0
    for ref in pieces:
        rows[first : first + ref.shape[0], :] = ref[...]
        first += ref.shape[0]
    for w_ref, out_ref in ((w_other, out_other), (w_own, out_own)):
        bias = w_ref[width : width + 1, :].astype(jnp.float32)
        value = jnp.dot(rows[...], w_ref[:width, :], preferred_element_type=jnp.float32)
        out_ref[...] = (value + bias).astype(out_ref.dtype)


def qkv_part(pieces, w_own, w_other):
    rows = sum(p.shape[0] for p in pieces)
    cols = w_own.shape[1]
    out = jax.ShapeDtypeStruct((rows, cols), jnp.bfloat16)
    return pl.pallas_call(
        functools.partial(qkv_kernel, len(pieces)),
        out_shape=(out, out),
        in_specs=[whole()] * (len(pieces) + 2),
        out_specs=(whole(), whole()),
        scratch_shapes=[pltpu.VMEM((rows, pieces[0].shape[1]), jnp.bfloat16)],
        cost_estimate=pl.CostEstimate(
            flops=4 * rows * cols * w_own.shape[0], bytes_accessed=4000000, transcendentals=0
        ),
        compiler_params=pltpu.CompilerParams(vmem_limit_bytes=16 << 20),
        name="qkv_part",
    )(*pieces, w_own, w_other)


def attend_kernel(head, where_ref, *refs):
    f32 = jnp.float32
    parts, (out_ref, q_ref, k_ref, v_ref, s_ref) = refs[:4], refs[4:]
    length = q_ref.shape[0]
    first = 0
    for ref in parts:
        rows = slice(first, first + ref.shape[0])
        q_ref[rows, :] = ref[:, :LANES]
        k_ref[rows, :] = ref[:, LANES : 2 * LANES]
        v_ref[rows, :] = ref[:, 2 * LANES :]
        first += ref.shape[0]
    block = s_ref.shape[1]
    steps = length // block
    scale = 1.4426950408889634 / head**0.5

    def scores(i):
        s_ref[i % 2] = lax.dot_general(
            q_ref[i * block : (i + 1) * block, :],
            k_ref[...],
            (((1,), (1,)), ((), ())),
            preferred_element_type=f32,
        )

    scores(0)
    for i in range(steps):
        value = s_ref[i % 2]
        if i + 1 < steps:
            scores(i + 1)
        top = jnp.max(value, axis=-1, keepdims=True)
        expo = jnp.exp2((value - top) * scale).astype(jnp.bfloat16)
        mixed = jnp.dot(expo, v_ref[...], preferred_element_type=f32)
        mixed = (mixed / mixed[:, head : head + 1]).astype(out_ref.dtype)
        for n in range(block // LANES):
            out_ref[where_ref[i * (block // LANES) + n]] = mixed[n * LANES : (n + 1) * LANES]


def attend(where, parts, head):
    length = sum(p.shape[0] for p in parts)
    block, bf16 = 256, jnp.bfloat16
    return pl.pallas_call(
        functools.partial(attend_kernel, head),
        out_shape=jax.ShapeDtypeStruct((length // LANES, LANES, LANES), bf16),
        in_specs=[pl.BlockSpec(memory_space=pltpu.SMEM)] + [whole()] * 4,
        out_specs=whole(),
        scratch_shapes=[pltpu.VMEM((length, LANES), bf16)] * 3
        + [pltpu.VMEM((2, block, length), jnp.float32)],
        cost_estimate=pl.CostEstimate(
            flops=4 * length * length * LANES, bytes_accessed=8000000, transcendentals=length * length
        ),
        compiler_params=pltpu.CompilerParams(vmem_limit_bytes=32 << 20),
        name="attend",
    )(where, *parts)


def proj_kernel(where_ref, heads_ref, own_ref, left_ref, right_ref, fa_ref, fb_ref,
                mine_ref, other_ref, h_ref, p_ref):
    own = mine_ref.shape[0]
    core = where_ref[8]
    head = own_ref.shape[1]
    for i in range(8):
        piece = (own_ref, left_ref, right_ref)[i // 2][i % 2] if i < 6 else (fa_ref, fb_ref)[i % 2][...]
        p_ref[i * LANES : i * LANES + head, :] = piece
        p_ref[i * LANES + head : (i + 1) * LANES, :] = jnp.zeros(
            (LANES - head, p_ref.shape[1]), p_ref.dtype
        )
        h_ref[:, i * LANES : (i + 1) * LANES] = heads_ref[where_ref[i]]
    for target, first in ((other_ref, (1 - core) * own), (mine_ref, core * own)):
        left = h_ref[pl.ds(pl.multiple_of(first, own), own), :]
        total = jnp.dot(left, p_ref[...], preferred_element_type=jnp.float32)
        target[...] = total.astype(target.dtype)


def project(where, heads, pieces, own, width):
    out = jax.ShapeDtypeStruct((own, width), jnp.bfloat16)
    return pl.pallas_call(
        proj_kernel,
        out_shape=(out, out),
        in_specs=[pl.BlockSpec(memory_space=pltpu.SMEM)] + [whole()] * 6,
        out_specs=(whole(), whole()),
        scratch_shapes=[
            pltpu.VMEM((2 * own, 8 * LANES), jnp.bfloat16),
            pltpu.VMEM((8 * LANES, width), jnp.bfloat16),
        ],
        cost_estimate=pl.CostEstimate(flops=740000000, bytes_accessed=4000000, transcendentals=0),
        compiler_params=pltpu.CompilerParams(vmem_limit_bytes=24 << 20),
        name="project",
    )(where, heads, *pieces)


def ln2_kernel(x_ref, mine_ref, other_ref, pbias_ref, gain_ref, bias_ref, ln2_ref, resid_ref):
    f32 = jnp.float32
    total = mine_ref[...].astype(f32) + other_ref[...].astype(f32)
    resid = x_ref[...].astype(f32) + total + row(pbias_ref).astype(f32)
    resid_ref[...] = resid
    ln2_ref[...] = norm_rows(resid, row(gain_ref), row(bias_ref)).astype(ln2_ref.dtype)


def second_norm(x, mine, other, pbias, gain, bias):
    return pl.pallas_call(
        ln2_kernel,
        out_shape=(
            jax.ShapeDtypeStruct(x.shape, jnp.bfloat16),
            jax.ShapeDtypeStruct(x.shape, jnp.float32),
        ),
        in_specs=[whole()] * 6,
        out_specs=(whole(), whole()),
        cost_estimate=pl.CostEstimate(flops=12 * x.size, bytes_accessed=12 * x.size, transcendentals=0),
        compiler_params=pltpu.CompilerParams(vmem_limit_bytes=8 << 20),
        name="second_norm",
    )(x, mine, other, pbias, gain, bias)


def pass_kernel(right_ref, via_a_ref, left_ref, via_b_ref, to_right_ref, to_left_ref):
    f32 = jnp.float32
    half = via_a_ref.shape[0]
    near, far = slice(0, half), slice(half, 2 * half)
    to_right_ref[near, :] = (right_ref[near, :] + via_a_ref[...].astype(f32)).astype(to_right_ref.dtype)
    to_right_ref[far, :] = right_ref[far, :].astype(to_right_ref.dtype)
    to_left_ref[near, :] = left_ref[near, :].astype(to_left_ref.dtype)
    to_left_ref[far, :] = (left_ref[far, :] + via_b_ref[...].astype(f32)).astype(to_left_ref.dtype)


def pass_on(right, via_a, left, via_b):
    out = jax.ShapeDtypeStruct(right.shape, via_a.dtype)
    return pl.pallas_call(
        pass_kernel,
        out_shape=(out, out),
        in_specs=[whole()] * 4,
        out_specs=(whole(), whole()),
        cost_estimate=pl.CostEstimate(flops=200000, bytes_accessed=1000000, transcendentals=0),
        compiler_params=pltpu.CompilerParams(vmem_limit_bytes=8 << 20),
        name="pass_on",
    )(right, via_a, left, via_b)


def gelu(x):
    return 0.5 * x * (1.0 + lax.erf(x * 0.7071067811865476))


def second_product(hidden, w2):
    return lax.dot_general(hidden, w2, (((1,), (1,)), ((), ())), preferred_element_type=jnp.float32)


def head_kernel(slab, own_ref, left_ref, right_ref, fa_ref, fb_ref, w_ref,
                hidden, w2, pfa_ref, pfb_ref, rows, w1, b1, sem1, sem2, sem3):
    f32 = jnp.float32
    own = own_ref.shape[0]
    hid = w_ref.shape[3]
    loads1 = [[], [], [], []]
    loads2 = [[], [], [], []]
    for b in range(4):
        cols = pl.ds(b * hid, hid)
        for r in range(8):
            rows_r = pl.ds(r * slab, slab)
            loads1[b].append(
                pltpu.make_async_copy(w_ref.at[r, b, pl.ds(0, slab)], w1.at[rows_r, cols], sem1.at[b, r])
            )
            loads2[b].append(
                pltpu.make_async_copy(w_ref.at[r, b, pl.ds(slab, slab)], w2.at[rows_r, cols], sem2.at[b, r])
            )
        loads1[b].append(
            pltpu.make_async_copy(w_ref.at[0, b, pl.ds(2 * slab, 16)], b1.at[b], sem3.at[b])
        )
    queue = loads1 + loads2
    for group in queue[:2]:
        for copy in group:
            copy.start()
    rows[:own] = own_ref[...]
    rows[own : 2 * own] = left_ref[...]
    rows[2 * own : 3 * own] = right_ref[...]
    rows[3 * own : 3 * own + own // 2] = fa_ref[...]
    rows[3 * own + own // 2 :] = fb_ref[...]
    for b in range(4):
        for copy in loads1[b]:
            copy.wait()
        for group in queue[b + 2 : b + 3] if b < 3 else queue[5:]:
            for copy in group:
                copy.start()
        cols = slice(b * hid, (b + 1) * hid)
        for m in range(2):
            part = slice(2 * own * m, 2 * own * (m + 1))
            value = jnp.dot(rows[part], w1[:, cols], preferred_element_type=f32)
            value = value + b1[b, 0:1].astype(f32)
            hidden[part, cols] = gelu(value).astype(hidden.dtype)
    for group in loads2:
        for copy in group:
            copy.wait()
    half = own // 2
    out = second_product(hidden[3 * own :], w2[...])
    pfa_ref[...] = out[:half].astype(pfa_ref.dtype)
    pfb_ref[...] = out[half:].astype(pfb_ref.dtype)


def mlp_head(pieces, weights, slab):
    own, width = pieces[0].shape
    hid = weights.shape[3]
    bf16 = jnp.bfloat16
    far = jax.ShapeDtypeStruct((own // 2, width), bf16)
    return pl.pallas_call(
        functools.partial(head_kernel, slab),
        out_shape=(
            jax.ShapeDtypeStruct((4 * own, 4 * hid), bf16),
            jax.ShapeDtypeStruct((width, 4 * hid), bf16),
            far,
            far,
        ),
        in_specs=[whole()] * 5 + [pl.BlockSpec(memory_space=pltpu.HBM)],
        out_specs=(whole(),) * 4,
        scratch_shapes=[
            pltpu.VMEM((4 * own, width), bf16),
            pltpu.VMEM((width, 4 * hid), bf16),
            pltpu.VMEM((4, 16, hid), bf16),
            pltpu.SemaphoreType.DMA((4, 8)),
            pltpu.SemaphoreType.DMA((4, 8)),
            pltpu.SemaphoreType.DMA((4,)),
        ],
        cost_estimate=pl.CostEstimate(flops=2770000000, bytes_accessed=12000000, transcendentals=800000),
        compiler_params=pltpu.CompilerParams(vmem_limit_bytes=46 << 20),
        name="mlp_head",
    )(*pieces, weights)


def sides_kernel(hidden, w2, left_ref, right_ref):
    own = left_ref.shape[0]
    out = second_product(hidden[own : 3 * own], w2[...])
    left_ref[...] = out[:own]
    right_ref[...] = out[own:]


def mlp_sides(hidden, w2):
    out = jax.ShapeDtypeStruct((hidden.shape[0] // 4, w2.shape[0]), jnp.float32)
    return pl.pallas_call(
        sides_kernel,
        out_shape=(out, out),
        in_specs=[whole()] * 2,
        out_specs=(whole(), whole()),
        cost_estimate=pl.CostEstimate(flops=1100000000, bytes_accessed=8000000, transcendentals=0),
        compiler_params=pltpu.CompilerParams(vmem_limit_bytes=24 << 20),
        name="mlp_sides",
    )(hidden, w2)


def own_kernel(hidden, w2, resid_ref, bias_ref, out_ref):
    own = out_ref.shape[0]
    out = second_product(hidden[:own], w2[...])
    out_ref[...] = resid_ref[...] + out + row(bias_ref).astype(jnp.float32)


def mlp_own(hidden, w2, resid, bias):
    return pl.pallas_call(
        own_kernel,
        out_shape=jax.ShapeDtypeStruct(resid.shape, jnp.float32),
        in_specs=[whole()] * 4,
        out_specs=whole(),
        cost_estimate=pl.CostEstimate(flops=550000000, bytes_accessed=8000000, transcendentals=0),
        compiler_params=pltpu.CompilerParams(vmem_limit_bytes=24 << 20),
        name="mlp_own",
    )(hidden, w2, resid, bias)


def layer(
    tokens_in,
    ln1_gain,
    ln1_bias,
    qkv_weight,
    qkv_bias,
    proj_weight,
    proj_bias,
    ln2_gain,
    ln2_bias,
    fc1_weight,
    fc1_bias,
    fc2_weight,
    fc2_bias,
):
    f32, bf16 = jnp.float32, jnp.bfloat16
    own = tokens_in.shape[0]
    width = tokens_in.shape[1]
    head = proj_weight.shape[0]
    slab = qkv_weight.shape[0]
    hid = fc1_weight.shape[1]
    core = lax.axis_index("core")
    z, yh = lax.axis_index("z"), lax.axis_index("yh")
    x, yl = lax.axis_index("x"), lax.axis_index("yl")

    half = own // 2

    wide = jnp.pad(proj_weight, ((0, 0), (0, qkv_weight.shape[1] - slab)))
    rowset = jnp.concatenate([qkv_weight, wide], axis=0)
    pair = jnp.stack([rowset, shift(rowset, dyh=1)])
    pieces = [pair] + [shift(pair, dz=dz) for dz in (1, 2, 3)]
    where = jnp.stack([(z + 4 - dz) % 4 * 2 + (yh + j) % 2 for dz in range(4) for j in range(2)])
    w_own, proj_own = place(where.astype(jnp.int32), qkv_bias, pieces, slab, head)
    w_other = shift(w_own, dc=1)
    proj_own = jnp.moveaxis(proj_own, 0, 1).reshape(head, width)
    p_pair = jnp.stack([proj_own, shift(proj_own, dyl=1)])
    p_left = shift(p_pair, dx=1)
    p_right = shift(p_pair, dx=3)
    p_fa = shift(p_left[0], dx=1)
    p_fb = shift(p_right[1], dx=3)

    bias_rows = jnp.broadcast_to(fc1_bias[None], (16, hid))
    stack = jnp.concatenate([fc1_weight, fc2_weight, bias_rows], axis=0)
    mlp = lax.all_gather(stack, ("z", "yh", "yl", "core"), axis=0, tiled=False)
    mlp = mlp.reshape(8, 4, stack.shape[0], hid)

    ln1 = first_norm(tokens_in, ln1_gain, ln1_bias)
    left = shift(ln1, dx=1)
    right = shift(ln1, dx=3)
    side = shift(ln1, dyl=1)
    side_left = shift(side, dx=1)
    side_right = shift(side, dx=3)
    far_a = shift(left[:half], dx=1)
    far_b = shift(right[half:], dx=3)
    side_far_a = shift(side_left[:half], dx=1)
    side_far_b = shift(side_right[half:], dx=3)
    near = qkv_part((ln1, left, right, side), w_own, w_other)
    rest = (side_left, side_right, far_a, far_b, side_far_a, side_far_b)
    rest = qkv_part(rest, w_own, w_other)
    parts = (near[0], rest[0], shift(near[1], dc=1), shift(rest[1], dc=1))
    spots = [(0, 0), (1, 0), (3, 0), (0, 1), (1, 1), (3, 1), (2, 0), (2, 1)]
    places = [
        ((x + 4 - dx) % 4 * 2 + (yl + j) % 2) * 2 + (core + k) % 2 for k in range(2) for dx, j in spots
    ]
    attn = attend(jnp.stack(places).astype(jnp.int32), parts, head)
    heads = lax.all_to_all(attn.reshape(8, 2 * own, LANES), ("x", "yl"), 0, 0, tiled=True)
    order = [(0, 0), (0, 1), (1, 0), (1, 1), (3, 0), (3, 1), (2, 0), (2, 1)]
    where = [(x + 4 - dx) % 4 * 2 + (yl + j) % 2 for dx, j in order]
    where = jnp.stack(where + [core]).astype(jnp.int32)
    proj_sets = (p_pair, p_left, p_right, p_fa, p_fb)
    mine, other = project(where, heads, proj_sets, own, width)
    other = shift(other, dc=1)
    ln2, resid = second_norm(tokens_in, mine, other, proj_bias, ln2_gain, ln2_bias)

    left = shift(ln2, dx=1)
    right = shift(ln2, dx=3)
    far_a = shift(left[:half], dx=1)
    far_b = shift(right[half:], dx=3)
    hidden, w2, fa, fb = mlp_head((ln2, left, right, far_a, far_b), mlp, slab)

    via_a = shift(fa, dx=1)
    via_b = shift(fb, dx=3)
    o_left, o_right = mlp_sides(hidden, w2)
    to_right, to_left = pass_on(o_right, via_a, o_left, via_b)
    from_left = shift(to_right, dx=1)
    from_right = shift(to_left, dx=3)
    mine = mlp_own(hidden, w2, resid, fc2_bias)
    return (mine + from_left.astype(f32) + from_right.astype(f32)).astype(bf16)


def solution(mesh):
    fine = Mesh(np.asarray(mesh.devices).reshape(SIZES), AXES)
    in_specs = (
        P(AXES, None),
        P(),
        P(),
        P(ROW, COL),
        P(COL),
        P(COL, ROW),
        P(),
        P(),
        P(),
        P(ROW, COL),
        P(COL),
        P(ROW, COL),
        P(),
    )
    return jax.shard_map(layer, mesh=fine, in_specs=in_specs, out_specs=P(AXES, None), check_vma=False)
```

```python
import functools
import itertools

import jax
import jax.numpy as jnp
import numpy as np
from jax import lax
from jax.experimental import pallas as pl
from jax.experimental.pallas import tpu as pltpu
from jax.sharding import Mesh
from jax.sharding import PartitionSpec as P


LANES = 128
AXES = ("z", "yh", "x", "yl", "core")
SIZES = (4, 2, 4, 2, 2)
ROW = ("z", "yh")
COL = ("x", "yl", "core")


def shift(value, dz=0, dyh=0, dx=0, dyl=0, dc=0):
    pairs = []
    for place in itertools.product(*[range(n) for n in SIZES]):
        target = [(p + d) % n for p, d, n in zip(place, (dz, dyh, dx, dyl, dc), SIZES)]
        pairs.append(
            (int(np.ravel_multi_index(place, SIZES)), int(np.ravel_multi_index(target, SIZES)))
        )
    return lax.ppermute(value, AXES, pairs)


def whole():
    return pl.BlockSpec(memory_space=pltpu.VMEM)


def norm_rows(values, gain, bias):
    mean = jnp.mean(values, axis=-1, keepdims=True)
    centred = values - mean
    var = jnp.mean(centred * centred, axis=-1, keepdims=True)
    return centred * lax.rsqrt(var + 1e-06) * gain.astype(jnp.float32) + bias.astype(jnp.float32)


def row(ref):
    return ref[...].reshape(1, ref.shape[0])


def ln1_kernel(x_ref, gain_ref, bias_ref, out_ref):
    values = x_ref[...].astype(jnp.float32)
    out_ref[...] = norm_rows(values, row(gain_ref), row(bias_ref)).astype(out_ref.dtype)


def first_norm(x, gain, bias):
    return pl.pallas_call(
        ln1_kernel,
        out_shape=jax.ShapeDtypeStruct(x.shape, jnp.bfloat16),
        in_specs=[whole()] * 3,
        out_specs=whole(),
        cost_estimate=pl.CostEstimate(flops=10 * x.size, bytes_accessed=4 * x.size, transcendentals=0),
        compiler_params=pltpu.CompilerParams(vmem_limit_bytes=8 << 20),
        name="first_norm",
    )(x, gain, bias)


def spread(values, head, ones):
    rows = values.shape[0]
    gap = jnp.zeros((rows, LANES - head), values.dtype)
    lane = lax.broadcasted_iota(jnp.int32, (rows, LANES - head), 1)
    last = jnp.where(lane == 0, jnp.ones_like(gap), gap) if ones else gap
    q, k, v = (values[:, n * head : (n + 1) * head] for n in range(3))
    return jnp.concatenate([q, gap, k, gap, v, last], axis=1)


def place_kernel(head, where_ref, bias_ref, own_ref, low_ref, high_ref, far_ref, w_ref):
    slab = own_ref.shape[1]
    for n, ref in enumerate((own_ref, low_ref, high_ref, far_ref)):
        for j in range(2):
            first = pl.multiple_of(where_ref[2 * n + j] * slab, 16)
            value = spread(ref[j].astype(jnp.float32), head, False)
            w_ref[pl.ds(first, slab), :] = value.astype(w_ref.dtype)
    bias = spread(row(bias_ref).astype(jnp.float32), head, True)
    w_ref[8 * slab :, :] = jnp.broadcast_to(bias, (16, bias.shape[1])).astype(w_ref.dtype)


def place(where, bias, pieces):
    _, slab, cols = pieces[0].shape
    return pl.pallas_call(
        functools.partial(place_kernel, cols // 3),
        out_shape=jax.ShapeDtypeStruct((8 * slab + 16, 3 * LANES), jnp.bfloat16),
        in_specs=[pl.BlockSpec(memory_space=pltpu.SMEM)] + [whole()] * 5,
        out_specs=whole(),
        cost_estimate=pl.CostEstimate(flops=1000000, bytes_accessed=3000000, transcendentals=0),
        compiler_params=pltpu.CompilerParams(vmem_limit_bytes=12 << 20),
        name="place_rows",
    )(where, bias, *pieces)


def place_proj_kernel(where_ref, own_ref, low_ref, high_ref, far_ref, out_ref):
    for n, ref in enumerate((own_ref, low_ref, high_ref, far_ref)):
        for j in range(2):
            out_ref[where_ref[2 * n + j]] = ref[j]


def place_proj(where, pieces):
    return pl.pallas_call(
        place_proj_kernel,
        out_shape=jax.ShapeDtypeStruct((8, *pieces[0].shape[1:]), jnp.bfloat16),
        in_specs=[pl.BlockSpec(memory_space=pltpu.SMEM)] + [whole()] * 4,
        out_specs=whole(),
        cost_estimate=pl.CostEstimate(flops=100000, bytes_accessed=1000000, transcendentals=0),
        compiler_params=pltpu.CompilerParams(vmem_limit_bytes=8 << 20),
        name="place_proj",
    )(where, *pieces)


def qkv_kernel(count, *refs):
    pieces, (w_own, w_other, out_own, out_other, rows) = refs[:count], refs[count:]
    width = rows.shape[1]
    first = 0
    for ref in pieces:
        rows[first : first + ref.shape[0], :] = ref[...]
        first += ref.shape[0]
    for w_ref, out_ref in ((w_other, out_other), (w_own, out_own)):
        bias = w_ref[width : width + 1, :].astype(jnp.float32)
        value = jnp.dot(rows[...], w_ref[:width, :], preferred_element_type=jnp.float32)
        out_ref[...] = (value + bias).astype(out_ref.dtype)


def qkv_part(pieces, w_own, w_other):
    rows = sum(p.shape[0] for p in pieces)
    cols = w_own.shape[1]
    out = jax.ShapeDtypeStruct((rows, cols), jnp.bfloat16)
    return pl.pallas_call(
        functools.partial(qkv_kernel, len(pieces)),
        out_shape=(out, out),
        in_specs=[whole()] * (len(pieces) + 2),
        out_specs=(whole(), whole()),
        scratch_shapes=[pltpu.VMEM((rows, pieces[0].shape[1]), jnp.bfloat16)],
        cost_estimate=pl.CostEstimate(
            flops=4 * rows * cols * w_own.shape[0], bytes_accessed=4000000, transcendentals=0
        ),
        compiler_params=pltpu.CompilerParams(vmem_limit_bytes=16 << 20),
        name="qkv_part",
    )(*pieces, w_own, w_other)


def attend_kernel(head, where_ref, *refs):
    f32 = jnp.float32
    parts, (out_ref, q_ref, k_ref, v_ref, s_ref) = refs[:4], refs[4:]
    length = q_ref.shape[0]
    first = 0
    for ref in parts:
        rows = slice(first, first + ref.shape[0])
        q_ref[rows, :] = ref[:, :LANES]
        k_ref[rows, :] = ref[:, LANES : 2 * LANES]
        v_ref[rows, :] = ref[:, 2 * LANES :]
        first += ref.shape[0]
    block = s_ref.shape[1]
    steps = length // block
    scale = 1.4426950408889634 / head**0.5

    def scores(i):
        s_ref[i % 2] = lax.dot_general(
            q_ref[i * block : (i + 1) * block, :],
            k_ref[...],
            (((1,), (1,)), ((), ())),
            preferred_element_type=f32,
        )

    scores(0)
    for i in range(steps):
        value = s_ref[i % 2]
        if i + 1 < steps:
            scores(i + 1)
        top = jnp.max(value, axis=-1, keepdims=True)
        expo = jnp.exp2((value - top) * scale).astype(jnp.bfloat16)
        mixed = jnp.dot(expo, v_ref[...], preferred_element_type=f32)
        mixed = (mixed / mixed[:, head : head + 1]).astype(out_ref.dtype)
        for n in range(block // LANES):
            out_ref[where_ref[i * (block // LANES) + n]] = mixed[n * LANES : (n + 1) * LANES]


def attend(where, parts, head):
    length = sum(p.shape[0] for p in parts)
    block, bf16 = 256, jnp.bfloat16
    return pl.pallas_call(
        functools.partial(attend_kernel, head),
        out_shape=jax.ShapeDtypeStruct((length // LANES, LANES, LANES), bf16),
        in_specs=[pl.BlockSpec(memory_space=pltpu.SMEM)] + [whole()] * 4,
        out_specs=whole(),
        scratch_shapes=[pltpu.VMEM((length, LANES), bf16)] * 3
        + [pltpu.VMEM((2, block, length), jnp.float32)],
        cost_estimate=pl.CostEstimate(
            flops=4 * length * length * LANES, bytes_accessed=8000000, transcendentals=length * length
        ),
        compiler_params=pltpu.CompilerParams(vmem_limit_bytes=32 << 20),
        name="attend",
    )(where, *parts)


def proj_kernel(where_ref, heads_ref, own_ref, left_ref, right_ref, fa_ref, fb_ref,
                mine_ref, other_ref, h_ref, p_ref):
    own = mine_ref.shape[0]
    core = where_ref[8]
    head = own_ref.shape[1]
    for i in range(8):
        piece = (own_ref, left_ref, right_ref)[i // 2][i % 2] if i < 6 else (fa_ref, fb_ref)[i % 2][...]
        p_ref[i * LANES : i * LANES + head, :] = piece
        p_ref[i * LANES + head : (i + 1) * LANES, :] = jnp.zeros(
            (LANES - head, p_ref.shape[1]), p_ref.dtype
        )
        h_ref[:, i * LANES : (i + 1) * LANES] = heads_ref[where_ref[i]]
    for target, first in ((other_ref, (1 - core) * own), (mine_ref, core * own)):
        left = h_ref[pl.ds(pl.multiple_of(first, own), own), :]
        total = jnp.dot(left, p_ref[...], preferred_element_type=jnp.float32)
        target[...] = total.astype(target.dtype)


def project(where, heads, pieces, own, width):
    out = jax.ShapeDtypeStruct((own, width), jnp.bfloat16)
    return pl.pallas_call(
        proj_kernel,
        out_shape=(out, out),
        in_specs=[pl.BlockSpec(memory_space=pltpu.SMEM)] + [whole()] * 6,
        out_specs=(whole(), whole()),
        scratch_shapes=[
            pltpu.VMEM((2 * own, 8 * LANES), jnp.bfloat16),
            pltpu.VMEM((8 * LANES, width), jnp.bfloat16),
        ],
        cost_estimate=pl.CostEstimate(flops=740000000, bytes_accessed=4000000, transcendentals=0),
        compiler_params=pltpu.CompilerParams(vmem_limit_bytes=24 << 20),
        name="project",
    )(where, heads, *pieces)


def ln2_kernel(x_ref, mine_ref, other_ref, pbias_ref, gain_ref, bias_ref, ln2_ref, resid_ref):
    f32 = jnp.float32
    total = mine_ref[...].astype(f32) + other_ref[...].astype(f32)
    resid = x_ref[...].astype(f32) + total + row(pbias_ref).astype(f32)
    resid_ref[...] = resid
    ln2_ref[...] = norm_rows(resid, row(gain_ref), row(bias_ref)).astype(ln2_ref.dtype)


def second_norm(x, mine, other, pbias, gain, bias):
    return pl.pallas_call(
        ln2_kernel,
        out_shape=(
            jax.ShapeDtypeStruct(x.shape, jnp.bfloat16),
            jax.ShapeDtypeStruct(x.shape, jnp.float32),
        ),
        in_specs=[whole()] * 6,
        out_specs=(whole(), whole()),
        cost_estimate=pl.CostEstimate(flops=12 * x.size, bytes_accessed=12 * x.size, transcendentals=0),
        compiler_params=pltpu.CompilerParams(vmem_limit_bytes=8 << 20),
        name="second_norm",
    )(x, mine, other, pbias, gain, bias)


def pass_kernel(right_ref, via_a_ref, left_ref, via_b_ref, to_right_ref, to_left_ref):
    f32 = jnp.float32
    half = via_a_ref.shape[0]
    near, far = slice(0, half), slice(half, 2 * half)
    to_right_ref[near, :] = (right_ref[near, :] + via_a_ref[...].astype(f32)).astype(to_right_ref.dtype)
    to_right_ref[far, :] = right_ref[far, :].astype(to_right_ref.dtype)
    to_left_ref[near, :] = left_ref[near, :].astype(to_left_ref.dtype)
    to_left_ref[far, :] = (left_ref[far, :] + via_b_ref[...].astype(f32)).astype(to_left_ref.dtype)


def pass_on(right, via_a, left, via_b):
    out = jax.ShapeDtypeStruct(right.shape, via_a.dtype)
    return pl.pallas_call(
        pass_kernel,
        out_shape=(out, out),
        in_specs=[whole()] * 4,
        out_specs=(whole(), whole()),
        cost_estimate=pl.CostEstimate(flops=200000, bytes_accessed=1000000, transcendentals=0),
        compiler_params=pltpu.CompilerParams(vmem_limit_bytes=8 << 20),
        name="pass_on",
    )(right, via_a, left, via_b)


def gelu(x):
    return 0.5 * x * (1.0 + lax.erf(x * 0.7071067811865476))


def second_product(hidden, w2):
    return lax.dot_general(hidden, w2, (((1,), (1,)), ((), ())), preferred_element_type=jnp.float32)


def head_kernel(slab, own_ref, left_ref, right_ref, fa_ref, fb_ref, w_ref,
                hidden, w2, pfa_ref, pfb_ref, rows, w1, b1, sem1, sem2, sem3):
    f32 = jnp.float32
    own = own_ref.shape[0]
    hid = w_ref.shape[3]
    loads1 = [[], [], [], []]
    loads2 = [[], [], [], []]
    for b in range(4):
        cols = pl.ds(b * hid, hid)
        for r in range(8):
            rows_r = pl.ds(r * slab, slab)
            loads1[b].append(
                pltpu.make_async_copy(w_ref.at[r, b, pl.ds(0, slab)], w1.at[rows_r, cols], sem1.at[b, r])
            )
            loads2[b].append(
                pltpu.make_async_copy(w_ref.at[r, b, pl.ds(slab, slab)], w2.at[rows_r, cols], sem2.at[b, r])
            )
        loads1[b].append(
            pltpu.make_async_copy(w_ref.at[0, b, pl.ds(2 * slab, 16)], b1.at[b], sem3.at[b])
        )
    queue = loads1 + loads2
    for group in queue[:2]:
        for copy in group:
            copy.start()
    rows[:own] = own_ref[...]
    rows[own : 2 * own] = left_ref[...]
    rows[2 * own : 3 * own] = right_ref[...]
    rows[3 * own : 3 * own + own // 2] = fa_ref[...]
    rows[3 * own + own // 2 :] = fb_ref[...]
    for b in range(4):
        for copy in loads1[b]:
            copy.wait()
        for group in queue[b + 2 : b + 3] if b < 3 else queue[5:]:
            for copy in group:
                copy.start()
        cols = slice(b * hid, (b + 1) * hid)
        for m in range(2):
            part = slice(2 * own * m, 2 * own * (m + 1))
            value = jnp.dot(rows[part], w1[:, cols], preferred_element_type=f32)
            value = value + b1[b, 0:1].astype(f32)
            hidden[part, cols] = gelu(value).astype(hidden.dtype)
    for group in loads2:
        for copy in group:
            copy.wait()
    half = own // 2
    out = second_product(hidden[3 * own :], w2[...])
    pfa_ref[...] = out[:half].astype(pfa_ref.dtype)
    pfb_ref[...] = out[half:].astype(pfb_ref.dtype)


def mlp_head(pieces, weights, slab):
    own, width = pieces[0].shape
    hid = weights.shape[3]
    bf16 = jnp.bfloat16
    far = jax.ShapeDtypeStruct((own // 2, width), bf16)
    return pl.pallas_call(
        functools.partial(head_kernel, slab),
        out_shape=(
            jax.ShapeDtypeStruct((4 * own, 4 * hid), bf16),
            jax.ShapeDtypeStruct((width, 4 * hid), bf16),
            far,
            far,
        ),
        in_specs=[whole()] * 5 + [pl.BlockSpec(memory_space=pltpu.HBM)],
        out_specs=(whole(),) * 4,
        scratch_shapes=[
            pltpu.VMEM((4 * own, width), bf16),
            pltpu.VMEM((width, 4 * hid), bf16),
            pltpu.VMEM((4, 16, hid), bf16),
            pltpu.SemaphoreType.DMA((4, 8)),
            pltpu.SemaphoreType.DMA((4, 8)),
            pltpu.SemaphoreType.DMA((4,)),
        ],
        cost_estimate=pl.CostEstimate(flops=2770000000, bytes_accessed=12000000, transcendentals=800000),
        compiler_params=pltpu.CompilerParams(vmem_limit_bytes=46 << 20),
        name="mlp_head",
    )(*pieces, weights)


def sides_kernel(hidden, w2, left_ref, right_ref):
    own = left_ref.shape[0]
    out = second_product(hidden[own : 3 * own], w2[...])
    left_ref[...] = out[:own]
    right_ref[...] = out[own:]


def mlp_sides(hidden, w2):
    out = jax.ShapeDtypeStruct((hidden.shape[0] // 4, w2.shape[0]), jnp.float32)
    return pl.pallas_call(
        sides_kernel,
        out_shape=(out, out),
        in_specs=[whole()] * 2,
        out_specs=(whole(), whole()),
        cost_estimate=pl.CostEstimate(flops=1100000000, bytes_accessed=8000000, transcendentals=0),
        compiler_params=pltpu.CompilerParams(vmem_limit_bytes=24 << 20),
        name="mlp_sides",
    )(hidden, w2)


def own_kernel(hidden, w2, resid_ref, bias_ref, out_ref):
    own = out_ref.shape[0]
    out = second_product(hidden[:own], w2[...])
    out_ref[...] = resid_ref[...] + out + row(bias_ref).astype(jnp.float32)


def mlp_own(hidden, w2, resid, bias):
    return pl.pallas_call(
        own_kernel,
        out_shape=jax.ShapeDtypeStruct(resid.shape, jnp.float32),
        in_specs=[whole()] * 4,
        out_specs=whole(),
        cost_estimate=pl.CostEstimate(flops=550000000, bytes_accessed=8000000, transcendentals=0),
        compiler_params=pltpu.CompilerParams(vmem_limit_bytes=24 << 20),
        name="mlp_own",
    )(hidden, w2, resid, bias)


def layer(
    tokens_in,
    ln1_gain,
    ln1_bias,
    qkv_weight,
    qkv_bias,
    proj_weight,
    proj_bias,
    ln2_gain,
    ln2_bias,
    fc1_weight,
    fc1_bias,
    fc2_weight,
    fc2_bias,
):
    f32, bf16 = jnp.float32, jnp.bfloat16
    own = tokens_in.shape[0]
    width = tokens_in.shape[1]
    head = proj_weight.shape[0]
    slab = qkv_weight.shape[0]
    hid = fc1_weight.shape[1]
    core = lax.axis_index("core")
    z, yh = lax.axis_index("z"), lax.axis_index("yh")
    x, yl = lax.axis_index("x"), lax.axis_index("yl")

    half = own // 2

    pair = jnp.stack([qkv_weight, shift(qkv_weight, dyh=1)])
    low = shift(pair, dz=1)
    high = shift(pair, dz=3)
    far = shift(low, dz=1)
    where = [(z + 4 - dz) % 4 * 2 + (yh + j) % 2 for dz in (0, 1, 3, 2) for j in range(2)]
    where = jnp.stack(where).astype(jnp.int32)
    w_own = place(where, qkv_bias, (pair, low, high, far))
    w_other = shift(w_own, dc=1)

    p_rows = jnp.stack([proj_weight, shift(proj_weight, dyh=1)])
    p_rows = [p_rows] + [shift(p_rows, dz=dz) for dz in (1, 3, 2)]
    proj_own = place_proj(where, p_rows)
    proj_own = jnp.moveaxis(proj_own, 0, 1).reshape(head, width)
    p_pair = jnp.stack([proj_own, shift(proj_own, dyl=1)])
    p_left = shift(p_pair, dx=1)
    p_right = shift(p_pair, dx=3)
    p_fa = shift(p_left[0], dx=1)
    p_fb = shift(p_right[1], dx=3)

    bias_rows = jnp.broadcast_to(fc1_bias[None], (16, hid))
    stack = jnp.concatenate([fc1_weight, fc2_weight, bias_rows], axis=0)
    mlp = lax.all_gather(stack, ("z", "yh", "yl", "core"), axis=0, tiled=False)
    mlp = mlp.reshape(8, 4, stack.shape[0], hid)

    ln1 = first_norm(tokens_in, ln1_gain, ln1_bias)
    left = shift(ln1, dx=1)
    right = shift(ln1, dx=3)
    side = shift(ln1, dyl=1)
    side_left = shift(side, dx=1)
    side_right = shift(side, dx=3)
    far = shift(left, dx=1)
    side_far = shift(side_right, dx=3)
    near = qkv_part((ln1, left, right, side), w_own, w_other)
    rest = qkv_part((side_left, side_right, far, side_far), w_own, w_other)
    parts = (near[0], rest[0], shift(near[1], dc=1), shift(rest[1], dc=1))
    spots = [(0, 0), (1, 0), (3, 0), (0, 1), (1, 1), (3, 1), (2, 0), (2, 1)]
    places = [
        ((x + 4 - dx) % 4 * 2 + (yl + j) % 2) * 2 + (core + k) % 2 for k in range(2) for dx, j in spots
    ]
    attn = attend(jnp.stack(places).astype(jnp.int32), parts, head)
    heads = lax.all_to_all(attn.reshape(8, 2 * own, LANES), ("x", "yl"), 0, 0, tiled=True)
    order = [(0, 0), (0, 1), (1, 0), (1, 1), (3, 0), (3, 1), (2, 0), (2, 1)]
    where = [(x + 4 - dx) % 4 * 2 + (yl + j) % 2 for dx, j in order]
    where = jnp.stack(where + [core]).astype(jnp.int32)
    proj_sets = (p_pair, p_left, p_right, p_fa, p_fb)
    mine, other = project(where, heads, proj_sets, own, width)
    other = shift(other, dc=1)
    ln2, resid = second_norm(tokens_in, mine, other, proj_bias, ln2_gain, ln2_bias)

    left = shift(ln2, dx=1)
    right = shift(ln2, dx=3)
    far_a = shift(left[:half], dx=1)
    far_b = shift(right[half:], dx=3)
    hidden, w2, fa, fb = mlp_head((ln2, left, right, far_a, far_b), mlp, slab)

    via_a = shift(fa, dx=1)
    via_b = shift(fb, dx=3)
    o_left, o_right = mlp_sides(hidden, w2)
    to_right, to_left = pass_on(o_right, via_a, o_left, via_b)
    from_left = shift(to_right, dx=1)
    from_right = shift(to_left, dx=3)
    mine = mlp_own(hidden, w2, resid, fc2_bias)
    return (mine + from_left.astype(f32) + from_right.astype(f32)).astype(bf16)


def solution(mesh):
    fine = Mesh(np.asarray(mesh.devices).reshape(SIZES), AXES)
    in_specs = (
        P(AXES, None),
        P(),
        P(),
        P(ROW, COL),
        P(COL),
        P(COL, ROW),
        P(),
        P(),
        P(),
        P(ROW, COL),
        P(COL),
        P(ROW, COL),
        P(),
    )
    return jax.shard_map(layer, mesh=fine, in_specs=in_specs, out_specs=P(AXES, None), check_vma=False)
```

```python
import functools
import itertools

import jax
import jax.numpy as jnp
import numpy as np
from jax import lax
from jax.experimental import pallas as pl
from jax.experimental.pallas import tpu as pltpu
from jax.sharding import Mesh
from jax.sharding import PartitionSpec as P


LANES = 128
AXES = ("z", "yh", "x", "yl", "core")
SIZES = (4, 2, 4, 2, 2)
ROW = ("z", "yh")
COL = ("x", "yl", "core")


def shift(value, dz=0, dyh=0, dx=0, dyl=0, dc=0):
    pairs = []
    for place in itertools.product(*[range(n) for n in SIZES]):
        target = [(p + d) % n for p, d, n in zip(place, (dz, dyh, dx, dyl, dc), SIZES)]
        pairs.append(
            (int(np.ravel_multi_index(place, SIZES)), int(np.ravel_multi_index(target, SIZES)))
        )
    return lax.ppermute(value, AXES, pairs)


def shift_far(value):
    pairs = []
    for place in itertools.product(*[range(n) for n in SIZES]):
        target = list(place)
        target[2] = (place[2] + (1 if place[4] == 0 else 3)) % 4
        pairs.append(
            (int(np.ravel_multi_index(place, SIZES)), int(np.ravel_multi_index(target, SIZES)))
        )
    return lax.ppermute(value, AXES, pairs)


def whole():
    return pl.BlockSpec(memory_space=pltpu.VMEM)


def norm_rows(values, gain, bias):
    mean = jnp.mean(values, axis=-1, keepdims=True)
    centred = values - mean
    var = jnp.mean(centred * centred, axis=-1, keepdims=True)
    return centred * lax.rsqrt(var + 1e-06) * gain.astype(jnp.float32) + bias.astype(jnp.float32)


def row(ref):
    return ref[...].reshape(1, ref.shape[0])


def ln1_kernel(x_ref, gain_ref, bias_ref, out_ref):
    values = x_ref[...].astype(jnp.float32)
    out_ref[...] = norm_rows(values, row(gain_ref), row(bias_ref)).astype(out_ref.dtype)


def first_norm(x, gain, bias):
    return pl.pallas_call(
        ln1_kernel,
        out_shape=jax.ShapeDtypeStruct(x.shape, jnp.bfloat16),
        in_specs=[whole()] * 3,
        out_specs=whole(),
        cost_estimate=pl.CostEstimate(flops=10 * x.size, bytes_accessed=4 * x.size, transcendentals=0),
        compiler_params=pltpu.CompilerParams(vmem_limit_bytes=8 << 20),
        name="first_norm",
    )(x, gain, bias)


def spread(values, head, ones):
    rows = values.shape[0]
    gap = jnp.zeros((rows, LANES - head), values.dtype)
    lane = lax.broadcasted_iota(jnp.int32, (rows, LANES - head), 1)
    last = jnp.where(lane == 0, jnp.ones_like(gap), gap) if ones else gap
    q, k, v = (values[:, n * head : (n + 1) * head] for n in range(3))
    return jnp.concatenate([q, gap, k, gap, v, last], axis=1)


def place_kernel(head, where_ref, bias_ref, own_ref, low_ref, high_ref, far_ref, w_ref):
    slab = own_ref.shape[1]
    for n, ref in enumerate((own_ref, low_ref, high_ref, far_ref)):
        for j in range(2):
            first = pl.multiple_of(where_ref[2 * n + j] * slab, 16)
            value = spread(ref[j].astype(jnp.float32), head, False)
            w_ref[pl.ds(first, slab), :] = value.astype(w_ref.dtype)
    bias = spread(row(bias_ref).astype(jnp.float32), head, True)
    w_ref[8 * slab :, :] = jnp.broadcast_to(bias, (16, bias.shape[1])).astype(w_ref.dtype)


def place(where, bias, pieces):
    _, slab, cols = pieces[0].shape
    return pl.pallas_call(
        functools.partial(place_kernel, cols // 3),
        out_shape=jax.ShapeDtypeStruct((8 * slab + 16, 3 * LANES), jnp.bfloat16),
        in_specs=[pl.BlockSpec(memory_space=pltpu.SMEM)] + [whole()] * 5,
        out_specs=whole(),
        cost_estimate=pl.CostEstimate(flops=1000000, bytes_accessed=3000000, transcendentals=0),
        compiler_params=pltpu.CompilerParams(vmem_limit_bytes=12 << 20),
        name="place_rows",
    )(where, bias, *pieces)


def place_proj_kernel(which_ref, own_ref, low_ref, high_ref, far_ref, out_ref, held):
    slab = own_ref.shape[2]
    for n, ref in enumerate((own_ref, low_ref, high_ref, far_ref)):
        for j in range(2):
            held[2 * n + j] = ref[j].astype(jnp.float32)
    for r in range(8):
        out_ref[:, r * slab : (r + 1) * slab] = held[which_ref[r]].astype(out_ref.dtype)


def place_proj(which, pieces):
    _, head, slab = pieces[0].shape
    return pl.pallas_call(
        place_proj_kernel,
        out_shape=jax.ShapeDtypeStruct((head, 8 * slab), jnp.bfloat16),
        in_specs=[pl.BlockSpec(memory_space=pltpu.SMEM)] + [whole()] * 4,
        out_specs=whole(),
        scratch_shapes=[pltpu.VMEM((8, head, slab), jnp.float32)],
        cost_estimate=pl.CostEstimate(flops=100000, bytes_accessed=1000000, transcendentals=0),
        compiler_params=pltpu.CompilerParams(vmem_limit_bytes=8 << 20),
        name="place_proj",
    )(which, *pieces)


def qkv_kernel(count, *refs):
    pieces, (w_ref, out_ref, rows) = refs[:count], refs[count:]
    width = rows.shape[1]
    first = 0
    for ref in pieces:
        rows[first : first + ref.shape[0], :] = ref[...]
        first += ref.shape[0]
    bias = w_ref[width : width + 1, :].astype(jnp.float32)
    value = jnp.dot(rows[...], w_ref[:width, :], preferred_element_type=jnp.float32)
    out_ref[...] = (value + bias).astype(out_ref.dtype)


def qkv_part(pieces, weights):
    rows = sum(p.shape[0] for p in pieces)
    cols = weights.shape[1]
    return pl.pallas_call(
        functools.partial(qkv_kernel, len(pieces)),
        out_shape=jax.ShapeDtypeStruct((rows, cols), jnp.bfloat16),
        in_specs=[whole()] * (len(pieces) + 1),
        out_specs=whole(),
        scratch_shapes=[pltpu.VMEM((rows, pieces[0].shape[1]), jnp.bfloat16)],
        cost_estimate=pl.CostEstimate(
            flops=2 * rows * cols * weights.shape[0], bytes_accessed=4000000, transcendentals=0
        ),
        compiler_params=pltpu.CompilerParams(vmem_limit_bytes=16 << 20),
        name="qkv_part",
    )(*pieces, weights)


def attend_kernel(head, where_ref, *refs):
    f32 = jnp.float32
    parts, (out_ref, q_ref, k_ref, v_ref, s_ref) = refs[:3], refs[3:]
    length = q_ref.shape[0]
    first = 0
    for ref in parts:
        rows = slice(first, first + ref.shape[0])
        q_ref[rows, :] = ref[:, :LANES]
        k_ref[rows, :] = ref[:, LANES : 2 * LANES]
        v_ref[rows, :] = ref[:, 2 * LANES :]
        first += ref.shape[0]
    block = s_ref.shape[1]
    steps = length // block
    scale = 1.4426950408889634 / head**0.5

    def scores(i):
        s_ref[i % 2] = lax.dot_general(
            q_ref[i * block : (i + 1) * block, :],
            k_ref[...],
            (((1,), (1,)), ((), ())),
            preferred_element_type=f32,
        )

    scores(0)
    for i in range(steps):
        value = s_ref[i % 2]
        if i + 1 < steps:
            scores(i + 1)
        top = jnp.max(value, axis=-1, keepdims=True)
        expo = jnp.exp2((value - top) * scale).astype(jnp.bfloat16)
        mixed = jnp.dot(expo, v_ref[...], preferred_element_type=f32)
        mixed = (mixed / mixed[:, head : head + 1]).astype(out_ref.dtype)
        for n in range(block // LANES):
            out_ref[where_ref[i * (block // LANES) + n]] = mixed[n * LANES : (n + 1) * LANES]


def attend(where, parts, head):
    length = sum(p.shape[0] for p in parts)
    block, bf16 = 256, jnp.bfloat16
    return pl.pallas_call(
        functools.partial(attend_kernel, head),
        out_shape=jax.ShapeDtypeStruct((length // LANES, LANES, LANES), bf16),
        in_specs=[pl.BlockSpec(memory_space=pltpu.SMEM)] + [whole()] * 3,
        out_specs=whole(),
        scratch_shapes=[pltpu.VMEM((length, LANES), bf16)] * 3
        + [pltpu.VMEM((2, block, length), jnp.float32)],
        cost_estimate=pl.CostEstimate(
            flops=4 * length * length * LANES, bytes_accessed=8000000, transcendentals=length * length
        ),
        compiler_params=pltpu.CompilerParams(vmem_limit_bytes=32 << 20),
        name="attend",
    )(where, *parts)


def proj_kernel(where_ref, heads_ref, own_ref, left_ref, right_ref, far_ref,
                mine_ref, other_ref, h_ref, p_ref):
    own = mine_ref.shape[0]
    core = where_ref[8]
    head = own_ref.shape[1]
    for i in range(8):
        piece = (own_ref, left_ref, right_ref, far_ref)[i // 2][i % 2]
        p_ref[i * LANES : i * LANES + head, :] = piece
        p_ref[i * LANES + head : (i + 1) * LANES, :] = jnp.zeros(
            (LANES - head, p_ref.shape[1]), p_ref.dtype
        )
        h_ref[:, i * LANES : (i + 1) * LANES] = heads_ref[where_ref[i]]
    for target, first in ((other_ref, (1 - core) * own), (mine_ref, core * own)):
        left = h_ref[pl.ds(pl.multiple_of(first, own), own), :]
        total = jnp.dot(left, p_ref[...], preferred_element_type=jnp.float32)
        target[...] = total.astype(target.dtype)


def project(where, heads, pieces, own, width):
    out = jax.ShapeDtypeStruct((own, width), jnp.bfloat16)
    return pl.pallas_call(
        proj_kernel,
        out_shape=(out, out),
        in_specs=[pl.BlockSpec(memory_space=pltpu.SMEM)] + [whole()] * 5,
        out_specs=(whole(), whole()),
        scratch_shapes=[
            pltpu.VMEM((2 * own, 8 * LANES), jnp.bfloat16),
            pltpu.VMEM((8 * LANES, width), jnp.bfloat16),
        ],
        cost_estimate=pl.CostEstimate(flops=740000000, bytes_accessed=4000000, transcendentals=0),
        compiler_params=pltpu.CompilerParams(vmem_limit_bytes=24 << 20),
        name="project",
    )(where, heads, *pieces)


def ln2_kernel(x_ref, mine_ref, other_ref, pbias_ref, gain_ref, bias_ref, ln2_ref, resid_ref):
    f32 = jnp.float32
    total = mine_ref[...].astype(f32) + other_ref[...].astype(f32)
    resid = x_ref[...].astype(f32) + total + row(pbias_ref).astype(f32)
    resid_ref[...] = resid
    ln2_ref[...] = norm_rows(resid, row(gain_ref), row(bias_ref)).astype(ln2_ref.dtype)


def second_norm(x, mine, other, pbias, gain, bias):
    return pl.pallas_call(
        ln2_kernel,
        out_shape=(
            jax.ShapeDtypeStruct(x.shape, jnp.bfloat16),
            jax.ShapeDtypeStruct(x.shape, jnp.float32),
        ),
        in_specs=[whole()] * 6,
        out_specs=(whole(), whole()),
        cost_estimate=pl.CostEstimate(flops=12 * x.size, bytes_accessed=12 * x.size, transcendentals=0),
        compiler_params=pltpu.CompilerParams(vmem_limit_bytes=8 << 20),
        name="second_norm",
    )(x, mine, other, pbias, gain, bias)


def pass_kernel(core_ref, right_ref, left_ref, via_ref, to_right_ref, to_left_ref):
    via = via_ref[...].astype(jnp.float32)
    none = jnp.zeros_like(via)
    first = core_ref[0] == 0
    to_right_ref[...] = (right_ref[...] + jnp.where(first, via, none)).astype(to_right_ref.dtype)
    to_left_ref[...] = (left_ref[...] + jnp.where(first, none, via)).astype(to_left_ref.dtype)


def pass_on(core, right, left, via):
    out = jax.ShapeDtypeStruct(right.shape, via.dtype)
    return pl.pallas_call(
        pass_kernel,
        out_shape=(out, out),
        in_specs=[pl.BlockSpec(memory_space=pltpu.SMEM)] + [whole()] * 3,
        out_specs=(whole(), whole()),
        cost_estimate=pl.CostEstimate(flops=200000, bytes_accessed=1000000, transcendentals=0),
        compiler_params=pltpu.CompilerParams(vmem_limit_bytes=8 << 20),
        name="pass_on",
    )(core, right, left, via)


def gelu(x):
    return 0.5 * x * (1.0 + lax.erf(x * 0.7071067811865476))


def second_product(hidden, w2):
    return lax.dot_general(hidden, w2, (((1,), (1,)), ((), ())), preferred_element_type=jnp.float32)


def head_kernel(slab, own_ref, left_ref, right_ref, far_ref, w_ref,
                hidden, w2, pfar_ref, rows, w1, b1, sem1, sem2, sem3):
    f32 = jnp.float32
    own = own_ref.shape[0]
    hid = w_ref.shape[3]
    loads1 = [[], [], [], []]
    loads2 = [[], [], [], []]
    for b in range(4):
        cols = pl.ds(b * hid, hid)
        for r in range(8):
            rows_r = pl.ds(r * slab, slab)
            loads1[b].append(
                pltpu.make_async_copy(w_ref.at[r, b, pl.ds(0, slab)], w1.at[rows_r, cols], sem1.at[b, r])
            )
            loads2[b].append(
                pltpu.make_async_copy(w_ref.at[r, b, pl.ds(slab, slab)], w2.at[rows_r, cols], sem2.at[b, r])
            )
        loads1[b].append(
            pltpu.make_async_copy(w_ref.at[0, b, pl.ds(2 * slab, 16)], b1.at[b], sem3.at[b])
        )
    queue = loads1 + loads2
    for group in queue[:2]:
        for copy in group:
            copy.start()
    rows[:own] = own_ref[...]
    rows[own : 2 * own] = left_ref[...]
    rows[2 * own : 3 * own] = right_ref[...]
    rows[3 * own :] = far_ref[...]
    for b in range(4):
        for copy in loads1[b]:
            copy.wait()
        for group in queue[b + 2 : b + 3] if b < 3 else queue[5:]:
            for copy in group:
                copy.start()
        cols = slice(b * hid, (b + 1) * hid)
        for m in range(2):
            part = slice(2 * own * m, 2 * own * (m + 1))
            value = jnp.dot(rows[part], w1[:, cols], preferred_element_type=f32)
            value = value + b1[b, 0:1].astype(f32)
            hidden[part, cols] = gelu(value).astype(hidden.dtype)
    for group in loads2:
        for copy in group:
            copy.wait()
    pfar_ref[...] = second_product(hidden[3 * own :], w2[...]).astype(pfar_ref.dtype)


def mlp_head(pieces, weights, slab):
    own, width = pieces[0].shape
    hid = weights.shape[3]
    bf16 = jnp.bfloat16
    return pl.pallas_call(
        functools.partial(head_kernel, slab),
        out_shape=(
            jax.ShapeDtypeStruct((4 * own, 4 * hid), bf16),
            jax.ShapeDtypeStruct((width, 4 * hid), bf16),
            jax.ShapeDtypeStruct((own, width), bf16),
        ),
        in_specs=[whole()] * 4 + [pl.BlockSpec(memory_space=pltpu.HBM)],
        out_specs=(whole(),) * 3,
        scratch_shapes=[
            pltpu.VMEM((4 * own, width), bf16),
            pltpu.VMEM((width, 4 * hid), bf16),
            pltpu.VMEM((4, 16, hid), bf16),
            pltpu.SemaphoreType.DMA((4, 8)),
            pltpu.SemaphoreType.DMA((4, 8)),
            pltpu.SemaphoreType.DMA((4,)),
        ],
        cost_estimate=pl.CostEstimate(flops=2770000000, bytes_accessed=12000000, transcendentals=800000),
        compiler_params=pltpu.CompilerParams(vmem_limit_bytes=46 << 20),
        name="mlp_head",
    )(*pieces, weights)


def sides_kernel(hidden, w2, left_ref, right_ref):
    own = left_ref.shape[0]
    out = second_product(hidden[own : 3 * own], w2[...])
    left_ref[...] = out[:own]
    right_ref[...] = out[own:]


def mlp_sides(hidden, w2):
    out = jax.ShapeDtypeStruct((hidden.shape[0] // 4, w2.shape[0]), jnp.float32)
    return pl.pallas_call(
        sides_kernel,
        out_shape=(out, out),
        in_specs=[whole()] * 2,
        out_specs=(whole(), whole()),
        cost_estimate=pl.CostEstimate(flops=1100000000, bytes_accessed=8000000, transcendentals=0),
        compiler_params=pltpu.CompilerParams(vmem_limit_bytes=24 << 20),
        name="mlp_sides",
    )(hidden, w2)


def own_kernel(hidden, w2, resid_ref, bias_ref, out_ref):
    own = out_ref.shape[0]
    out = second_product(hidden[:own], w2[...])
    out_ref[...] = resid_ref[...] + out + row(bias_ref).astype(jnp.float32)


def mlp_own(hidden, w2, resid, bias):
    return pl.pallas_call(
        own_kernel,
        out_shape=jax.ShapeDtypeStruct(resid.shape, jnp.float32),
        in_specs=[whole()] * 4,
        out_specs=whole(),
        cost_estimate=pl.CostEstimate(flops=550000000, bytes_accessed=8000000, transcendentals=0),
        compiler_params=pltpu.CompilerParams(vmem_limit_bytes=24 << 20),
        name="mlp_own",
    )(hidden, w2, resid, bias)


def layer(
    tokens_in,
    ln1_gain,
    ln1_bias,
    qkv_weight,
    qkv_bias,
    proj_weight,
    proj_bias,
    ln2_gain,
    ln2_bias,
    fc1_weight,
    fc1_bias,
    fc2_weight,
    fc2_bias,
):
    f32, bf16 = jnp.float32, jnp.bfloat16
    own = tokens_in.shape[0]
    width = tokens_in.shape[1]
    head = proj_weight.shape[0]
    slab = qkv_weight.shape[0]
    hid = fc1_weight.shape[1]
    core = lax.axis_index("core")
    z, yh = lax.axis_index("z"), lax.axis_index("yh")
    x, yl = lax.axis_index("x"), lax.axis_index("yl")

    pair = jnp.stack([qkv_weight, shift(qkv_weight, dyh=1)])
    low = shift(pair, dz=1)
    high = shift(pair, dz=3)
    bias_rows = jnp.broadcast_to(fc1_bias[None], (16, hid))
    stack = jnp.concatenate([fc1_weight, fc2_weight, bias_rows], axis=0)
    mlp = lax.all_gather(stack, ("z", "yh", "yl", "core"), axis=0, tiled=False)
    mlp = mlp.reshape(8, 4, stack.shape[0], hid)

    far = shift(low, dz=1)
    where = [(z + 4 - dz) % 4 * 2 + (yh + j) % 2 for dz in (0, 1, 3, 2) for j in range(2)]
    where = jnp.stack(where).astype(jnp.int32)
    w_own = place(where, qkv_bias, (pair, low, high, far))
    w_other = shift(w_own, dc=1)

    p_rows = jnp.stack([proj_weight, shift(proj_weight, dyh=1)])
    p_rows = [p_rows] + [shift(p_rows, dz=dz) for dz in (1, 3, 2)]
    which = []
    for r in range(8):
        dz = (z + 4 - r // 2) % 4
        which.append(jnp.where(dz > 1, 5 - dz, dz) * 2 + (r % 2 + yh) % 2)
    proj_own = place_proj(jnp.stack(which).astype(jnp.int32), p_rows)
    p_side = shift(proj_own, dyl=1)

    ln1 = first_norm(tokens_in, ln1_gain, ln1_bias)
    left = shift(ln1, dx=1)
    right = shift(ln1, dx=3)
    side = shift(ln1, dyl=1)
    side_left = shift(side, dx=1)
    side_right = shift(side, dx=3)
    far = shift(left, dx=1)
    side_far = shift(side_right, dx=3)
    near = (ln1, left, right, side)
    rest = (side_left, side_right, far, side_far)
    other = qkv_part(rest, w_other)
    swapped = [shift(qkv_part(near, w_other), dc=1), shift(other, dc=1)]
    p_side, _ = lax.optimization_barrier((p_side, other))
    p_pair = jnp.stack([proj_own, p_side])
    p_left = shift(p_pair, dx=1)
    p_right = shift(p_pair, dx=3)
    p_far = shift_far(jnp.where(core == 0, p_left, p_right))
    parts = [qkv_part(near + rest, w_own)] + swapped
    spots = [(0, 0), (1, 0), (3, 0), (0, 1), (1, 1), (3, 1), (2, 0), (2, 1)]
    places = [
        ((x + 4 - dx) % 4 * 2 + (yl + j) % 2) * 2 + (core + k) % 2 for k in range(2) for dx, j in spots
    ]
    attn = attend(jnp.stack(places).astype(jnp.int32), parts, head)
    heads = lax.all_to_all(attn.reshape(8, 2 * own, LANES), ("x", "yl"), 0, 0, tiled=True)
    order = [(0, 0), (0, 1), (1, 0), (1, 1), (3, 0), (3, 1), (2, 0), (2, 1)]
    where = [(x + 4 - dx) % 4 * 2 + (yl + j) % 2 for dx, j in order]
    where = jnp.stack(where + [core]).astype(jnp.int32)
    proj_sets = (p_pair, p_left, p_right, p_far)
    mine, other = project(where, heads, proj_sets, own, width)
    other = shift(other, dc=1)
    ln2, resid = second_norm(tokens_in, mine, other, proj_bias, ln2_gain, ln2_bias)

    left = shift(ln2, dx=1)
    right = shift(ln2, dx=3)
    far = shift_far(jnp.where(core == 0, left, right))
    hidden, w2, p_far = mlp_head((ln2, left, right, far), mlp, slab)

    via = shift_far(p_far)
    o_left, o_right = mlp_sides(hidden, w2)
    to_right, to_left = pass_on(core.astype(jnp.int32)[None], o_right, o_left, via)
    from_left = shift(to_right, dx=1)
    from_right = shift(to_left, dx=3)
    mine = mlp_own(hidden, w2, resid, fc2_bias)
    return (mine + from_left.astype(f32) + from_right.astype(f32)).astype(bf16)


def solution(mesh):
    fine = Mesh(np.asarray(mesh.devices).reshape(SIZES), AXES)
    in_specs = (
        P(AXES, None),
        P(),
        P(),
        P(ROW, COL),
        P(COL),
        P(COL, ROW),
        P(),
        P(),
        P(),
        P(ROW, COL),
        P(COL),
        P(ROW, COL),
        P(),
    )
    return jax.shard_map(layer, mesh=fine, in_specs=in_specs, out_specs=P(AXES, None), check_vma=False)
```

```python
import functools
import itertools

import jax
import jax.numpy as jnp
import numpy as np
from jax import lax
from jax.experimental import pallas as pl
from jax.experimental.pallas import tpu as pltpu
from jax.sharding import Mesh
from jax.sharding import PartitionSpec as P


LANES = 128
AXES = ("z", "yh", "x", "yl", "core")
SIZES = (4, 2, 4, 2, 2)
ROW = ("z", "yh")
COL = ("x", "yl", "core")


def shift(value, dz=0, dyh=0, dx=0, dyl=0, dc=0):
    pairs = []
    for place in itertools.product(*[range(n) for n in SIZES]):
        target = [(p + d) % n for p, d, n in zip(place, (dz, dyh, dx, dyl, dc), SIZES)]
        pairs.append(
            (int(np.ravel_multi_index(place, SIZES)), int(np.ravel_multi_index(target, SIZES)))
        )
    return lax.ppermute(value, AXES, pairs)


def whole():
    return pl.BlockSpec(memory_space=pltpu.VMEM)


def norm_rows(values, gain, bias):
    mean = jnp.mean(values, axis=-1, keepdims=True)
    centred = values - mean
    var = jnp.mean(centred * centred, axis=-1, keepdims=True)
    return centred * lax.rsqrt(var + 1e-06) * gain.astype(jnp.float32) + bias.astype(jnp.float32)


def row(ref):
    return ref[...].reshape(1, ref.shape[0])


def ln1_kernel(x_ref, gain_ref, bias_ref, out_ref):
    values = x_ref[...].astype(jnp.float32)
    out_ref[...] = norm_rows(values, row(gain_ref), row(bias_ref)).astype(out_ref.dtype)


def first_norm(x, gain, bias):
    return pl.pallas_call(
        ln1_kernel,
        out_shape=jax.ShapeDtypeStruct(x.shape, jnp.bfloat16),
        in_specs=[whole()] * 3,
        out_specs=whole(),
        cost_estimate=pl.CostEstimate(flops=10 * x.size, bytes_accessed=4 * x.size, transcendentals=0),
        compiler_params=pltpu.CompilerParams(vmem_limit_bytes=8 << 20),
        name="first_norm",
    )(x, gain, bias)


def spread(values, head, ones):
    rows = values.shape[0]
    gap = jnp.zeros((rows, LANES - head), values.dtype)
    lane = lax.broadcasted_iota(jnp.int32, (rows, LANES - head), 1)
    last = jnp.where(lane == 0, jnp.ones_like(gap), gap) if ones else gap
    q, k, v = (values[:, n * head : (n + 1) * head] for n in range(3))
    return jnp.concatenate([q, gap, k, gap, v, last], axis=1)


def place_kernel(head, where_ref, bias_ref, own_ref, low_ref, high_ref, far_ref, w_ref):
    slab = own_ref.shape[1]
    for n, ref in enumerate((own_ref, low_ref, high_ref, far_ref)):
        for j in range(2):
            first = pl.multiple_of(where_ref[2 * n + j] * slab, 16)
            value = spread(ref[j].astype(jnp.float32), head, False)
            w_ref[pl.ds(first, slab), :] = value.astype(w_ref.dtype)
    bias = spread(row(bias_ref).astype(jnp.float32), head, True)
    w_ref[8 * slab :, :] = jnp.broadcast_to(bias, (16, bias.shape[1])).astype(w_ref.dtype)


def place(where, bias, pieces):
    _, slab, cols = pieces[0].shape
    return pl.pallas_call(
        functools.partial(place_kernel, cols // 3),
        out_shape=jax.ShapeDtypeStruct((8 * slab + 16, 3 * LANES), jnp.bfloat16),
        in_specs=[pl.BlockSpec(memory_space=pltpu.SMEM)] + [whole()] * 5,
        out_specs=whole(),
        cost_estimate=pl.CostEstimate(flops=1000000, bytes_accessed=3000000, transcendentals=0),
        compiler_params=pltpu.CompilerParams(vmem_limit_bytes=12 << 20),
        name="place_rows",
    )(where, bias, *pieces)


def place_proj_kernel(which_ref, own_ref, low_ref, high_ref, far_ref, out_ref, held):
    slab = own_ref.shape[2]
    for n, ref in enumerate((own_ref, low_ref, high_ref, far_ref)):
        for j in range(2):
            held[2 * n + j] = ref[j].astype(jnp.float32)
    for r in range(8):
        out_ref[:, r * slab : (r + 1) * slab] = held[which_ref[r]].astype(out_ref.dtype)


def place_proj(which, pieces):
    _, head, slab = pieces[0].shape
    return pl.pallas_call(
        place_proj_kernel,
        out_shape=jax.ShapeDtypeStruct((head, 8 * slab), jnp.bfloat16),
        in_specs=[pl.BlockSpec(memory_space=pltpu.SMEM)] + [whole()] * 4,
        out_specs=whole(),
        scratch_shapes=[pltpu.VMEM((8, head, slab), jnp.float32)],
        cost_estimate=pl.CostEstimate(flops=100000, bytes_accessed=1000000, transcendentals=0),
        compiler_params=pltpu.CompilerParams(vmem_limit_bytes=8 << 20),
        name="place_proj",
    )(which, *pieces)


def qkv_kernel(count, *refs):
    pieces, (w_ref, out_ref, rows) = refs[:count], refs[count:]
    width = rows.shape[1]
    first = 0
    for ref in pieces:
        rows[first : first + ref.shape[0], :] = ref[...]
        first += ref.shape[0]
    bias = w_ref[width : width + 1, :].astype(jnp.float32)
    value = jnp.dot(rows[...], w_ref[:width, :], preferred_element_type=jnp.float32)
    out_ref[...] = (value + bias).astype(out_ref.dtype)


def qkv_part(pieces, weights):
    rows = sum(p.shape[0] for p in pieces)
    cols = weights.shape[1]
    return pl.pallas_call(
        functools.partial(qkv_kernel, len(pieces)),
        out_shape=jax.ShapeDtypeStruct((rows, cols), jnp.bfloat16),
        in_specs=[whole()] * (len(pieces) + 1),
        out_specs=whole(),
        scratch_shapes=[pltpu.VMEM((rows, pieces[0].shape[1]), jnp.bfloat16)],
        cost_estimate=pl.CostEstimate(
            flops=2 * rows * cols * weights.shape[0], bytes_accessed=4000000, transcendentals=0
        ),
        compiler_params=pltpu.CompilerParams(vmem_limit_bytes=16 << 20),
        name="qkv_part",
    )(*pieces, weights)


def attend_kernel(head, where_ref, *refs):
    f32 = jnp.float32
    parts, (out_ref, q_ref, k_ref, v_ref, s_ref) = refs[:3], refs[3:]
    length = q_ref.shape[0]
    first = 0
    for ref in parts:
        rows = slice(first, first + ref.shape[0])
        q_ref[rows, :] = ref[:, :LANES]
        k_ref[rows, :] = ref[:, LANES : 2 * LANES]
        v_ref[rows, :] = ref[:, 2 * LANES :]
        first += ref.shape[0]
    block = s_ref.shape[1]
    steps = length // block
    scale = 1.4426950408889634 / head**0.5

    def scores(i):
        s_ref[i % 2] = lax.dot_general(
            q_ref[i * block : (i + 1) * block, :],
            k_ref[...],
            (((1,), (1,)), ((), ())),
            preferred_element_type=f32,
        )

    scores(0)
    for i in range(steps):
        value = s_ref[i % 2]
        if i + 1 < steps:
            scores(i + 1)
        top = jnp.max(value, axis=-1, keepdims=True)
        expo = jnp.exp2((value - top) * scale).astype(jnp.bfloat16)
        mixed = jnp.dot(expo, v_ref[...], preferred_element_type=f32)
        mixed = (mixed / mixed[:, head : head + 1]).astype(out_ref.dtype)
        for n in range(block // LANES):
            out_ref[where_ref[i * (block // LANES) + n]] = mixed[n * LANES : (n + 1) * LANES]


def attend(where, parts, head):
    length = sum(p.shape[0] for p in parts)
    block, bf16 = 256, jnp.bfloat16
    return pl.pallas_call(
        functools.partial(attend_kernel, head),
        out_shape=jax.ShapeDtypeStruct((length // LANES, LANES, LANES), bf16),
        in_specs=[pl.BlockSpec(memory_space=pltpu.SMEM)] + [whole()] * 3,
        out_specs=whole(),
        scratch_shapes=[pltpu.VMEM((length, LANES), bf16)] * 3
        + [pltpu.VMEM((2, block, length), jnp.float32)],
        cost_estimate=pl.CostEstimate(
            flops=4 * length * length * LANES, bytes_accessed=8000000, transcendentals=length * length
        ),
        compiler_params=pltpu.CompilerParams(vmem_limit_bytes=32 << 20),
        name="attend",
    )(where, *parts)


def proj_kernel(where_ref, heads_ref, own_ref, left_ref, right_ref, fa_ref, fb_ref,
                mine_ref, other_ref, h_ref, p_ref):
    own = mine_ref.shape[0]
    core = where_ref[8]
    head = own_ref.shape[1]
    for i in range(8):
        piece = (own_ref, left_ref, right_ref)[i // 2][i % 2] if i < 6 else (fa_ref, fb_ref)[i % 2][...]
        p_ref[i * LANES : i * LANES + head, :] = piece
        p_ref[i * LANES + head : (i + 1) * LANES, :] = jnp.zeros(
            (LANES - head, p_ref.shape[1]), p_ref.dtype
        )
        h_ref[:, i * LANES : (i + 1) * LANES] = heads_ref[where_ref[i]]
    for target, first in ((other_ref, (1 - core) * own), (mine_ref, core * own)):
        left = h_ref[pl.ds(pl.multiple_of(first, own), own), :]
        total = jnp.dot(left, p_ref[...], preferred_element_type=jnp.float32)
        target[...] = total.astype(target.dtype)


def project(where, heads, pieces, own, width):
    out = jax.ShapeDtypeStruct((own, width), jnp.bfloat16)
    return pl.pallas_call(
        proj_kernel,
        out_shape=(out, out),
        in_specs=[pl.BlockSpec(memory_space=pltpu.SMEM)] + [whole()] * 6,
        out_specs=(whole(), whole()),
        scratch_shapes=[
            pltpu.VMEM((2 * own, 8 * LANES), jnp.bfloat16),
            pltpu.VMEM((8 * LANES, width), jnp.bfloat16),
        ],
        cost_estimate=pl.CostEstimate(flops=740000000, bytes_accessed=4000000, transcendentals=0),
        compiler_params=pltpu.CompilerParams(vmem_limit_bytes=24 << 20),
        name="project",
    )(where, heads, *pieces)


def ln2_kernel(x_ref, mine_ref, other_ref, pbias_ref, gain_ref, bias_ref, ln2_ref, resid_ref):
    f32 = jnp.float32
    total = mine_ref[...].astype(f32) + other_ref[...].astype(f32)
    resid = x_ref[...].astype(f32) + total + row(pbias_ref).astype(f32)
    resid_ref[...] = resid
    ln2_ref[...] = norm_rows(resid, row(gain_ref), row(bias_ref)).astype(ln2_ref.dtype)


def second_norm(x, mine, other, pbias, gain, bias):
    return pl.pallas_call(
        ln2_kernel,
        out_shape=(
            jax.ShapeDtypeStruct(x.shape, jnp.bfloat16),
            jax.ShapeDtypeStruct(x.shape, jnp.float32),
        ),
        in_specs=[whole()] * 6,
        out_specs=(whole(), whole()),
        cost_estimate=pl.CostEstimate(flops=12 * x.size, bytes_accessed=12 * x.size, transcendentals=0),
        compiler_params=pltpu.CompilerParams(vmem_limit_bytes=8 << 20),
        name="second_norm",
    )(x, mine, other, pbias, gain, bias)


def pass_kernel(right_ref, via_a_ref, left_ref, via_b_ref, to_right_ref, to_left_ref):
    f32 = jnp.float32
    half = via_a_ref.shape[0]
    near, far = slice(0, half), slice(half, 2 * half)
    to_right_ref[near, :] = (right_ref[near, :] + via_a_ref[...].astype(f32)).astype(to_right_ref.dtype)
    to_right_ref[far, :] = right_ref[far, :].astype(to_right_ref.dtype)
    to_left_ref[near, :] = left_ref[near, :].astype(to_left_ref.dtype)
    to_left_ref[far, :] = (left_ref[far, :] + via_b_ref[...].astype(f32)).astype(to_left_ref.dtype)


def pass_on(right, via_a, left, via_b):
    out = jax.ShapeDtypeStruct(right.shape, via_a.dtype)
    return pl.pallas_call(
        pass_kernel,
        out_shape=(out, out),
        in_specs=[whole()] * 4,
        out_specs=(whole(), whole()),
        cost_estimate=pl.CostEstimate(flops=200000, bytes_accessed=1000000, transcendentals=0),
        compiler_params=pltpu.CompilerParams(vmem_limit_bytes=8 << 20),
        name="pass_on",
    )(right, via_a, left, via_b)


def gelu(x):
    return 0.5 * x * (1.0 + lax.erf(x * 0.7071067811865476))


def second_product(hidden, w2):
    return lax.dot_general(hidden, w2, (((1,), (1,)), ((), ())), preferred_element_type=jnp.float32)


def head_kernel(slab, own_ref, left_ref, right_ref, fa_ref, fb_ref, w_ref,
                hidden, w2, pfa_ref, pfb_ref, rows, w1, b1, sem1, sem2, sem3):
    f32 = jnp.float32
    own = own_ref.shape[0]
    hid = w_ref.shape[3]
    loads1 = [[], [], [], []]
    loads2 = [[], [], [], []]
    for b in range(4):
        cols = pl.ds(b * hid, hid)
        for r in range(8):
            rows_r = pl.ds(r * slab, slab)
            loads1[b].append(
                pltpu.make_async_copy(w_ref.at[r, b, pl.ds(0, slab)], w1.at[rows_r, cols], sem1.at[b, r])
            )
            loads2[b].append(
                pltpu.make_async_copy(w_ref.at[r, b, pl.ds(slab, slab)], w2.at[rows_r, cols], sem2.at[b, r])
            )
        loads1[b].append(
            pltpu.make_async_copy(w_ref.at[0, b, pl.ds(2 * slab, 16)], b1.at[b], sem3.at[b])
        )
    queue = loads1 + loads2
    for group in queue[:2]:
        for copy in group:
            copy.start()
    rows[:own] = own_ref[...]
    rows[own : 2 * own] = left_ref[...]
    rows[2 * own : 3 * own] = right_ref[...]
    rows[3 * own : 3 * own + own // 2] = fa_ref[...]
    rows[3 * own + own // 2 :] = fb_ref[...]
    for b in range(4):
        for copy in loads1[b]:
            copy.wait()
        for group in queue[b + 2 : b + 3] if b < 3 else queue[5:]:
            for copy in group:
                copy.start()
        cols = slice(b * hid, (b + 1) * hid)
        for m in range(2):
            part = slice(2 * own * m, 2 * own * (m + 1))
            value = jnp.dot(rows[part], w1[:, cols], preferred_element_type=f32)
            value = value + b1[b, 0:1].astype(f32)
            hidden[part, cols] = gelu(value).astype(hidden.dtype)
    for group in loads2:
        for copy in group:
            copy.wait()
    half = own // 2
    out = second_product(hidden[3 * own :], w2[...])
    pfa_ref[...] = out[:half].astype(pfa_ref.dtype)
    pfb_ref[...] = out[half:].astype(pfb_ref.dtype)


def mlp_head(pieces, weights, slab):
    own, width = pieces[0].shape
    hid = weights.shape[3]
    bf16 = jnp.bfloat16
    far = jax.ShapeDtypeStruct((own // 2, width), bf16)
    return pl.pallas_call(
        functools.partial(head_kernel, slab),
        out_shape=(
            jax.ShapeDtypeStruct((4 * own, 4 * hid), bf16),
            jax.ShapeDtypeStruct((width, 4 * hid), bf16),
            far,
            far,
        ),
        in_specs=[whole()] * 5 + [pl.BlockSpec(memory_space=pltpu.HBM)],
        out_specs=(whole(),) * 4,
        scratch_shapes=[
            pltpu.VMEM((4 * own, width), bf16),
            pltpu.VMEM((width, 4 * hid), bf16),
            pltpu.VMEM((4, 16, hid), bf16),
            pltpu.SemaphoreType.DMA((4, 8)),
            pltpu.SemaphoreType.DMA((4, 8)),
            pltpu.SemaphoreType.DMA((4,)),
        ],
        cost_estimate=pl.CostEstimate(flops=2770000000, bytes_accessed=12000000, transcendentals=800000),
        compiler_params=pltpu.CompilerParams(vmem_limit_bytes=46 << 20),
        name="mlp_head",
    )(*pieces, weights)


def sides_kernel(hidden, w2, left_ref, right_ref):
    own = left_ref.shape[0]
    out = second_product(hidden[own : 3 * own], w2[...])
    left_ref[...] = out[:own]
    right_ref[...] = out[own:]


def mlp_sides(hidden, w2):
    out = jax.ShapeDtypeStruct((hidden.shape[0] // 4, w2.shape[0]), jnp.float32)
    return pl.pallas_call(
        sides_kernel,
        out_shape=(out, out),
        in_specs=[whole()] * 2,
        out_specs=(whole(), whole()),
        cost_estimate=pl.CostEstimate(flops=1100000000, bytes_accessed=8000000, transcendentals=0),
        compiler_params=pltpu.CompilerParams(vmem_limit_bytes=24 << 20),
        name="mlp_sides",
    )(hidden, w2)


def own_kernel(hidden, w2, resid_ref, bias_ref, out_ref):
    own = out_ref.shape[0]
    out = second_product(hidden[:own], w2[...])
    out_ref[...] = resid_ref[...] + out + row(bias_ref).astype(jnp.float32)


def mlp_own(hidden, w2, resid, bias):
    return pl.pallas_call(
        own_kernel,
        out_shape=jax.ShapeDtypeStruct(resid.shape, jnp.float32),
        in_specs=[whole()] * 4,
        out_specs=whole(),
        cost_estimate=pl.CostEstimate(flops=550000000, bytes_accessed=8000000, transcendentals=0),
        compiler_params=pltpu.CompilerParams(vmem_limit_bytes=24 << 20),
        name="mlp_own",
    )(hidden, w2, resid, bias)


def layer(
    tokens_in,
    ln1_gain,
    ln1_bias,
    qkv_weight,
    qkv_bias,
    proj_weight,
    proj_bias,
    ln2_gain,
    ln2_bias,
    fc1_weight,
    fc1_bias,
    fc2_weight,
    fc2_bias,
):
    f32, bf16 = jnp.float32, jnp.bfloat16
    own = tokens_in.shape[0]
    width = tokens_in.shape[1]
    head = proj_weight.shape[0]
    slab = qkv_weight.shape[0]
    hid = fc1_weight.shape[1]
    core = lax.axis_index("core")
    z, yh = lax.axis_index("z"), lax.axis_index("yh")
    x, yl = lax.axis_index("x"), lax.axis_index("yl")

    pair = jnp.stack([qkv_weight, shift(qkv_weight, dyh=1)])
    low = shift(pair, dz=1)
    high = shift(pair, dz=3)
    bias_rows = jnp.broadcast_to(fc1_bias[None], (16, hid))
    stack = jnp.concatenate([fc1_weight, fc2_weight, bias_rows], axis=0)
    mlp = lax.all_gather(stack, ("z", "yh", "yl", "core"), axis=0, tiled=False)
    mlp = mlp.reshape(8, 4, stack.shape[0], hid)

    far = shift(low, dz=1)
    where = [(z + 4 - dz) % 4 * 2 + (yh + j) % 2 for dz in (0, 1, 3, 2) for j in range(2)]
    where = jnp.stack(where).astype(jnp.int32)
    w_own = place(where, qkv_bias, (pair, low, high, far))
    w_other = shift(w_own, dc=1)

    p_rows = jnp.stack([proj_weight, shift(proj_weight, dyh=1)])
    p_rows = [p_rows] + [shift(p_rows, dz=dz) for dz in (1, 3, 2)]
    which = []
    for r in range(8):
        dz = (z + 4 - r // 2) % 4
        which.append(jnp.where(dz > 1, 5 - dz, dz) * 2 + (r % 2 + yh) % 2)
    proj_own = place_proj(jnp.stack(which).astype(jnp.int32), p_rows)
    p_side = shift(proj_own, dyl=1)

    ln1 = first_norm(tokens_in, ln1_gain, ln1_bias)
    left = shift(ln1, dx=1)
    right = shift(ln1, dx=3)
    side = shift(ln1, dyl=1)
    side_left = shift(side, dx=1)
    side_right = shift(side, dx=3)
    far = shift(left, dx=1)
    side_far = shift(side_right, dx=3)
    near = (ln1, left, right, side)
    rest = (side_left, side_right, far, side_far)
    other = qkv_part(rest, w_other)
    swapped = [shift(qkv_part(near, w_other), dc=1), shift(other, dc=1)]
    mine = qkv_part(near + rest, w_own)
    p_side, _ = lax.optimization_barrier((p_side, mine))
    p_pair = jnp.stack([proj_own, p_side])
    p_left = shift(p_pair, dx=1)
    p_right = shift(p_pair, dx=3)
    p_fa = shift(p_left[0], dx=1)
    p_fb = shift(p_right[1], dx=3)
    parts = [mine] + swapped
    spots = [(0, 0), (1, 0), (3, 0), (0, 1), (1, 1), (3, 1), (2, 0), (2, 1)]
    places = [
        ((x + 4 - dx) % 4 * 2 + (yl + j) % 2) * 2 + (core + k) % 2 for k in range(2) for dx, j in spots
    ]
    attn = attend(jnp.stack(places).astype(jnp.int32), parts, head)
    heads = lax.all_to_all(attn.reshape(8, 2 * own, LANES), ("x", "yl"), 0, 0, tiled=True)
    order = [(0, 0), (0, 1), (1, 0), (1, 1), (3, 0), (3, 1), (2, 0), (2, 1)]
    where = [(x + 4 - dx) % 4 * 2 + (yl + j) % 2 for dx, j in order]
    where = jnp.stack(where + [core]).astype(jnp.int32)
    proj_sets = (p_pair, p_left, p_right, p_fa, p_fb)
    mine, other = project(where, heads, proj_sets, own, width)
    other = shift(other, dc=1)
    ln2, resid = second_norm(tokens_in, mine, other, proj_bias, ln2_gain, ln2_bias)

    left = shift(ln2, dx=1)
    right = shift(ln2, dx=3)
    half = own // 2
    far_a = shift(left[:half], dx=1)
    far_b = shift(right[half:], dx=3)
    hidden, w2, fa, fb = mlp_head((ln2, left, right, far_a, far_b), mlp, slab)

    via_a = shift(fa, dx=1)
    via_b = shift(fb, dx=3)
    o_left, o_right = mlp_sides(hidden, w2)
    to_right, to_left = pass_on(o_right, via_a, o_left, via_b)
    from_left = shift(to_right, dx=1)
    from_right = shift(to_left, dx=3)
    mine = mlp_own(hidden, w2, resid, fc2_bias)
    return (mine + from_left.astype(f32) + from_right.astype(f32)).astype(bf16)


def solution(mesh):
    fine = Mesh(np.asarray(mesh.devices).reshape(SIZES), AXES)
    in_specs = (
        P(AXES, None),
        P(),
        P(),
        P(ROW, COL),
        P(COL),
        P(COL, ROW),
        P(),
        P(),
        P(),
        P(ROW, COL),
        P(COL),
        P(ROW, COL),
        P(),
    )
    return jax.shard_map(layer, mesh=fine, in_specs=in_specs, out_specs=P(AXES, None), check_vma=False)
```

```python
import functools
import itertools

import jax
import jax.numpy as jnp
import numpy as np
from jax import lax
from jax.experimental import pallas as pl
from jax.experimental.pallas import tpu as pltpu
from jax.sharding import Mesh
from jax.sharding import PartitionSpec as P


LANES = 128
AXES = ("z", "yh", "x", "yl", "core")
SIZES = (4, 2, 4, 2, 2)
ROW = ("z", "yh")
COL = ("x", "yl", "core")


def shift(value, dz=0, dyh=0, dx=0, dyl=0, dc=0):
    pairs = []
    for place in itertools.product(*[range(n) for n in SIZES]):
        target = [(p + d) % n for p, d, n in zip(place, (dz, dyh, dx, dyl, dc), SIZES)]
        pairs.append(
            (int(np.ravel_multi_index(place, SIZES)), int(np.ravel_multi_index(target, SIZES)))
        )
    return lax.ppermute(value, AXES, pairs)


def whole():
    return pl.BlockSpec(memory_space=pltpu.VMEM)


def norm_rows(values, gain, bias):
    mean = jnp.mean(values, axis=-1, keepdims=True)
    centred = values - mean
    var = jnp.mean(centred * centred, axis=-1, keepdims=True)
    return centred * lax.rsqrt(var + 1e-06) * gain.astype(jnp.float32) + bias.astype(jnp.float32)


def row(ref):
    return ref[...].reshape(1, ref.shape[0])


def ln1_kernel(x_ref, gain_ref, bias_ref, out_ref):
    values = x_ref[...].astype(jnp.float32)
    out_ref[...] = norm_rows(values, row(gain_ref), row(bias_ref)).astype(out_ref.dtype)


def first_norm(x, gain, bias):
    return pl.pallas_call(
        ln1_kernel,
        out_shape=jax.ShapeDtypeStruct(x.shape, jnp.bfloat16),
        in_specs=[whole()] * 3,
        out_specs=whole(),
        cost_estimate=pl.CostEstimate(flops=10 * x.size, bytes_accessed=4 * x.size, transcendentals=0),
        compiler_params=pltpu.CompilerParams(vmem_limit_bytes=8 << 20),
        name="first_norm",
    )(x, gain, bias)


def spread(values, head, ones):
    rows = values.shape[0]
    gap = jnp.zeros((rows, LANES - head), values.dtype)
    lane = lax.broadcasted_iota(jnp.int32, (rows, LANES - head), 1)
    last = jnp.where(lane == 0, jnp.ones_like(gap), gap) if ones else gap
    q, k, v = (values[:, n * head : (n + 1) * head] for n in range(3))
    return jnp.concatenate([q, gap, k, gap, v, last], axis=1)


def place_kernel(head, where_ref, bias_ref, own_ref, low_ref, high_ref, far_ref, w_ref):
    slab = own_ref.shape[1]
    for n, ref in enumerate((own_ref, low_ref, high_ref, far_ref)):
        for j in range(2):
            first = pl.multiple_of(where_ref[2 * n + j] * slab, 16)
            value = spread(ref[j].astype(jnp.float32), head, False)
            w_ref[pl.ds(first, slab), :] = value.astype(w_ref.dtype)
    bias = spread(row(bias_ref).astype(jnp.float32), head, True)
    w_ref[8 * slab :, :] = jnp.broadcast_to(bias, (16, bias.shape[1])).astype(w_ref.dtype)


def place(where, bias, pieces):
    _, slab, cols = pieces[0].shape
    return pl.pallas_call(
        functools.partial(place_kernel, cols // 3),
        out_shape=jax.ShapeDtypeStruct((8 * slab + 16, 3 * LANES), jnp.bfloat16),
        in_specs=[pl.BlockSpec(memory_space=pltpu.SMEM)] + [whole()] * 5,
        out_specs=whole(),
        cost_estimate=pl.CostEstimate(flops=1000000, bytes_accessed=3000000, transcendentals=0),
        compiler_params=pltpu.CompilerParams(vmem_limit_bytes=12 << 20),
        name="place_rows",
    )(where, bias, *pieces)


def place_proj_kernel(which_ref, own_ref, low_ref, high_ref, far_ref, out_ref, held):
    slab = own_ref.shape[2]
    for n, ref in enumerate((own_ref, low_ref, high_ref, far_ref)):
        for j in range(2):
            held[2 * n + j] = ref[j].astype(jnp.float32)
    for r in range(8):
        out_ref[:, r * slab : (r + 1) * slab] = held[which_ref[r]].astype(out_ref.dtype)


def place_proj(which, pieces):
    _, head, slab = pieces[0].shape
    return pl.pallas_call(
        place_proj_kernel,
        out_shape=jax.ShapeDtypeStruct((head, 8 * slab), jnp.bfloat16),
        in_specs=[pl.BlockSpec(memory_space=pltpu.SMEM)] + [whole()] * 4,
        out_specs=whole(),
        scratch_shapes=[pltpu.VMEM((8, head, slab), jnp.float32)],
        cost_estimate=pl.CostEstimate(flops=100000, bytes_accessed=1000000, transcendentals=0),
        compiler_params=pltpu.CompilerParams(vmem_limit_bytes=8 << 20),
        name="place_proj",
    )(which, *pieces)


def qkv_kernel(count, *refs):
    pieces, (w_ref, out_ref, rows) = refs[:count], refs[count:]
    width = rows.shape[1]
    first = 0
    for ref in pieces:
        rows[first : first + ref.shape[0], :] = ref[...]
        first += ref.shape[0]
    bias = w_ref[width : width + 1, :].astype(jnp.float32)
    value = jnp.dot(rows[...], w_ref[:width, :], preferred_element_type=jnp.float32)
    out_ref[...] = (value + bias).astype(out_ref.dtype)


def qkv_part(pieces, weights):
    rows = sum(p.shape[0] for p in pieces)
    cols = weights.shape[1]
    return pl.pallas_call(
        functools.partial(qkv_kernel, len(pieces)),
        out_shape=jax.ShapeDtypeStruct((rows, cols), jnp.bfloat16),
        in_specs=[whole()] * (len(pieces) + 1),
        out_specs=whole(),
        scratch_shapes=[pltpu.VMEM((rows, pieces[0].shape[1]), jnp.bfloat16)],
        cost_estimate=pl.CostEstimate(
            flops=2 * rows * cols * weights.shape[0], bytes_accessed=4000000, transcendentals=0
        ),
        compiler_params=pltpu.CompilerParams(vmem_limit_bytes=16 << 20),
        name="qkv_part",
    )(*pieces, weights)


def attend_kernel(head, where_ref, *refs):
    f32 = jnp.float32
    parts, (out_ref, q_ref, k_ref, v_ref, s_ref) = refs[:3], refs[3:]
    length = q_ref.shape[0]
    first = 0
    for ref in parts:
        rows = slice(first, first + ref.shape[0])
        q_ref[rows, :] = ref[:, :LANES]
        k_ref[rows, :] = ref[:, LANES : 2 * LANES]
        v_ref[rows, :] = ref[:, 2 * LANES :]
        first += ref.shape[0]
    block = s_ref.shape[1]
    steps = length // block
    scale = 1.4426950408889634 / head**0.5

    def scores(i):
        s_ref[i % 2] = lax.dot_general(
            q_ref[i * block : (i + 1) * block, :],
            k_ref[...],
            (((1,), (1,)), ((), ())),
            preferred_element_type=f32,
        )

    scores(0)
    for i in range(steps):
        value = s_ref[i % 2]
        if i + 1 < steps:
            scores(i + 1)
        top = jnp.max(value, axis=-1, keepdims=True)
        expo = jnp.exp2((value - top) * scale).astype(jnp.bfloat16)
        mixed = jnp.dot(expo, v_ref[...], preferred_element_type=f32)
        mixed = (mixed / mixed[:, head : head + 1]).astype(out_ref.dtype)
        for n in range(block // LANES):
            out_ref[where_ref[i * (block // LANES) + n]] = mixed[n * LANES : (n + 1) * LANES]


def attend(where, parts, head):
    length = sum(p.shape[0] for p in parts)
    block, bf16 = 256, jnp.bfloat16
    return pl.pallas_call(
        functools.partial(attend_kernel, head),
        out_shape=jax.ShapeDtypeStruct((length // LANES, LANES, LANES), bf16),
        in_specs=[pl.BlockSpec(memory_space=pltpu.SMEM)] + [whole()] * 3,
        out_specs=whole(),
        scratch_shapes=[pltpu.VMEM((length, LANES), bf16)] * 3
        + [pltpu.VMEM((2, block, length), jnp.float32)],
        cost_estimate=pl.CostEstimate(
            flops=4 * length * length * LANES, bytes_accessed=8000000, transcendentals=length * length
        ),
        compiler_params=pltpu.CompilerParams(vmem_limit_bytes=32 << 20),
        name="attend",
    )(where, *parts)


def proj_kernel(where_ref, heads_ref, own_ref, left_ref, right_ref, fa_ref, fb_ref,
                mine_ref, other_ref, h_ref, p_ref):
    own = mine_ref.shape[0]
    core = where_ref[8]
    head = own_ref.shape[1]
    for i in range(8):
        piece = (own_ref, left_ref, right_ref)[i // 2][i % 2] if i < 6 else (fa_ref, fb_ref)[i % 2][...]
        p_ref[i * LANES : i * LANES + head, :] = piece
        p_ref[i * LANES + head : (i + 1) * LANES, :] = jnp.zeros(
            (LANES - head, p_ref.shape[1]), p_ref.dtype
        )
        h_ref[:, i * LANES : (i + 1) * LANES] = heads_ref[where_ref[i]]
    for target, first in ((other_ref, (1 - core) * own), (mine_ref, core * own)):
        left = h_ref[pl.ds(pl.multiple_of(first, own), own), :]
        total = jnp.dot(left, p_ref[...], preferred_element_type=jnp.float32)
        target[...] = total.astype(target.dtype)


def project(where, heads, pieces, own, width):
    out = jax.ShapeDtypeStruct((own, width), jnp.bfloat16)
    return pl.pallas_call(
        proj_kernel,
        out_shape=(out, out),
        in_specs=[pl.BlockSpec(memory_space=pltpu.SMEM)] + [whole()] * 6,
        out_specs=(whole(), whole()),
        scratch_shapes=[
            pltpu.VMEM((2 * own, 8 * LANES), jnp.bfloat16),
            pltpu.VMEM((8 * LANES, width), jnp.bfloat16),
        ],
        cost_estimate=pl.CostEstimate(flops=740000000, bytes_accessed=4000000, transcendentals=0),
        compiler_params=pltpu.CompilerParams(vmem_limit_bytes=24 << 20),
        name="project",
    )(where, heads, *pieces)


def ln2_kernel(x_ref, mine_ref, other_ref, pbias_ref, gain_ref, bias_ref, low_ref, high_ref, resid_ref):
    f32 = jnp.float32
    total = mine_ref[...].astype(f32) + other_ref[...].astype(f32)
    resid = x_ref[...].astype(f32) + total + row(pbias_ref).astype(f32)
    resid_ref[...] = resid
    half = low_ref.shape[0]
    value = norm_rows(resid, row(gain_ref), row(bias_ref)).astype(low_ref.dtype)
    low_ref[...] = value[:half]
    high_ref[...] = value[half:]


def second_norm(x, mine, other, pbias, gain, bias):
    half = jax.ShapeDtypeStruct((x.shape[0] // 2, x.shape[1]), jnp.bfloat16)
    return pl.pallas_call(
        ln2_kernel,
        out_shape=(
            half,
            half,
            jax.ShapeDtypeStruct(x.shape, jnp.float32),
        ),
        in_specs=[whole()] * 6,
        out_specs=(whole(),) * 3,
        cost_estimate=pl.CostEstimate(flops=12 * x.size, bytes_accessed=12 * x.size, transcendentals=0),
        compiler_params=pltpu.CompilerParams(vmem_limit_bytes=8 << 20),
        name="second_norm",
    )(x, mine, other, pbias, gain, bias)


def pass_kernel(right_ref, via_a_ref, left_ref, via_b_ref, to_right_ref, to_left_ref):
    f32 = jnp.float32
    half = via_a_ref.shape[0]
    near, far = slice(0, half), slice(half, 2 * half)
    to_right_ref[near, :] = (right_ref[near, :] + via_a_ref[...].astype(f32)).astype(to_right_ref.dtype)
    to_right_ref[far, :] = right_ref[far, :].astype(to_right_ref.dtype)
    to_left_ref[near, :] = left_ref[near, :].astype(to_left_ref.dtype)
    to_left_ref[far, :] = (left_ref[far, :] + via_b_ref[...].astype(f32)).astype(to_left_ref.dtype)


def pass_on(right, via_a, left, via_b):
    out = jax.ShapeDtypeStruct(right.shape, via_a.dtype)
    return pl.pallas_call(
        pass_kernel,
        out_shape=(out, out),
        in_specs=[whole()] * 4,
        out_specs=(whole(), whole()),
        cost_estimate=pl.CostEstimate(flops=200000, bytes_accessed=1000000, transcendentals=0),
        compiler_params=pltpu.CompilerParams(vmem_limit_bytes=8 << 20),
        name="pass_on",
    )(right, via_a, left, via_b)


def gelu(x):
    return 0.5 * x * (1.0 + lax.erf(x * 0.7071067811865476))


def second_product(hidden, w2):
    return lax.dot_general(hidden, w2, (((1,), (1,)), ((), ())), preferred_element_type=jnp.float32)


def load_kernel(slab, w_ref, w1, w2, b1, sem1, sem2, sem3):
    hid = w_ref.shape[3]
    copies = []
    for b in range(4):
        cols = pl.ds(b * hid, hid)
        for r in range(8):
            rows = pl.ds(r * slab, slab)
            copies.append(
                pltpu.make_async_copy(w_ref.at[r, b, pl.ds(0, slab)], w1.at[rows, cols], sem1.at[b, r])
            )
            copies.append(
                pltpu.make_async_copy(w_ref.at[r, b, pl.ds(slab, slab)], w2.at[rows, cols], sem2.at[b, r])
            )
        copies.append(pltpu.make_async_copy(w_ref.at[0, b, pl.ds(2 * slab, 16)], b1.at[b], sem3.at[b]))
    for copy in copies:
        copy.start()
    for copy in copies:
        copy.wait()


def load_weights(weights, slab):
    hid = weights.shape[3]
    panel = jax.ShapeDtypeStruct((8 * slab, 4 * hid), jnp.bfloat16)
    return pl.pallas_call(
        functools.partial(load_kernel, slab),
        out_shape=(panel, panel, jax.ShapeDtypeStruct((4, 16, hid), jnp.bfloat16)),
        in_specs=[pl.BlockSpec(memory_space=pltpu.HBM)],
        out_specs=(whole(),) * 3,
        scratch_shapes=[
            pltpu.SemaphoreType.DMA((4, 8)),
            pltpu.SemaphoreType.DMA((4, 8)),
            pltpu.SemaphoreType.DMA((4,)),
        ],
        cost_estimate=pl.CostEstimate(flops=1000000, bytes_accessed=18000000, transcendentals=0),
        compiler_params=pltpu.CompilerParams(vmem_limit_bytes=42 << 20),
        name="load_weights",
    )(weights)


def head_kernel(*refs):
    pieces, (w1, w2, b1, hidden, pfa_ref, pfb_ref, rows) = refs[:8], refs[8:]
    f32 = jnp.float32
    half = pieces[0].shape[0]
    for i, ref in enumerate(pieces):
        rows[i * half : (i + 1) * half] = ref[...]
    hid = b1.shape[2]
    for b in range(4):
        cols = slice(b * hid, (b + 1) * hid)
        for m in range(2):
            part = slice(4 * half * m, 4 * half * (m + 1))
            value = jnp.dot(rows[part], w1[:, cols], preferred_element_type=f32)
            value = value + b1[b, 0:1].astype(f32)
            hidden[part, cols] = gelu(value).astype(hidden.dtype)
    out = second_product(hidden[6 * half :], w2[...])
    pfa_ref[...] = out[:half].astype(pfa_ref.dtype)
    pfb_ref[...] = out[half:].astype(pfb_ref.dtype)


def mlp_head(pieces, w1, w2, b1):
    half, width = pieces[0].shape
    bf16 = jnp.bfloat16
    far = jax.ShapeDtypeStruct((half, width), bf16)
    return pl.pallas_call(
        head_kernel,
        out_shape=(jax.ShapeDtypeStruct((8 * half, w1.shape[1]), bf16), far, far),
        in_specs=[whole()] * 11,
        out_specs=(whole(),) * 3,
        scratch_shapes=[pltpu.VMEM((8 * half, width), bf16)],
        cost_estimate=pl.CostEstimate(flops=2770000000, bytes_accessed=12000000, transcendentals=800000),
        compiler_params=pltpu.CompilerParams(vmem_limit_bytes=40 << 20),
        name="mlp_head",
    )(*pieces, w1, w2, b1)


def sides_kernel(hidden, w2, left_ref, right_ref):
    own = left_ref.shape[0]
    out = second_product(hidden[own : 3 * own], w2[...])
    left_ref[...] = out[:own]
    right_ref[...] = out[own:]


def mlp_sides(hidden, w2):
    out = jax.ShapeDtypeStruct((hidden.shape[0] // 4, w2.shape[0]), jnp.float32)
    return pl.pallas_call(
        sides_kernel,
        out_shape=(out, out),
        in_specs=[whole()] * 2,
        out_specs=(whole(), whole()),
        cost_estimate=pl.CostEstimate(flops=1100000000, bytes_accessed=8000000, transcendentals=0),
        compiler_params=pltpu.CompilerParams(vmem_limit_bytes=24 << 20),
        name="mlp_sides",
    )(hidden, w2)


def own_kernel(hidden, w2, resid_ref, bias_ref, out_ref):
    own = out_ref.shape[0]
    out = second_product(hidden[:own], w2[...])
    out_ref[...] = resid_ref[...] + out + row(bias_ref).astype(jnp.float32)


def mlp_own(hidden, w2, resid, bias):
    return pl.pallas_call(
        own_kernel,
        out_shape=jax.ShapeDtypeStruct(resid.shape, jnp.float32),
        in_specs=[whole()] * 4,
        out_specs=whole(),
        cost_estimate=pl.CostEstimate(flops=550000000, bytes_accessed=8000000, transcendentals=0),
        compiler_params=pltpu.CompilerParams(vmem_limit_bytes=24 << 20),
        name="mlp_own",
    )(hidden, w2, resid, bias)


def layer(
    tokens_in,
    ln1_gain,
    ln1_bias,
    qkv_weight,
    qkv_bias,
    proj_weight,
    proj_bias,
    ln2_gain,
    ln2_bias,
    fc1_weight,
    fc1_bias,
    fc2_weight,
    fc2_bias,
):
    f32, bf16 = jnp.float32, jnp.bfloat16
    own = tokens_in.shape[0]
    width = tokens_in.shape[1]
    head = proj_weight.shape[0]
    slab = qkv_weight.shape[0]
    hid = fc1_weight.shape[1]
    core = lax.axis_index("core")
    z, yh = lax.axis_index("z"), lax.axis_index("yh")
    x, yl = lax.axis_index("x"), lax.axis_index("yl")

    pair = jnp.stack([qkv_weight, shift(qkv_weight, dyh=1)])
    low = shift(pair, dz=1)
    high = shift(pair, dz=3)
    bias_rows = jnp.broadcast_to(fc1_bias[None], (16, hid))
    stack = jnp.concatenate([fc1_weight, fc2_weight, bias_rows], axis=0)
    mlp = lax.all_gather(stack, ("z", "yh", "yl", "core"), axis=0, tiled=False)
    mlp = mlp.reshape(8, 4, stack.shape[0], hid)

    far = shift(low, dz=1)
    where = [(z + 4 - dz) % 4 * 2 + (yh + j) % 2 for dz in (0, 1, 3, 2) for j in range(2)]
    where = jnp.stack(where).astype(jnp.int32)
    w_own = place(where, qkv_bias, (pair, low, high, far))
    w_other = shift(w_own, dc=1)

    p_rows = jnp.stack([proj_weight, shift(proj_weight, dyh=1)])
    p_rows = [p_rows] + [shift(p_rows, dz=dz) for dz in (1, 3, 2)]
    which = []
    for r in range(8):
        dz = (z + 4 - r // 2) % 4
        which.append(jnp.where(dz > 1, 5 - dz, dz) * 2 + (r % 2 + yh) % 2)
    proj_own = place_proj(jnp.stack(which).astype(jnp.int32), p_rows)
    p_side = shift(proj_own, dyl=1)

    ln1 = first_norm(tokens_in, ln1_gain, ln1_bias)
    left = shift(ln1, dx=1)
    right = shift(ln1, dx=3)
    side = shift(ln1, dyl=1)
    side_left = shift(side, dx=1)
    side_right = shift(side, dx=3)
    far = shift(left, dx=1)
    side_far = shift(side_right, dx=3)
    near = (ln1, left, right, side)
    rest = (side_left, side_right, far, side_far)
    other = qkv_part(rest, w_other)
    swapped = [shift(qkv_part(near, w_other), dc=1), shift(other, dc=1)]
    mine = qkv_part(near + rest, w_own)
    p_side, _ = lax.optimization_barrier((p_side, mine))
    p_pair = jnp.stack([proj_own, p_side])
    p_left = shift(p_pair, dx=1)
    p_right = shift(p_pair, dx=3)
    p_fa = shift(p_left[0], dx=1)
    p_fb = shift(p_right[1], dx=3)
    parts = [mine] + swapped
    spots = [(0, 0), (1, 0), (3, 0), (0, 1), (1, 1), (3, 1), (2, 0), (2, 1)]
    places = [
        ((x + 4 - dx) % 4 * 2 + (yl + j) % 2) * 2 + (core + k) % 2 for k in range(2) for dx, j in spots
    ]
    attn = attend(jnp.stack(places).astype(jnp.int32), parts, head)
    heads = lax.all_to_all(attn.reshape(8, 2 * own, LANES), ("x", "yl"), 0, 0, tiled=True)
    order = [(0, 0), (0, 1), (1, 0), (1, 1), (3, 0), (3, 1), (2, 0), (2, 1)]
    where = [(x + 4 - dx) % 4 * 2 + (yl + j) % 2 for dx, j in order]
    where = jnp.stack(where + [core]).astype(jnp.int32)
    proj_sets = (p_pair, p_left, p_right, p_fa, p_fb)
    mine, other = project(where, heads, proj_sets, own, width)
    other = shift(other, dc=1)
    low2, high2, resid = second_norm(tokens_in, mine, other, proj_bias, ln2_gain, ln2_bias)

    left_low = shift(low2, dx=1)
    right_high = shift(high2, dx=3)
    left_high = shift(high2, dx=1)
    right_low = shift(low2, dx=3)
    far_low = shift(left_low, dx=1)
    far_high = shift(right_high, dx=3)
    w1, w2, b1 = load_weights(mlp, slab)
    pieces = (low2, high2, left_low, left_high, right_low, right_high, far_low, far_high)
    hidden, fa, fb = mlp_head(pieces, w1, w2, b1)

    via_a = shift(fa, dx=1)
    via_b = shift(fb, dx=3)
    o_left, o_right = mlp_sides(hidden, w2)
    to_right, to_left = pass_on(o_right, via_a, o_left, via_b)
    from_left = shift(to_right, dx=1)
    from_right = shift(to_left, dx=3)
    mine = mlp_own(hidden, w2, resid, fc2_bias)
    return (mine + from_left.astype(f32) + from_right.astype(f32)).astype(bf16)


def solution(mesh):
    fine = Mesh(np.asarray(mesh.devices).reshape(SIZES), AXES)
    in_specs = (
        P(AXES, None),
        P(),
        P(),
        P(ROW, COL),
        P(COL),
        P(COL, ROW),
        P(),
        P(),
        P(),
        P(ROW, COL),
        P(COL),
        P(ROW, COL),
        P(),
    )
    return jax.shard_map(layer, mesh=fine, in_specs=in_specs, out_specs=P(AXES, None), check_vma=False)
```

```python
import functools
import itertools

import jax
import jax.numpy as jnp
import numpy as np
from jax import lax
from jax.experimental import pallas as pl
from jax.experimental.pallas import tpu as pltpu
from jax.sharding import Mesh
from jax.sharding import PartitionSpec as P


LANES = 128
AXES = ("z", "yh", "x", "yl", "core")
SIZES = (4, 2, 4, 2, 2)
ROW = ("z", "yh")
COL = ("x", "yl", "core")


def shift(value, dz=0, dyh=0, dx=0, dyl=0, dc=0):
    pairs = []
    for place in itertools.product(*[range(n) for n in SIZES]):
        target = [(p + d) % n for p, d, n in zip(place, (dz, dyh, dx, dyl, dc), SIZES)]
        pairs.append(
            (int(np.ravel_multi_index(place, SIZES)), int(np.ravel_multi_index(target, SIZES)))
        )
    return lax.ppermute(value, AXES, pairs)


def whole():
    return pl.BlockSpec(memory_space=pltpu.VMEM)


def norm_rows(values, gain, bias):
    mean = jnp.mean(values, axis=-1, keepdims=True)
    centred = values - mean
    var = jnp.mean(centred * centred, axis=-1, keepdims=True)
    return centred * lax.rsqrt(var + 1e-06) * gain.astype(jnp.float32) + bias.astype(jnp.float32)


def row(ref):
    return ref[...].reshape(1, ref.shape[0])


def ln1_kernel(x_ref, gain_ref, bias_ref, out_ref):
    values = x_ref[...].astype(jnp.float32)
    out_ref[...] = norm_rows(values, row(gain_ref), row(bias_ref)).astype(out_ref.dtype)


def first_norm(x, gain, bias):
    return pl.pallas_call(
        ln1_kernel,
        out_shape=jax.ShapeDtypeStruct(x.shape, jnp.bfloat16),
        in_specs=[whole()] * 3,
        out_specs=whole(),
        cost_estimate=pl.CostEstimate(flops=10 * x.size, bytes_accessed=4 * x.size, transcendentals=0),
        compiler_params=pltpu.CompilerParams(vmem_limit_bytes=8 << 20),
        name="first_norm",
    )(x, gain, bias)


def spread(values, head, ones):
    rows = values.shape[0]
    gap = jnp.zeros((rows, LANES - head), values.dtype)
    lane = lax.broadcasted_iota(jnp.int32, (rows, LANES - head), 1)
    last = jnp.where(lane == 0, jnp.ones_like(gap), gap) if ones else gap
    q, k, v = (values[:, n * head : (n + 1) * head] for n in range(3))
    return jnp.concatenate([q, gap, k, gap, v, last], axis=1)


def place_kernel(head, where_ref, bias_ref, own_ref, low_ref, high_ref, far_ref, w_ref):
    slab = own_ref.shape[1]
    for n, ref in enumerate((own_ref, low_ref, high_ref, far_ref)):
        for j in range(2):
            first = pl.multiple_of(where_ref[2 * n + j] * slab, 16)
            value = spread(ref[j].astype(jnp.float32), head, False)
            w_ref[pl.ds(first, slab), :] = value.astype(w_ref.dtype)
    bias = spread(row(bias_ref).astype(jnp.float32), head, True)
    w_ref[8 * slab :, :] = jnp.broadcast_to(bias, (16, bias.shape[1])).astype(w_ref.dtype)


def place(where, bias, pieces):
    _, slab, cols = pieces[0].shape
    return pl.pallas_call(
        functools.partial(place_kernel, cols // 3),
        out_shape=jax.ShapeDtypeStruct((8 * slab + 16, 3 * LANES), jnp.bfloat16),
        in_specs=[pl.BlockSpec(memory_space=pltpu.SMEM)] + [whole()] * 5,
        out_specs=whole(),
        cost_estimate=pl.CostEstimate(flops=1000000, bytes_accessed=3000000, transcendentals=0),
        compiler_params=pltpu.CompilerParams(vmem_limit_bytes=12 << 20),
        name="place_rows",
    )(where, bias, *pieces)


def place_proj_kernel(which_ref, own_ref, low_ref, high_ref, far_ref, out_ref, held):
    slab = own_ref.shape[2]
    for n, ref in enumerate((own_ref, low_ref, high_ref, far_ref)):
        for j in range(2):
            held[2 * n + j] = ref[j].astype(jnp.float32)
    for r in range(8):
        out_ref[:, r * slab : (r + 1) * slab] = held[which_ref[r]].astype(out_ref.dtype)


def place_proj(which, pieces):
    _, head, slab = pieces[0].shape
    return pl.pallas_call(
        place_proj_kernel,
        out_shape=jax.ShapeDtypeStruct((head, 8 * slab), jnp.bfloat16),
        in_specs=[pl.BlockSpec(memory_space=pltpu.SMEM)] + [whole()] * 4,
        out_specs=whole(),
        scratch_shapes=[pltpu.VMEM((8, head, slab), jnp.float32)],
        cost_estimate=pl.CostEstimate(flops=100000, bytes_accessed=1000000, transcendentals=0),
        compiler_params=pltpu.CompilerParams(vmem_limit_bytes=8 << 20),
        name="place_proj",
    )(which, *pieces)


def qkv_kernel(count, *refs):
    pieces, (w_ref, out_ref, rows, sems) = refs[:count], refs[count:]
    width = rows.shape[1]
    first = 0
    copies = []
    for n, ref in enumerate(pieces):
        copies.append(pltpu.make_async_copy(ref, rows.at[pl.ds(first, ref.shape[0])], sems.at[n]))
        first += ref.shape[0]
    for copy in copies:
        copy.start()
    for copy in copies:
        copy.wait()
    bias = w_ref[width : width + 1, :].astype(jnp.float32)
    value = jnp.dot(rows[...], w_ref[:width, :], preferred_element_type=jnp.float32)
    out_ref[...] = (value + bias).astype(out_ref.dtype)


def qkv_part(pieces, weights):
    rows = sum(p.shape[0] for p in pieces)
    cols = weights.shape[1]
    return pl.pallas_call(
        functools.partial(qkv_kernel, len(pieces)),
        out_shape=jax.ShapeDtypeStruct((rows, cols), jnp.bfloat16),
        in_specs=[pl.BlockSpec(memory_space=pl.ANY)] * len(pieces) + [whole()],
        out_specs=whole(),
        scratch_shapes=[
            pltpu.VMEM((rows, pieces[0].shape[1]), jnp.bfloat16),
            pltpu.SemaphoreType.DMA((len(pieces),)),
        ],
        cost_estimate=pl.CostEstimate(
            flops=2 * rows * cols * weights.shape[0], bytes_accessed=4000000, transcendentals=0
        ),
        compiler_params=pltpu.CompilerParams(vmem_limit_bytes=16 << 20),
        name="qkv_part",
    )(*pieces, weights)


def attend_kernel(head, where_ref, *refs):
    f32 = jnp.float32
    parts, (out_ref, q_ref, k_ref, v_ref, s_ref, sems) = refs[:3], refs[3:]
    length = q_ref.shape[0]
    first = 0
    copies = []
    for n, ref in enumerate(parts):
        rows = pl.ds(first, ref.shape[0])
        for m, target in enumerate((q_ref, k_ref, v_ref)):
            source = ref.at[:, pl.ds(m * LANES, LANES)]
            copies.append(pltpu.make_async_copy(source, target.at[rows], sems.at[n, m]))
        first += ref.shape[0]
    for copy in copies:
        copy.start()
    for copy in copies:
        copy.wait()
    block = s_ref.shape[1]
    steps = length // block
    scale = 1.4426950408889634 / head**0.5

    def scores(i):
        s_ref[i % 2] = lax.dot_general(
            q_ref[i * block : (i + 1) * block, :],
            k_ref[...],
            (((1,), (1,)), ((), ())),
            preferred_element_type=f32,
        )

    scores(0)
    for i in range(steps):
        value = s_ref[i % 2]
        if i + 1 < steps:
            scores(i + 1)
        top = jnp.max(value, axis=-1, keepdims=True)
        expo = jnp.exp2((value - top) * scale).astype(jnp.bfloat16)
        mixed = jnp.dot(expo, v_ref[...], preferred_element_type=f32)
        mixed = (mixed / mixed[:, head : head + 1]).astype(out_ref.dtype)
        for n in range(block // LANES):
            out_ref[where_ref[i * (block // LANES) + n]] = mixed[n * LANES : (n + 1) * LANES]


def attend(where, parts, head):
    length = sum(p.shape[0] for p in parts)
    block, bf16 = 256, jnp.bfloat16
    return pl.pallas_call(
        functools.partial(attend_kernel, head),
        out_shape=jax.ShapeDtypeStruct((length // LANES, LANES, LANES), bf16),
        in_specs=[pl.BlockSpec(memory_space=pltpu.SMEM)] + [pl.BlockSpec(memory_space=pl.ANY)] * 3,
        out_specs=whole(),
        scratch_shapes=[pltpu.VMEM((length, LANES), bf16)] * 3
        + [pltpu.VMEM((2, block, length), jnp.float32), pltpu.SemaphoreType.DMA((3, 3))],
        cost_estimate=pl.CostEstimate(
            flops=4 * length * length * LANES, bytes_accessed=8000000, transcendentals=length * length
        ),
        compiler_params=pltpu.CompilerParams(vmem_limit_bytes=32 << 20),
        name="attend",
    )(where, *parts)


def proj_kernel(where_ref, heads_ref, own_ref, left_ref, right_ref, fa_ref, fb_ref,
                mine_ref, other_ref, h_ref, p_ref):
    own = mine_ref.shape[0]
    core = where_ref[8]
    head = own_ref.shape[1]
    for i in range(8):
        piece = (own_ref, left_ref, right_ref)[i // 2][i % 2] if i < 6 else (fa_ref, fb_ref)[i % 2][...]
        p_ref[i * LANES : i * LANES + head, :] = piece
        p_ref[i * LANES + head : (i + 1) * LANES, :] = jnp.zeros(
            (LANES - head, p_ref.shape[1]), p_ref.dtype
        )
        h_ref[:, i * LANES : (i + 1) * LANES] = heads_ref[where_ref[i]]
    for target, first in ((other_ref, (1 - core) * own), (mine_ref, core * own)):
        left = h_ref[pl.ds(pl.multiple_of(first, own), own), :]
        total = jnp.dot(left, p_ref[...], preferred_element_type=jnp.float32)
        target[...] = total.astype(target.dtype)


def project(where, heads, pieces, own, width):
    out = jax.ShapeDtypeStruct((own, width), jnp.bfloat16)
    return pl.pallas_call(
        proj_kernel,
        out_shape=(out, out),
        in_specs=[pl.BlockSpec(memory_space=pltpu.SMEM)] + [whole()] * 6,
        out_specs=(whole(), whole()),
        scratch_shapes=[
            pltpu.VMEM((2 * own, 8 * LANES), jnp.bfloat16),
            pltpu.VMEM((8 * LANES, width), jnp.bfloat16),
        ],
        cost_estimate=pl.CostEstimate(flops=740000000, bytes_accessed=4000000, transcendentals=0),
        compiler_params=pltpu.CompilerParams(vmem_limit_bytes=24 << 20),
        name="project",
    )(where, heads, *pieces)


def ln2_kernel(x_ref, mine_ref, other_ref, pbias_ref, gain_ref, bias_ref, low_ref, high_ref, resid_ref):
    f32 = jnp.float32
    total = mine_ref[...].astype(f32) + other_ref[...].astype(f32)
    resid = x_ref[...].astype(f32) + total + row(pbias_ref).astype(f32)
    resid_ref[...] = resid
    half = low_ref.shape[0]
    value = norm_rows(resid, row(gain_ref), row(bias_ref)).astype(low_ref.dtype)
    low_ref[...] = value[:half]
    high_ref[...] = value[half:]


def second_norm(x, mine, other, pbias, gain, bias):
    half = jax.ShapeDtypeStruct((x.shape[0] // 2, x.shape[1]), jnp.bfloat16)
    return pl.pallas_call(
        ln2_kernel,
        out_shape=(
            half,
            half,
            jax.ShapeDtypeStruct(x.shape, jnp.float32),
        ),
        in_specs=[whole()] * 6,
        out_specs=(whole(),) * 3,
        cost_estimate=pl.CostEstimate(flops=12 * x.size, bytes_accessed=12 * x.size, transcendentals=0),
        compiler_params=pltpu.CompilerParams(vmem_limit_bytes=8 << 20),
        name="second_norm",
    )(x, mine, other, pbias, gain, bias)


def pass_kernel(right_ref, via_a_ref, left_ref, via_b_ref, to_right_ref, to_left_ref):
    f32 = jnp.float32
    half = via_a_ref.shape[0]
    near, far = slice(0, half), slice(half, 2 * half)
    to_right_ref[near, :] = (right_ref[near, :] + via_a_ref[...].astype(f32)).astype(to_right_ref.dtype)
    to_right_ref[far, :] = right_ref[far, :].astype(to_right_ref.dtype)
    to_left_ref[near, :] = left_ref[near, :].astype(to_left_ref.dtype)
    to_left_ref[far, :] = (left_ref[far, :] + via_b_ref[...].astype(f32)).astype(to_left_ref.dtype)


def pass_on(right, via_a, left, via_b):
    out = jax.ShapeDtypeStruct(right.shape, via_a.dtype)
    return pl.pallas_call(
        pass_kernel,
        out_shape=(out, out),
        in_specs=[whole()] * 4,
        out_specs=(whole(), whole()),
        cost_estimate=pl.CostEstimate(flops=200000, bytes_accessed=1000000, transcendentals=0),
        compiler_params=pltpu.CompilerParams(vmem_limit_bytes=8 << 20),
        name="pass_on",
    )(right, via_a, left, via_b)


def gelu(x):
    return 0.5 * x * (1.0 + lax.erf(x * 0.7071067811865476))


def second_product(hidden, w2):
    return lax.dot_general(hidden, w2, (((1,), (1,)), ((), ())), preferred_element_type=jnp.float32)


def load_kernel(slab, w_ref, w1, w2, b1, sem1, sem2, sem3):
    hid = w_ref.shape[3]
    copies = []
    for b in range(4):
        cols = pl.ds(b * hid, hid)
        for r in range(8):
            rows = pl.ds(r * slab, slab)
            copies.append(
                pltpu.make_async_copy(w_ref.at[r, b, pl.ds(0, slab)], w1.at[rows, cols], sem1.at[b, r])
            )
            copies.append(
                pltpu.make_async_copy(w_ref.at[r, b, pl.ds(slab, slab)], w2.at[rows, cols], sem2.at[b, r])
            )
        copies.append(pltpu.make_async_copy(w_ref.at[0, b, pl.ds(2 * slab, 16)], b1.at[b], sem3.at[b]))
    for copy in copies:
        copy.start()
    for copy in copies:
        copy.wait()


def load_weights(weights, slab):
    hid = weights.shape[3]
    panel = jax.ShapeDtypeStruct((8 * slab, 4 * hid), jnp.bfloat16)
    return pl.pallas_call(
        functools.partial(load_kernel, slab),
        out_shape=(panel, panel, jax.ShapeDtypeStruct((4, 16, hid), jnp.bfloat16)),
        in_specs=[pl.BlockSpec(memory_space=pltpu.HBM)],
        out_specs=(whole(),) * 3,
        scratch_shapes=[
            pltpu.SemaphoreType.DMA((4, 8)),
            pltpu.SemaphoreType.DMA((4, 8)),
            pltpu.SemaphoreType.DMA((4,)),
        ],
        cost_estimate=pl.CostEstimate(flops=1000000, bytes_accessed=18000000, transcendentals=0),
        compiler_params=pltpu.CompilerParams(vmem_limit_bytes=42 << 20),
        name="load_weights",
    )(weights)


def head_kernel(*refs):
    pieces, (w1, w2, b1, hidden, pfa_ref, pfb_ref, rows) = refs[:8], refs[8:]
    f32 = jnp.float32
    half = pieces[0].shape[0]
    for i, ref in enumerate(pieces):
        rows[i * half : (i + 1) * half] = ref[...]
    hid = b1.shape[2]
    for b in range(4):
        cols = slice(b * hid, (b + 1) * hid)
        for m in range(2):
            part = slice(4 * half * m, 4 * half * (m + 1))
            value = jnp.dot(rows[part], w1[:, cols], preferred_element_type=f32)
            value = value + b1[b, 0:1].astype(f32)
            hidden[part, cols] = gelu(value).astype(hidden.dtype)
    out = second_product(hidden[6 * half :], w2[...])
    pfa_ref[...] = out[:half].astype(pfa_ref.dtype)
    pfb_ref[...] = out[half:].astype(pfb_ref.dtype)


def mlp_head(pieces, w1, w2, b1):
    half, width = pieces[0].shape
    bf16 = jnp.bfloat16
    far = jax.ShapeDtypeStruct((half, width), bf16)
    return pl.pallas_call(
        head_kernel,
        out_shape=(jax.ShapeDtypeStruct((8 * half, w1.shape[1]), bf16), far, far),
        in_specs=[whole()] * 11,
        out_specs=(whole(),) * 3,
        scratch_shapes=[pltpu.VMEM((8 * half, width), bf16)],
        cost_estimate=pl.CostEstimate(flops=2770000000, bytes_accessed=12000000, transcendentals=800000),
        compiler_params=pltpu.CompilerParams(vmem_limit_bytes=40 << 20),
        name="mlp_head",
    )(*pieces, w1, w2, b1)


def sides_kernel(hidden, w2, left_ref, right_ref):
    own = left_ref.shape[0]
    out = second_product(hidden[own : 3 * own], w2[...])
    left_ref[...] = out[:own]
    right_ref[...] = out[own:]


def mlp_sides(hidden, w2):
    out = jax.ShapeDtypeStruct((hidden.shape[0] // 4, w2.shape[0]), jnp.float32)
    return pl.pallas_call(
        sides_kernel,
        out_shape=(out, out),
        in_specs=[whole()] * 2,
        out_specs=(whole(), whole()),
        cost_estimate=pl.CostEstimate(flops=1100000000, bytes_accessed=8000000, transcendentals=0),
        compiler_params=pltpu.CompilerParams(vmem_limit_bytes=24 << 20),
        name="mlp_sides",
    )(hidden, w2)


def own_kernel(hidden, w2, resid_ref, bias_ref, out_ref):
    own = out_ref.shape[0]
    out = second_product(hidden[:own], w2[...])
    out_ref[...] = resid_ref[...] + out + row(bias_ref).astype(jnp.float32)


def mlp_own(hidden, w2, resid, bias):
    return pl.pallas_call(
        own_kernel,
        out_shape=jax.ShapeDtypeStruct(resid.shape, jnp.float32),
        in_specs=[whole()] * 4,
        out_specs=whole(),
        cost_estimate=pl.CostEstimate(flops=550000000, bytes_accessed=8000000, transcendentals=0),
        compiler_params=pltpu.CompilerParams(vmem_limit_bytes=24 << 20),
        name="mlp_own",
    )(hidden, w2, resid, bias)


def layer(
    tokens_in,
    ln1_gain,
    ln1_bias,
    qkv_weight,
    qkv_bias,
    proj_weight,
    proj_bias,
    ln2_gain,
    ln2_bias,
    fc1_weight,
    fc1_bias,
    fc2_weight,
    fc2_bias,
):
    f32, bf16 = jnp.float32, jnp.bfloat16
    own = tokens_in.shape[0]
    width = tokens_in.shape[1]
    head = proj_weight.shape[0]
    slab = qkv_weight.shape[0]
    hid = fc1_weight.shape[1]
    core = lax.axis_index("core")
    z, yh = lax.axis_index("z"), lax.axis_index("yh")
    x, yl = lax.axis_index("x"), lax.axis_index("yl")

    pair = jnp.stack([qkv_weight, shift(qkv_weight, dyh=1)])
    low = shift(pair, dz=1)
    high = shift(pair, dz=3)
    bias_rows = jnp.broadcast_to(fc1_bias[None], (16, hid))
    stack = jnp.concatenate([fc1_weight, fc2_weight, bias_rows], axis=0)
    mlp = lax.all_gather(stack, ("z", "yh", "yl", "core"), axis=0, tiled=False)
    mlp = mlp.reshape(8, 4, stack.shape[0], hid)

    far = shift(low, dz=1)
    where = [(z + 4 - dz) % 4 * 2 + (yh + j) % 2 for dz in (0, 1, 3, 2) for j in range(2)]
    where = jnp.stack(where).astype(jnp.int32)
    w_own = place(where, qkv_bias, (pair, low, high, far))
    w_other = shift(w_own, dc=1)

    p_rows = jnp.stack([proj_weight, shift(proj_weight, dyh=1)])
    p_rows = [p_rows] + [shift(p_rows, dz=dz) for dz in (1, 3, 2)]
    which = []
    for r in range(8):
        dz = (z + 4 - r // 2) % 4
        which.append(jnp.where(dz > 1, 5 - dz, dz) * 2 + (r % 2 + yh) % 2)
    proj_own = place_proj(jnp.stack(which).astype(jnp.int32), p_rows)
    p_side = shift(proj_own, dyl=1)

    ln1 = first_norm(tokens_in, ln1_gain, ln1_bias)
    left = shift(ln1, dx=1)
    right = shift(ln1, dx=3)
    side = shift(ln1, dyl=1)
    side_left = shift(side, dx=1)
    side_right = shift(side, dx=3)
    far = shift(left, dx=1)
    side_far = shift(side_right, dx=3)
    near = (ln1, left, right, side)
    rest = (side_left, side_right, far, side_far)
    other = qkv_part(rest, w_other)
    swapped = [shift(qkv_part(near, w_other), dc=1), shift(other, dc=1)]
    mine = qkv_part(near + rest, w_own)
    p_side, _ = lax.optimization_barrier((p_side, mine))
    p_pair = jnp.stack([proj_own, p_side])
    p_left = shift(p_pair, dx=1)
    p_right = shift(p_pair, dx=3)
    p_fa = shift(p_left[0], dx=1)
    p_fb = shift(p_right[1], dx=3)
    parts = [mine] + swapped
    spots = [(0, 0), (1, 0), (3, 0), (0, 1), (1, 1), (3, 1), (2, 0), (2, 1)]
    places = [
        ((x + 4 - dx) % 4 * 2 + (yl + j) % 2) * 2 + (core + k) % 2 for k in range(2) for dx, j in spots
    ]
    attn = attend(jnp.stack(places).astype(jnp.int32), parts, head)
    heads = lax.all_to_all(attn.reshape(8, 2 * own, LANES), ("x", "yl"), 0, 0, tiled=True)
    order = [(0, 0), (0, 1), (1, 0), (1, 1), (3, 0), (3, 1), (2, 0), (2, 1)]
    where = [(x + 4 - dx) % 4 * 2 + (yl + j) % 2 for dx, j in order]
    where = jnp.stack(where + [core]).astype(jnp.int32)
    proj_sets = (p_pair, p_left, p_right, p_fa, p_fb)
    mine, other = project(where, heads, proj_sets, own, width)
    other = shift(other, dc=1)
    low2, high2, resid = second_norm(tokens_in, mine, other, proj_bias, ln2_gain, ln2_bias)

    left_low = shift(low2, dx=1)
    right_high = shift(high2, dx=3)
    left_high = shift(high2, dx=1)
    right_low = shift(low2, dx=3)
    far_low = shift(left_low, dx=1)
    far_high = shift(right_high, dx=3)
    w1, w2, b1 = load_weights(mlp, slab)
    pieces = (low2, high2, left_low, left_high, right_low, right_high, far_low, far_high)
    hidden, fa, fb = mlp_head(pieces, w1, w2, b1)

    via_a = shift(fa, dx=1)
    via_b = shift(fb, dx=3)
    o_left, o_right = mlp_sides(hidden, w2)
    to_right, to_left = pass_on(o_right, via_a, o_left, via_b)
    from_left = shift(to_right, dx=1)
    from_right = shift(to_left, dx=3)
    mine = mlp_own(hidden, w2, resid, fc2_bias)
    return (mine + from_left.astype(f32) + from_right.astype(f32)).astype(bf16)


def solution(mesh):
    fine = Mesh(np.asarray(mesh.devices).reshape(SIZES), AXES)
    in_specs = (
        P(AXES, None),
        P(),
        P(),
        P(ROW, COL),
        P(COL),
        P(COL, ROW),
        P(),
        P(),
        P(),
        P(ROW, COL),
        P(COL),
        P(ROW, COL),
        P(),
    )
    return jax.shard_map(layer, mesh=fine, in_specs=in_specs, out_specs=P(AXES, None), check_vma=False)
```
